32 devices in a mesh: sa: 2 (over y), gx: 8 (over z, core), gy: 2 (over x).
Axes of the slice: x: 2, y: 2, z: 4, core: 2. Of those that a mesh axis runs over, the one named last changes fastest.
Arguments:
- pred_frames: float32 [12, 4096], P(None, ('sa', 'gx', 'gy')), parts along dimension 1, may hold values from -24 to 24, as said below
- true_frames: float32 [12, 4096], P(None, ('sa', 'gx', 'gy')), parts along dimension 1, may hold values from -24 to 24, as said below
- pred_atoms: float32 [3, 7168], P(None, ('sa', 'gx', 'gy')), parts along dimension 1, may hold values from -24 to 24
- true_atoms: float32 [3, 7168], P(None, ('sa', 'gx', 'gy')), parts along dimension 1, may hold values from -24 to 24
- atom_mask: int32 [7168], P(('sa', 'gx', 'gy')), parts along dimension 0, may hold values from 0 to 1, as said below
- residue_types: int32 [512], P(('sa', 'gx', 'gy')), parts along dimension 0, may hold values from 0 to 19
- swap_flags: int32 [512], P(('sa', 'gx', 'gy')), parts along dimension 0, may hold values from 0 to 1
Outputs:
- frame_loss: float32 [4096], P(('sa', 'gx', 'gy')), parts along dimension 0
- atom_loss: float32 [7168], P(('sa', 'gx', 'gy')), parts along dimension 0
- total_loss: float32 [2], P('sa'), parts along dimension 0
The draws below stay inside these ranges and needn't reach their ends.
There are 2 independent parts, one for each index of `sa`. The reference program is written for one: setup_inputs(seed, part) draws one part's arguments, and reference() takes and returns one part's arrays. A program takes and returns all parts, laid end to end along the dimension named above; each array names one. Nothing has to cross between parts.
Inputs may be any that keep to these rules, and one draw needn't show every extreme that they name: `atom_mask`: atom slots 0 to 3 of every residue, its backbone atoms, are 1. `pred_frames`: rows 0 to 8 of each frame hold a rotation matrix, row-major; rows 9 to 11 its translation. `true_frames`: rows 0 to 8 of each frame hold a rotation matrix, row-major; rows 9 to 11 its translation.
All inputs are finite; a program needn't handle non-finite values.
Results may differ from the reference program's by a relative error of at most 0.0001.
Values sent between devices are 32-bit elements; how exact they have to be, the bound alone decides.
No kernel may reach another device: no remote copies, remote signals or barrier semaphores. Data moves between devices by JAX's collectives and lax.ppermute only.
A program may use at most 64 MiB of HBM per device.

```python
import math
import jax
import jax.numpy as jnp
import numpy as np
from jax import lax

RES = 256


def quaternion_rotation(quats):
    quats = quats / jnp.sqrt(jnp.sum(quats * quats, axis=0, keepdims=True) + 1e-12)
    real_part = quats[0]
    first_imag = quats[1]
    second_imag = quats[2]
    third_imag = quats[3]
    entries = [1.0 - 2.0 * (second_imag * second_imag + third_imag * third_imag), 2.0 * (first_imag * second_imag - real_part * third_imag), 2.0 * (first_imag * third_imag + real_part * second_imag), 2.0 * (first_imag * second_imag + real_part * third_imag), 1.0 - 2.0 * (first_imag * first_imag + third_imag * third_imag), 2.0 * (second_imag * third_imag - real_part * first_imag), 2.0 * (first_imag * third_imag - real_part * second_imag), 2.0 * (second_imag * third_imag + real_part * first_imag), 1.0 - 2.0 * (first_imag * first_imag + second_imag * second_imag)]
    return jnp.stack(entries, axis=0)


def geometry(key):
    frames_total = RES * 8
    atoms_total = RES * 14
    half_side = 8.0 + RES // 64
    streams = jax.random.split(jax.random.fold_in(key, 7771), 8)
    centers = jax.random.uniform(streams[0], (3, RES), jnp.float32, -half_side, half_side)
    spread = jnp.exp(jnp.log(8.0) * jnp.arange(RES, dtype=jnp.float32) / RES)
    spread = spread * jax.random.uniform(streams[1], (RES,), jnp.float32, 0.5, 1.5)
    true_rotation = quaternion_rotation(jax.random.normal(streams[2], (4, frames_total), jnp.float32))
    true_shift = (centers[:, :, None] + jax.random.uniform(streams[3], (3, RES, 8), jnp.float32, -2.0, 2.0)).reshape(3, frames_total)
    true_positions = (centers[:, :, None] + jax.random.uniform(streams[4], (3, RES, 14), jnp.float32, -3.0, 3.0)).reshape(3, atoms_total)
    frame_spread = jnp.repeat(spread, 8)
    atom_spread = jnp.repeat(spread, 14)
    tilt_axis = jax.random.normal(streams[5], (3, frames_total), jnp.float32)
    atom_noise = 0.5 * jax.random.uniform(streams[7], (3, atoms_total), jnp.float32, -1.0, 1.0)
    tilt = 0.02 * frame_spread[None, :] * tilt_axis
    delta = quaternion_rotation(jnp.concatenate([jnp.ones((1, frames_total), jnp.float32), 0.5 * tilt], axis=0))
    pred_rotation = jnp.einsum('akf,kbf->abf', true_rotation.reshape(3, 3, frames_total), delta.reshape(3, 3, frames_total)).reshape(9, frames_total)
    pred_shift = true_shift + 0.4 * frame_spread[None, :] * jax.random.uniform(streams[6], (3, frames_total), jnp.float32, -1.0, 1.0)
    pred_positions = true_positions + atom_spread[None, :] * atom_noise
    pred_frames = jnp.concatenate([pred_rotation, pred_shift], axis=0)
    true_frames = jnp.concatenate([true_rotation, true_shift], axis=0)
    return (pred_frames, true_frames, pred_positions, true_positions)


def draw_pred_frames(key, part):
    return geometry(key)[0]


def draw_true_frames(key, part):
    return geometry(key)[1]


def draw_pred_atoms(key, part):
    return geometry(key)[2]


def draw_true_atoms(key, part):
    return geometry(key)[3]


def draw_atom_mask(key, part):
    levels = jax.random.randint(jax.random.fold_in(key, 5113), (RES, 14), 0, 5)
    backbone = jnp.arange(14)[None, :] < 4
    return jnp.where(backbone | (levels > 0), 1, 0).astype(jnp.int32).reshape(RES * 14)


def place_ends(result, own_key, least, largest):
    longest = result.shape.index(max(result.shape))
    spots = []
    for shift in (0, 1):
        where = [jax.random.randint(jax.random.fold_in(own_key, axis), (), 0, length) for axis, length in enumerate(result.shape)]
        where[longest] = (where[longest] + shift) % result.shape[longest]
        spots.append(tuple(where))
    return result.at[spots[0]].set(least).at[spots[1]].set(largest)


def setup_inputs(seed: int = 0, part: int = 0) -> dict:
    seeds = jax.random.split(jax.random.key(seed), 8)
    part_splits = jax.random.split(jax.random.fold_in(seeds[7], part), 8)
    return {
        "pred_frames": draw_pred_frames(jax.random.fold_in(jax.random.fold_in(seeds[7], part), 71), part),
        "true_frames": draw_true_frames(jax.random.fold_in(jax.random.fold_in(seeds[7], part), 71), part),
        "pred_atoms": draw_pred_atoms(jax.random.fold_in(jax.random.fold_in(seeds[7], part), 71), part),
        "true_atoms": draw_true_atoms(jax.random.fold_in(jax.random.fold_in(seeds[7], part), 71), part),
        "atom_mask": draw_atom_mask(jax.random.fold_in(jax.random.fold_in(seeds[7], part), 71), part),
        "residue_types": place_ends(jax.random.randint(part_splits[5], (RES,), 0, 20), jax.random.fold_in(part_splits[5], 1), 0, 19).astype(jnp.int32),
        "swap_flags": place_ends(jax.random.randint(part_splits[6], (RES,), 0, 2), jax.random.fold_in(part_splits[6], 1), 0, 1).astype(jnp.int32),
    }


eps_square = 0.0001
clamp_length = 10.0

def residue_tables():
    atom_counts = np.array([5, 11, 8, 8, 6, 9, 9, 4, 10, 8, 8, 9, 8, 11, 7, 6, 7, 14, 12, 7])
    chi_counts = np.array([0, 4, 2, 2, 1, 3, 3, 0, 2, 2, 2, 4, 3, 2, 2, 1, 1, 2, 2, 1])
    atom_table = (np.arange(14)[None, :] < atom_counts[:, None]).astype(np.float32)
    slot_ids = np.arange(8)[None, :]
    frame_table = ((slot_ids == 0) | (slot_ids == 3) | (slot_ids >= 4) & (slot_ids - 3 <= chi_counts[:, None])).astype(np.float32)
    partner_table = np.tile(np.arange(14), (20, 1))
    for restype, swap_pairs in ((3, ((6, 7),)), (6, ((7, 8),)), (13, ((6, 7), (8, 9))), (18, ((6, 7), (8, 9)))):
        for first_slot, second_slot in swap_pairs:
            partner_table[restype, first_slot] = second_slot
            partner_table[restype, second_slot] = first_slot
    flip_table = np.zeros((20, 8), np.float32)
    flip_table[3, 5] = 1.0
    flip_table[13, 5] = 1.0
    flip_table[18, 5] = 1.0
    flip_table[6, 6] = 1.0
    sign_table = np.array([1, -1, -1, 1, -1, -1, 1, -1, -1, 1, 1, 1], np.float32)
    return (atom_table, frame_table, partner_table, flip_table, sign_table)

def type_onehot(residue_types):
    return residue_types[:, None] == jnp.arange(20, dtype=jnp.int32)[None, :]

def frame_terms(pred_frames, true_frames, residue_types, swap_flags):
    tables = residue_tables()
    onehot = type_onehot(residue_types).astype(jnp.float32)
    frame_table = jnp.asarray(tables[1], dtype=jnp.float32)
    flip_table = jnp.asarray(tables[3], dtype=jnp.float32)
    sign_table = jnp.asarray(tables[4], dtype=jnp.float32)
    exists = lax.optimization_barrier(jnp.sum(onehot[:, :, None] * frame_table[None], axis=1))
    flips = lax.optimization_barrier(jnp.sum(onehot[:, :, None] * flip_table[None], axis=1)) * swap_flags[:, None].astype(jnp.float32)
    residues = residue_types.shape[0]
    shaped = true_frames.reshape(12, residues, 8)
    resolved = jnp.where(flips[None] > 0.5, shaped * sign_table[:, None, None], shaped).reshape(12, residues * 8)
    rot_pred = pred_frames[:9]
    rot_true = resolved[:9]
    offsets = []
    for column in range(3):
        true_part = rot_true[column] * resolved[9] + rot_true[3 + column] * resolved[10] + rot_true[6 + column] * resolved[11]
        pred_part = rot_pred[column] * pred_frames[9] + rot_pred[3 + column] * pred_frames[10] + rot_pred[6 + column] * pred_frames[11]
        offsets.append(true_part - pred_part)
    return (rot_pred, rot_true, jnp.stack(offsets, axis=0), exists.reshape(residues * 8))

def atom_terms(true_atoms, atom_mask, residue_types, swap_flags):
    tables = residue_tables()
    onehot_int = type_onehot(residue_types).astype(jnp.int32)
    onehot = onehot_int.astype(jnp.float32)
    partner_table = jnp.asarray(tables[2], dtype=jnp.int32)
    atom_table = jnp.asarray(tables[0], dtype=jnp.float32)
    partners = lax.optimization_barrier(jnp.sum(onehot_int[:, :, None] * partner_table[None], axis=1)).astype(jnp.int32)
    own_slots = jnp.broadcast_to(jnp.arange(14, dtype=jnp.int32)[None, :], partners.shape)
    source = jnp.where(swap_flags[:, None] == 1, partners, own_slots).astype(jnp.int32)
    residues = residue_types.shape[0]
    shaped = true_atoms.reshape(3, residues, 14)
    resolved = jnp.take_along_axis(shaped, jnp.broadcast_to(source[None], shaped.shape), axis=2).reshape(3, residues * 14)
    mask_resolved = jnp.take_along_axis(atom_mask.reshape(residues, 14), source, axis=1)
    exists = lax.optimization_barrier(jnp.sum(onehot[:, :, None] * atom_table[None], axis=1))
    weight = (exists * mask_resolved.astype(jnp.float32)).reshape(residues * 14)
    return (resolved, weight)

def clamped_errors(frame_side, atom_side):
    rot_pred, rot_true, offset = frame_side
    pred_pos, true_pos = atom_side
    squares = jnp.zeros((offset.shape[1], pred_pos.shape[1]), jnp.float32)
    for column in range(3):
        error = offset[column][:, None]
        for axis_row in range(3):
            error = error + rot_pred[3 * axis_row + column][:, None] * pred_pos[axis_row][None, :]
            error = error - rot_true[3 * axis_row + column][:, None] * true_pos[axis_row][None, :]
        squares = squares + error * error
    return jnp.minimum(jnp.sqrt(squares + eps_square), clamp_length) / clamp_length

def reference(pred_frames, true_frames, pred_atoms, true_atoms, atom_mask, residue_types, swap_flags):
    rot_pred, rot_true, offset, exists = frame_terms(pred_frames, true_frames, residue_types, swap_flags)
    true_resolved, weight = atom_terms(true_atoms, atom_mask, residue_types, swap_flags)
    frames_total = exists.shape[0]
    block_rows = math.gcd(frames_total, 256)
    count_blocks = frames_total // block_rows

    def split_blocks(stacked):
        return stacked.reshape(stacked.shape[0], count_blocks, block_rows).transpose(1, 0, 2)
    blocks = (split_blocks(rot_pred), split_blocks(rot_true), split_blocks(offset), exists.reshape(count_blocks, block_rows))

    def scan_step(atom_sum, pieces):
        clamped = clamped_errors((pieces[0], pieces[1], pieces[2]), (pred_atoms, true_resolved))
        frame_sum = pieces[3] * lax.optimization_barrier(jnp.sum(clamped * weight[None, :], axis=1))
        atom_sum = atom_sum + lax.optimization_barrier(jnp.sum(clamped * pieces[3][:, None], axis=0))
        return (atom_sum, frame_sum)
    atom_sum, frame_sums = lax.scan(scan_step, jnp.zeros((pred_atoms.shape[1],), jnp.float32), blocks)
    frame_sum = frame_sums.reshape(frames_total)
    frame_count = jnp.sum(exists)
    atom_count = jnp.sum(weight)
    frame_loss = frame_sum / atom_count
    atom_loss = weight * atom_sum / frame_count
    total_loss = (jnp.sum(frame_sum) / (frame_count * atom_count)).reshape(1)
    return (frame_loss, atom_loss, total_loss)
```

```python
import functools

import jax
import jax.numpy as jnp
import numpy as np
from jax import lax
from jax.experimental import pallas as pl
from jax.experimental.pallas import tpu as pltpu
from jax.sharding import PartitionSpec as P

eps_square = 0.0001
clamp_length = 10.0

ATOM_COUNTS = (5, 11, 8, 8, 6, 9, 9, 4, 10, 8, 8, 9, 8, 11, 7, 6, 7, 14, 12, 7)
CHI_COUNTS = (0, 4, 2, 2, 1, 3, 3, 0, 2, 2, 2, 4, 3, 2, 2, 1, 1, 2, 2, 1)
FRAME_SLOTS = 8
ATOM_SLOTS = 14
WEIGHT_ROW = 6
FRAME_ROWS = 32
EXISTS_ROW = 24
VMEM = pl.BlockSpec(memory_space=pltpu.VMEM)
SMEM = pl.BlockSpec(memory_space=pltpu.SMEM)
PARAMS = pltpu.CompilerParams(vmem_limit_bytes=8 << 20)


def spread_residues(scalars, positions, width):
    value = jnp.full(positions.shape, scalars[0], jnp.int32)
    first = jnp.zeros(positions.shape, jnp.int32)
    for residue in range(1, len(scalars)):
        here = positions >= residue * width
        value = jnp.where(here, scalars[residue], value)
        first = jnp.where(here, residue * width, first)
    return value, positions - first


def table_lookup(types, table):
    value = jnp.full(types.shape, table[0], jnp.int32)
    for kind in range(1, len(table)):
        if table[kind] != table[0]:
            value = jnp.where(types == kind, table[kind], value)
    return value


def prep_kernel(types_ref, flags_ref, pf_ref, tf_ref, pa_ref, ta_ref, mask_ref, atoms_ref, frames_ref, pad_ref):
    residues = types_ref.shape[0]
    copies, _, lanes = atoms_ref.shape
    frames = pf_ref.shape[1]
    own_atoms = pa_ref.shape[1]
    codes = [types_ref[r] + 32 * flags_ref[r] for r in range(residues)]

    place = lax.broadcasted_iota(jnp.int32, (1, frames), 1)
    code, slot = spread_residues(codes, place, FRAME_SLOTS)
    types = code & 31
    swapped = code >= 32
    chi = table_lookup(types, CHI_COUNTS)
    exists = (slot == 0) | (slot == 3) | ((slot >= 4) & (slot - 3 <= chi))
    half_turn = ((types == 3) | (types == 13) | (types == 18)) & (slot == 5)
    half_turn = swapped & (half_turn | ((types == 6) & (slot == 6)))
    sign = jnp.where(half_turn, -1.0, 1.0)
    rot_pred = [[pf_ref[pl.ds(3 * a + c, 1), :] for c in range(3)] for a in range(3)]
    rot_true = [[tf_ref[pl.ds(3 * a + c, 1), :] for c in range(3)] for a in range(3)]
    rot_true = [[row[0], row[1] * sign, row[2] * sign] for row in rot_true]
    zero = jnp.zeros((1, frames), jnp.float32)
    one = jnp.ones((1, frames), jnp.float32)
    rows = []
    for a in range(3):
        rel = []
        for b in range(3):
            rel.append(
                rot_pred[a][0] * rot_true[b][0]
                + rot_pred[a][1] * rot_true[b][1]
                + rot_pred[a][2] * rot_true[b][2]
            )
        shift = rel[0] * tf_ref[9:10, :] + rel[1] * tf_ref[10:11, :] + rel[2] * tf_ref[11:12, :]
        shift = shift - pf_ref[pl.ds(9 + a, 1), :]
        rows += [one if a == k else zero for k in range(3)]
        rows += [-rel[0], -rel[1], -rel[2], zero, shift]
    for index, row in enumerate(rows):
        frames_ref[pl.ds(index, 1), :] = row
    frames_ref[pl.ds(EXISTS_ROW, 8), :] = jnp.zeros((8, frames), jnp.float32)
    frames_ref[pl.ds(EXISTS_ROW, 1), :] = jnp.where(exists, 1.0, 0.0)

    pad_ref[...] = jnp.zeros(pad_ref.shape, jnp.float32)
    pad_ref[0:3, 0:own_atoms] = pa_ref[...]
    pad_ref[3:6, 0:own_atoms] = ta_ref[...]
    pad_ref[6:7, 0:own_atoms] = mask_ref[...].astype(jnp.float32)
    block = pad_ref[...]
    place = lax.broadcasted_iota(jnp.int32, (1, lanes), 1)
    code, slot = spread_residues(codes, place, ATOM_SLOTS)
    types = code & 31
    swapped = code >= 32
    twice = (types == 13) | (types == 18)

    def opens_pair(s):
        pair = ((s == 6) & ((types == 3) | twice)) | ((s == 7) & (types == 6)) | ((s == 8) & twice)
        return swapped & pair

    after = jnp.where(opens_pair(slot), 1, 0)
    before = jnp.where(opens_pair(slot - 1), 1, 0)
    row = lax.broadcasted_iota(jnp.int32, (8, lanes), 0)
    renamed = jnp.where(
        jnp.broadcast_to(after, (8, lanes)) == 1,
        pltpu.roll(block, lanes - 1, 1),
        jnp.where(jnp.broadcast_to(before, (8, lanes)) == 1, pltpu.roll(block, 1, 1), block),
    )
    block = jnp.where(row < 3, block, renamed)
    real = (slot < table_lookup(types, ATOM_COUNTS)) & (place < own_atoms)
    real = jnp.broadcast_to(jnp.where(real, 1, 0), (8, lanes)) == 1
    block = jnp.where((row == WEIGHT_ROW) & ~real, 0.0, block)
    block = jnp.where(row == 7, 1.0, block)
    for copy in range(copies):
        atoms_ref[copy] = block


def split_rows(x):
    high = x.astype(jnp.bfloat16).astype(jnp.float32)
    rest = x - high
    middle = rest.astype(jnp.bfloat16).astype(jnp.float32)
    return high, middle, rest - middle


def pair_kernel(axes, *refs):
    gx, gy = axes
    atoms_ref = refs[0]
    frame_refs = refs[1 : 1 + gy]
    out_ref = refs[1 + gy]
    lhs_ref, exist_ref, row_ref = refs[2 + gy :]
    frames = frame_refs[0].shape[1]
    lanes = atoms_ref.shape[2]
    chunk = 64
    my_gx = lax.axis_index("gx")
    my_gy = lax.axis_index("gy")

    for block, ref in enumerate(frame_refs):
        for c in range(3):
            high, middle, low = split_rows(ref[pl.ds(8 * c, 8), :])
            zeros = jnp.zeros((frames - 48, frames), jnp.float32)
            stacked = jnp.concatenate([high, middle, low, high, middle, high, zeros], axis=0)
            lhs_ref[c, pl.ds(block * frames, frames), :] = stacked.T.astype(jnp.bfloat16)
        wide = jnp.broadcast_to(ref[pl.ds(EXISTS_ROW, 1), :] * clamp_length, (frames, frames))
        exist_ref[pl.ds(block * frames, frames), :] = wide.T
    row_ref[...] = jnp.zeros(row_ref.shape, jnp.float32)
    out_ref[...] = jnp.zeros(out_ref.shape, jnp.float32)

    def one_source(source, carry):
        block = atoms_ref[source]
        high, middle, low = split_rows(block)
        rhs = jnp.concatenate([high, high, high, middle, middle, low], axis=0).astype(jnp.bfloat16)
        cap = block[WEIGHT_ROW : WEIGHT_ROW + 1] * clamp_length
        column = jnp.zeros((8, lanes), jnp.float32)
        for start in range(0, gy * frames, chunk):
            square = eps_square
            for c in range(3):
                w = jnp.dot(
                    lhs_ref[c, pl.ds(start, chunk), pl.ds(0, 48)], rhs, preferred_element_type=jnp.float32
                )
                square = square + w * w
            limit = exist_ref[pl.ds(start, chunk), :]
            distance = square * lax.rsqrt(square)
            distance = jnp.minimum(jnp.minimum(distance, cap), jnp.concatenate([limit] * (lanes // 128), axis=1))
            total = row_ref[pl.ds(start, chunk), :]
            for lane in range(0, lanes, 128):
                total = total + distance[:, lane : lane + 128]
            row_ref[pl.ds(start, chunk), :] = total
            column = column + jnp.sum(distance.reshape(chunk // 8, 8, lanes), axis=0)
        sums = jnp.sum(column, axis=0, keepdims=True)
        slot = source * gy + my_gy
        for lane in range(0, lanes, 128):
            out_ref[slot, pl.ds(lane // 128, 1), :] = sums[:, lane : lane + 128]
        return carry

    lax.fori_loop(0, gx, one_source, 0)

    loss = jnp.zeros((1, 128), jnp.float32)
    for block in range(gy):
        sums = jnp.sum(row_ref[pl.ds(block * frames, frames), :].T, axis=0, keepdims=True)
        owner = lax.rem(my_gy + block, gy)
        out_ref[my_gx * gy + owner, pl.ds(lanes // 128, 1), :] = sums
        loss = loss + sums
    lane = lax.broadcasted_iota(jnp.int32, (1, 128), 1)
    loss = jnp.sum(loss, axis=1, keepdims=True)
    frame_count = jnp.sum(frame_refs[0][pl.ds(EXISTS_ROW, 1), :], axis=1, keepdims=True)
    atom_count = jnp.sum(atoms_ref[my_gx][WEIGHT_ROW : WEIGHT_ROW + 1], axis=1, keepdims=True)
    scalars = jnp.where(lane == 0, loss, jnp.where(lane == 1, frame_count, atom_count))
    for slot in range(gx * gy):
        out_ref[slot, pl.ds(lanes // 128 + 1, 1), :] = scalars


def finish_kernel(parts_ref, frame_ref, atom_ref, total_ref):
    sums = parts_ref[0]
    for slot in range(1, parts_ref.shape[0]):
        sums = sums + parts_ref[slot]
    atom_rows = sums.shape[0] - 2
    scalars = sums[atom_rows + 1 : atom_rows + 2]
    loss = scalars[:, 0:1]
    frame_count = scalars[:, 1:2]
    atom_count = scalars[:, 2:3]
    scale = 1.0 / clamp_length
    frame_ref[...] = sums[atom_rows : atom_rows + 1] * scale / atom_count
    atoms = jnp.concatenate([sums[i : i + 1] for i in range(atom_rows)], axis=1) * scale / frame_count
    atom_ref[...] = atoms[:, : atom_ref.shape[1]]
    total_ref[...] = loss * scale / (frame_count * atom_count)


def shards(pred_frames, true_frames, pred_atoms, true_atoms, atom_mask, residue_types, swap_flags):
    gx = lax.axis_size("gx")
    gy = lax.axis_size("gy")
    frames = pred_frames.shape[1]
    own_atoms = pred_atoms.shape[1]
    lanes = -(-own_atoms // 128) * 128
    rows = lanes // 128 + 2
    f32 = jnp.float32
    atoms, own_frames = pl.pallas_call(
        prep_kernel,
        out_shape=(
            jax.ShapeDtypeStruct((gx, 8, lanes), f32),
            jax.ShapeDtypeStruct((FRAME_ROWS, frames), f32),
        ),
        in_specs=[SMEM, SMEM, VMEM, VMEM, VMEM, VMEM, VMEM],
        out_specs=(VMEM, VMEM),
        scratch_shapes=[pltpu.VMEM((8, lanes), f32)],
        compiler_params=PARAMS,
        name="prep",
    )(residue_types, swap_flags, pred_frames, true_frames, pred_atoms, true_atoms, atom_mask.reshape(1, own_atoms))
    frame_blocks = [own_frames]
    for step in range(1, gy):
        pairs = [((i + step) % gy, i) for i in range(gy)]
        frame_blocks.append(lax.ppermute(own_frames, "gy", pairs))
    atoms = lax.all_to_all(atoms, "gx", 0, 0, tiled=True)
    parts = pl.pallas_call(
        functools.partial(pair_kernel, (gx, gy)),
        out_shape=jax.ShapeDtypeStruct((gx * gy, rows, 128), f32),
        in_specs=[VMEM] * (1 + gy),
        out_specs=VMEM,
        scratch_shapes=[
            pltpu.VMEM((3, gy * frames, 128), jnp.bfloat16),
            pltpu.VMEM((gy * frames, 128), f32),
            pltpu.VMEM((gy * frames, 128), f32),
        ],
        compiler_params=PARAMS,
        name="pairs",
    )(atoms, *frame_blocks)
    parts = lax.all_to_all(parts, ("gx", "gy"), 0, 0, tiled=True)
    frame_loss, atom_loss, total_loss = pl.pallas_call(
        finish_kernel,
        out_shape=(
            jax.ShapeDtypeStruct((1, frames), f32),
            jax.ShapeDtypeStruct((1, own_atoms), f32),
            jax.ShapeDtypeStruct((1, 1), f32),
        ),
        in_specs=[VMEM],
        out_specs=(VMEM, VMEM, VMEM),
        compiler_params=PARAMS,
        name="finish",
    )(parts)
    return (frame_loss.reshape(frames), atom_loss.reshape(own_atoms), total_loss.reshape(1))


def solution(mesh):
    both = P(None, ("sa", "gx", "gy"))
    flat = P(("sa", "gx", "gy"))
    return jax.shard_map(
        shards,
        mesh=mesh,
        in_specs=(both, both, both, both, flat, flat, flat),
        out_specs=(flat, flat, P("sa")),
        check_vma=False,
    )
```

```python
import functools

import jax
import jax.numpy as jnp
from jax import lax
from jax.experimental import pallas as pl
from jax.experimental.pallas import tpu as pltpu
from jax.sharding import PartitionSpec as P

eps_square = 0.0001
clamp_length = 10.0

ATOM_COUNTS = (5, 11, 8, 8, 6, 9, 9, 4, 10, 8, 8, 9, 8, 11, 7, 6, 7, 14, 12, 7)
CHI_COUNTS = (0, 4, 2, 2, 1, 3, 3, 0, 2, 2, 2, 4, 3, 2, 2, 1, 1, 2, 2, 1)
FRAME_SLOTS = 8
ATOM_SLOTS = 14
WEIGHT_ROW = 6
FRAME_ROWS = 32
EXISTS_ROW = 24
VMEM = pl.BlockSpec(memory_space=pltpu.VMEM)
HBM = pl.BlockSpec(memory_space=pltpu.HBM)
PARAMS = pltpu.CompilerParams(vmem_limit_bytes=8 << 20)


def spread_residues(scalars, positions, width):
    value = jnp.full(positions.shape, scalars[0], jnp.int32)
    first = jnp.zeros(positions.shape, jnp.int32)
    for residue in range(1, len(scalars)):
        here = positions >= residue * width
        value = jnp.where(here, scalars[residue], value)
        first = jnp.where(here, residue * width, first)
    return value, positions - first


def table_lookup(types, table):
    value = jnp.full(types.shape, table[0], jnp.int32)
    for kind in range(1, len(table)):
        if table[kind] != table[0]:
            value = jnp.where(types == kind, table[kind], value)
    return value


def prep_kernel(*refs):
    inputs, (atoms_ref, frames_ref), scratch = refs[:7], refs[7:9], refs[9:]
    (types_ref, flags_ref, pf_ref, tf_ref, pa_ref, ta_ref, mask_ref, pad_ref, sems) = scratch
    fetches = [pltpu.make_async_copy(src, dst, sems.at[i]) for i, (src, dst) in enumerate(zip(inputs, scratch))]
    for fetch in fetches:
        fetch.start()
    for fetch in fetches:
        fetch.wait()
    residues = types_ref.shape[0]
    copies, _, lanes = atoms_ref.shape
    frames = pf_ref.shape[1]
    own_atoms = pa_ref.shape[1]
    codes = [types_ref[r] + 32 * flags_ref[r] for r in range(residues)]

    place = lax.broadcasted_iota(jnp.int32, (1, frames), 1)
    code, slot = spread_residues(codes, place, FRAME_SLOTS)
    types = code & 31
    swapped = code >= 32
    chi = table_lookup(types, CHI_COUNTS)
    exists = (slot == 0) | (slot == 3) | ((slot >= 4) & (slot - 3 <= chi))
    half_turn = ((types == 3) | (types == 13) | (types == 18)) & (slot == 5)
    half_turn = swapped & (half_turn | ((types == 6) & (slot == 6)))
    sign = jnp.where(half_turn, -1.0, 1.0)
    rot_pred = [[pf_ref[pl.ds(3 * a + c, 1), :] for c in range(3)] for a in range(3)]
    rot_true = [[tf_ref[pl.ds(3 * a + c, 1), :] for c in range(3)] for a in range(3)]
    rot_true = [[row[0], row[1] * sign, row[2] * sign] for row in rot_true]
    zero = jnp.zeros((1, frames), jnp.float32)
    one = jnp.ones((1, frames), jnp.float32)
    rows = []
    for a in range(3):
        rel = []
        for b in range(3):
            rel.append(
                rot_pred[a][0] * rot_true[b][0]
                + rot_pred[a][1] * rot_true[b][1]
                + rot_pred[a][2] * rot_true[b][2]
            )
        shift = rel[0] * tf_ref[9:10, :] + rel[1] * tf_ref[10:11, :] + rel[2] * tf_ref[11:12, :]
        shift = shift - pf_ref[pl.ds(9 + a, 1), :]
        rows += [one if a == k else zero for k in range(3)]
        rows += [-rel[0], -rel[1], -rel[2], zero, shift]
    for index, row in enumerate(rows):
        frames_ref[pl.ds(index, 1), :] = row
    frames_ref[pl.ds(EXISTS_ROW, 8), :] = jnp.zeros((8, frames), jnp.float32)
    frames_ref[pl.ds(EXISTS_ROW, 1), :] = jnp.where(exists, 1.0, 0.0)

    pad_ref[...] = jnp.zeros(pad_ref.shape, jnp.float32)
    pad_ref[0:3, 0:own_atoms] = pa_ref[...]
    pad_ref[3:6, 0:own_atoms] = ta_ref[...]
    pad_ref[6:7, 0:own_atoms] = mask_ref[...].astype(jnp.float32)
    block = pad_ref[...]
    place = lax.broadcasted_iota(jnp.int32, (1, lanes), 1)
    code, slot = spread_residues(codes, place, ATOM_SLOTS)
    types = code & 31
    swapped = code >= 32
    twice = (types == 13) | (types == 18)

    def opens_pair(s):
        pair = ((s == 6) & ((types == 3) | twice)) | ((s == 7) & (types == 6)) | ((s == 8) & twice)
        return swapped & pair

    after = jnp.where(opens_pair(slot), 1, 0)
    before = jnp.where(opens_pair(slot - 1), 1, 0)
    row = lax.broadcasted_iota(jnp.int32, (8, lanes), 0)
    renamed = jnp.where(
        jnp.broadcast_to(after, (8, lanes)) == 1,
        pltpu.roll(block, lanes - 1, 1),
        jnp.where(jnp.broadcast_to(before, (8, lanes)) == 1, pltpu.roll(block, 1, 1), block),
    )
    block = jnp.where(row < 3, block, renamed)
    real = (slot < table_lookup(types, ATOM_COUNTS)) & (place < own_atoms)
    real = jnp.broadcast_to(jnp.where(real, 1, 0), (8, lanes)) == 1
    block = jnp.where((row == WEIGHT_ROW) & ~real, 0.0, block)
    block = jnp.where(row == 7, 1.0, block)
    for copy in range(copies):
        atoms_ref[copy] = block


def split_rows(x):
    high = x.astype(jnp.bfloat16).astype(jnp.float32)
    rest = x - high
    middle = rest.astype(jnp.bfloat16).astype(jnp.float32)
    return high, middle, rest - middle


def pair_kernel(axes, *refs):
    gx, gy = axes
    atoms_ref = refs[0]
    frame_refs = refs[1 : 1 + gy]
    out_ref = refs[1 + gy]
    lhs_ref, exist_ref, row_ref = refs[2 + gy :]
    frames = frame_refs[0].shape[1]
    lanes = atoms_ref.shape[2]
    chunk = 64
    my_gx = lax.axis_index("gx")
    my_gy = lax.axis_index("gy")

    for block, ref in enumerate(frame_refs):
        for c in range(3):
            high, middle, low = split_rows(ref[pl.ds(8 * c, 8), :])
            zeros = jnp.zeros((frames - 48, frames), jnp.float32)
            stacked = jnp.concatenate([high, middle, low, high, middle, high, zeros], axis=0)
            lhs_ref[c, pl.ds(block * frames, frames), :] = stacked.T.astype(jnp.bfloat16)
        wide = jnp.broadcast_to(ref[pl.ds(EXISTS_ROW, 1), :] * clamp_length, (frames, frames))
        exist_ref[pl.ds(block * frames, frames), :] = wide.T
    row_ref[...] = jnp.zeros(row_ref.shape, jnp.float32)
    out_ref[...] = jnp.zeros(out_ref.shape, jnp.float32)

    def one_source(source, carry):
        block = atoms_ref[source]
        high, middle, low = split_rows(block)
        rhs = jnp.concatenate([high, high, high, middle, middle, low], axis=0).astype(jnp.bfloat16)
        cap = block[WEIGHT_ROW : WEIGHT_ROW + 1] * clamp_length
        column = jnp.zeros((8, lanes), jnp.float32)
        for start in range(0, gy * frames, chunk):
            square = eps_square
            for c in range(3):
                w = jnp.dot(
                    lhs_ref[c, pl.ds(start, chunk), pl.ds(0, 48)], rhs, preferred_element_type=jnp.float32
                )
                square = square + w * w
            limit = exist_ref[pl.ds(start, chunk), :]
            distance = square * lax.rsqrt(square)
            distance = jnp.minimum(jnp.minimum(distance, cap), jnp.concatenate([limit] * (lanes // 128), axis=1))
            total = row_ref[pl.ds(start, chunk), :]
            for lane in range(0, lanes, 128):
                total = total + distance[:, lane : lane + 128]
            row_ref[pl.ds(start, chunk), :] = total
            column = column + jnp.sum(distance.reshape(chunk // 8, 8, lanes), axis=0)
        sums = jnp.sum(column, axis=0, keepdims=True)
        slot = source * gy + my_gy
        for lane in range(0, lanes, 128):
            out_ref[slot, pl.ds(lane // 128, 1), :] = sums[:, lane : lane + 128]
        return carry

    lax.fori_loop(0, gx, one_source, 0)

    loss = jnp.zeros((1, 128), jnp.float32)
    for block in range(gy):
        sums = jnp.sum(row_ref[pl.ds(block * frames, frames), :].T, axis=0, keepdims=True)
        owner = lax.rem(my_gy + block, gy)
        out_ref[my_gx * gy + owner, pl.ds(lanes // 128, 1), :] = sums
        loss = loss + sums
    lane = lax.broadcasted_iota(jnp.int32, (1, 128), 1)
    loss = jnp.sum(loss, axis=1, keepdims=True)
    frame_count = jnp.sum(frame_refs[0][pl.ds(EXISTS_ROW, 1), :], axis=1, keepdims=True)
    atom_count = jnp.sum(atoms_ref[my_gx][WEIGHT_ROW : WEIGHT_ROW + 1], axis=1, keepdims=True)
    scalars = jnp.where(lane == 0, loss, jnp.where(lane == 1, frame_count, atom_count))
    for slot in range(gx * gy):
        out_ref[slot, pl.ds(lanes // 128 + 1, 1), :] = scalars


def finish_kernel(parts_ref, frame_ref, atom_ref, total_ref):
    sums = parts_ref[0]
    for slot in range(1, parts_ref.shape[0]):
        sums = sums + parts_ref[slot]
    atom_rows = sums.shape[0] - 2
    scalars = sums[atom_rows + 1 : atom_rows + 2]
    loss = scalars[:, 0:1]
    frame_count = scalars[:, 1:2]
    atom_count = scalars[:, 2:3]
    scale = 1.0 / clamp_length
    frame_ref[...] = sums[atom_rows : atom_rows + 1] * scale / atom_count
    atoms = jnp.concatenate([sums[i : i + 1] for i in range(atom_rows)], axis=1) * scale / frame_count
    atom_ref[...] = atoms[:, : atom_ref.shape[1]]
    total_ref[...] = loss * scale / (frame_count * atom_count)


def shards(pred_frames, true_frames, pred_atoms, true_atoms, atom_mask, residue_types, swap_flags):
    gx = lax.axis_size("gx")
    gy = lax.axis_size("gy")
    frames = pred_frames.shape[1]
    own_atoms = pred_atoms.shape[1]
    lanes = -(-own_atoms // 128) * 128
    rows = lanes // 128 + 2
    f32 = jnp.float32
    inputs = (residue_types, swap_flags, pred_frames, true_frames, pred_atoms, true_atoms)
    inputs += (atom_mask.reshape(1, own_atoms),)
    atoms, own_frames = pl.pallas_call(
        prep_kernel,
        out_shape=(
            jax.ShapeDtypeStruct((gx, 8, lanes), f32),
            jax.ShapeDtypeStruct((FRAME_ROWS, frames), f32),
        ),
        in_specs=[HBM] * 7,
        out_specs=(VMEM, VMEM),
        scratch_shapes=[
            pltpu.SMEM(residue_types.shape, jnp.int32),
            pltpu.SMEM(swap_flags.shape, jnp.int32),
            pltpu.VMEM(pred_frames.shape, f32),
            pltpu.VMEM(true_frames.shape, f32),
            pltpu.VMEM(pred_atoms.shape, f32),
            pltpu.VMEM(true_atoms.shape, f32),
            pltpu.VMEM((1, own_atoms), jnp.int32),
            pltpu.VMEM((8, lanes), f32),
            pltpu.SemaphoreType.DMA((7,)),
        ],
        compiler_params=PARAMS,
        name="prep",
    )(*[pltpu.with_memory_space_constraint(x, pltpu.HBM) for x in inputs])
    frame_blocks = [own_frames]
    for step in range(1, gy):
        pairs = [((i + step) % gy, i) for i in range(gy)]
        frame_blocks.append(lax.ppermute(own_frames, "gy", pairs))
    atoms = lax.all_to_all(atoms, "gx", 0, 0, tiled=True)
    parts = pl.pallas_call(
        functools.partial(pair_kernel, (gx, gy)),
        out_shape=jax.ShapeDtypeStruct((gx * gy, rows, 128), f32),
        in_specs=[VMEM] * (1 + gy),
        out_specs=VMEM,
        scratch_shapes=[
            pltpu.VMEM((3, gy * frames, 128), jnp.bfloat16),
            pltpu.VMEM((gy * frames, 128), f32),
            pltpu.VMEM((gy * frames, 128), f32),
        ],
        compiler_params=PARAMS,
        name="pairs",
    )(atoms, *frame_blocks)
    parts = lax.all_to_all(parts, ("gx", "gy"), 0, 0, tiled=True)
    frame_loss, atom_loss, total_loss = pl.pallas_call(
        finish_kernel,
        out_shape=(
            jax.ShapeDtypeStruct((1, frames), f32),
            jax.ShapeDtypeStruct((1, own_atoms), f32),
            jax.ShapeDtypeStruct((1, 1), f32),
        ),
        in_specs=[VMEM],
        out_specs=(VMEM, VMEM, VMEM),
        compiler_params=PARAMS,
        name="finish",
    )(parts)
    return (frame_loss.reshape(frames), atom_loss.reshape(own_atoms), total_loss.reshape(1))


def solution(mesh):
    both = P(None, ("sa", "gx", "gy"))
    flat = P(("sa", "gx", "gy"))
    return jax.shard_map(
        shards,
        mesh=mesh,
        in_specs=(both, both, both, both, flat, flat, flat),
        out_specs=(flat, flat, P("sa")),
        check_vma=False,
    )
```

```python
import functools

import jax
import jax.numpy as jnp
from jax import lax
from jax.experimental import pallas as pl
from jax.experimental.pallas import tpu as pltpu
from jax.sharding import PartitionSpec as P

eps_square = 0.0001
clamp_length = 10.0

ATOM_COUNTS = (5, 11, 8, 8, 6, 9, 9, 4, 10, 8, 8, 9, 8, 11, 7, 6, 7, 14, 12, 7)
CHI_COUNTS = (0, 4, 2, 2, 1, 3, 3, 0, 2, 2, 2, 4, 3, 2, 2, 1, 1, 2, 2, 1)
FRAME_SLOTS = 8
USED_SLOTS = 6
ATOM_SLOTS = 14
ROW_CHUNK = 384
TILE = 256
TILE_GROUP = 2
VMEM = pl.BlockSpec(memory_space=pltpu.VMEM)
HBM = pl.BlockSpec(memory_space=pltpu.HBM)


def spread_residues(scalars, positions, width):
    value = jnp.full(positions.shape, scalars[0], jnp.int32)
    first = jnp.zeros(positions.shape, jnp.int32)
    for residue in range(1, len(scalars)):
        here = positions >= residue * width
        value = jnp.where(here, scalars[residue], value)
        first = jnp.where(here, residue * width, first)
    return value, positions - first


def table_lookup(types, table):
    value = jnp.full(types.shape, table[0], jnp.int32)
    for kind in range(1, len(table)):
        if table[kind] != table[0]:
            value = jnp.where(types == kind, table[kind], value)
    return value


def split_rows(x):
    high = x.astype(jnp.bfloat16).astype(jnp.float32)
    rest = x - high
    middle = rest.astype(jnp.bfloat16).astype(jnp.float32)
    return high, middle, rest - middle


def one_hot(rank):
    size = rank.shape[1]
    place = lax.broadcasted_iota(jnp.int32, (size, size), 0)
    return jnp.where(place == rank, 1.0, 0.0).astype(jnp.bfloat16)


def exact_dot(x, selection, contract):
    rows = x.shape[0]
    parts = jnp.concatenate(split_rows(x), axis=0).astype(jnp.bfloat16)
    out = lax.dot_general(parts, selection, (((1,), (contract,)), ((), ())), preferred_element_type=jnp.float32)
    return out[:rows] + out[rows : 2 * rows] + out[2 * rows :]


def prep_kernel(*refs):
    inputs, (block_ref, rank_ref), scratch = refs[:7], refs[7:9], refs[9:]
    (types_ref, flags_ref, pf_ref, tf_ref, pa_ref, ta_ref, mask_ref, pad_ref, sems) = scratch
    fetches = [pltpu.make_async_copy(src, dst, sems.at[i]) for i, (src, dst) in enumerate(zip(inputs, scratch))]
    for fetch in fetches:
        fetch.start()
    residues = types_ref.shape[0]
    frames = pf_ref.shape[1]
    own_atoms = pa_ref.shape[1]
    lanes = pad_ref.shape[1]
    pad_ref[...] = jnp.zeros(pad_ref.shape, jnp.float32)
    for fetch in fetches:
        fetch.wait()
    codes = [types_ref[r] + 32 * flags_ref[r] for r in range(residues)]

    pad_ref[0:3, 0:own_atoms] = pa_ref[...]
    pad_ref[3:6, 0:own_atoms] = ta_ref[...]
    pad_ref[6:7, 0:own_atoms] = mask_ref[...].astype(jnp.float32)
    atoms = pad_ref[...]
    place = lax.broadcasted_iota(jnp.int32, (1, lanes), 1)
    code, slot = spread_residues(codes, place, ATOM_SLOTS)
    types = code & 31
    swapped = code >= 32
    twice = (types == 13) | (types == 18)

    def opens_pair(s):
        pair = ((s == 6) & ((types == 3) | twice)) | ((s == 7) & (types == 6)) | ((s == 8) & twice)
        return swapped & pair

    after = jnp.where(opens_pair(slot), 1, 0)
    before = jnp.where(opens_pair(slot - 1), 1, 0)
    row = lax.broadcasted_iota(jnp.int32, (8, lanes), 0)
    renamed = jnp.where(
        jnp.broadcast_to(after, (8, lanes)) == 1,
        pltpu.roll(atoms, lanes - 1, 1),
        jnp.where(jnp.broadcast_to(before, (8, lanes)) == 1, pltpu.roll(atoms, 1, 1), atoms),
    )
    atoms = jnp.where(row < 3, atoms, renamed)
    real = (slot < table_lookup(types, ATOM_COUNTS)) & (place < own_atoms)
    real = jnp.broadcast_to(jnp.where(real, 1, 0), (8, lanes)) == 1
    atoms = jnp.where((row == 6) & ~real, 0.0, atoms)
    weight = atoms[6:7]
    earlier = lax.broadcasted_iota(jnp.int32, (lanes, lanes), 0) < lax.broadcasted_iota(jnp.int32, (lanes, lanes), 1)
    earlier = jnp.where(earlier, 1.0, 0.0).astype(jnp.bfloat16)
    rank = jnp.dot(
        jnp.broadcast_to(weight, (16, lanes)).astype(jnp.bfloat16), earlier, preferred_element_type=jnp.float32
    )[0:1]
    atom_rank = jnp.where(weight > 0.5, rank, -1.0).astype(jnp.int32)
    atom_count = jnp.sum(weight, axis=1, keepdims=True)

    place = lax.broadcasted_iota(jnp.int32, (1, frames), 1)
    code, slot = spread_residues(codes, place, FRAME_SLOTS)
    types = code & 31
    swapped = code >= 32
    chi = table_lookup(types, CHI_COUNTS)
    exists = (slot == 0) | (slot == 3) | ((slot >= 4) & (slot - 3 <= chi))
    exists = jnp.where(exists, 1.0, 0.0)
    half_turn = ((types == 3) | (types == 13) | (types == 18)) & (slot == 5)
    half_turn = swapped & (half_turn | ((types == 6) & (slot == 6)))
    sign = jnp.where(half_turn, -1.0, 1.0)
    rot_pred = [[pf_ref[pl.ds(3 * a + c, 1), :] for c in range(3)] for a in range(3)]
    rot_true = [[tf_ref[pl.ds(3 * a + c, 1), :] for c in range(3)] for a in range(3)]
    rot_true = [[r[0], r[1] * sign, r[2] * sign] for r in rot_true]
    rows = []
    shifts = []
    for a in range(3):
        rel = [
            rot_pred[a][0] * rot_true[b][0] + rot_pred[a][1] * rot_true[b][1] + rot_pred[a][2] * rot_true[b][2]
            for b in range(3)
        ]
        shift = rel[0] * tf_ref[9:10, :] + rel[1] * tf_ref[10:11, :] + rel[2] * tf_ref[11:12, :]
        shifts.append(shift - pf_ref[pl.ds(9 + a, 1), :])
        if a < 2:
            rows += [-rel[0], -rel[1], -rel[2]]
    rows += shifts + [exists]
    rows += [jnp.zeros((16 - len(rows), frames), jnp.float32)]
    rank = jnp.dot(
        jnp.broadcast_to(exists, (16, frames)).astype(jnp.bfloat16),
        earlier[:frames, :frames],
        preferred_element_type=jnp.float32,
    )[0:1]
    frame_rank = jnp.where(exists > 0.5, rank, -1.0).astype(jnp.int32)
    frame_count = jnp.sum(exists, axis=1, keepdims=True)

    atoms = exact_dot(atoms, one_hot(atom_rank), 1)
    packed = exact_dot(jnp.concatenate(rows, axis=0), one_hot(frame_rank), 1)
    first = jnp.where(place == 0, frame_count, jnp.where(place == 1, atom_count, packed[9:10]))
    extra = jnp.concatenate([first, packed[8:9]], axis=1)
    atoms = jnp.where(row == 7, jnp.broadcast_to(extra, (8, lanes)), atoms)
    block = jnp.concatenate([atoms, packed[0:8]], axis=1)
    for copy in range(block_ref.shape[0]):
        block_ref[copy] = block
    rank_ref[...] = jnp.zeros(rank_ref.shape, jnp.int32)
    rank_ref[0:1, :] = atom_rank
    rank_ref[1:2, 0:frames] = frame_rank


def pair_kernel(
    gy_size, blocks_ref, rank_ref, frame_ref, atom_ref, total_ref, src_ref, rhs_ref, lhs_ref, row_ref, col_ref
):
    devices = blocks_ref.shape[0]
    frames = frame_ref.shape[1]
    own_atoms = atom_ref.shape[1]
    most = frames * USED_SLOTS // FRAME_SLOTS // 16
    row_step = ROW_CHUNK // 16
    per_tile = TILE // 128
    me = lax.axis_index("gx") * gy_size + lax.axis_index("gy")
    lane = lax.broadcasted_iota(jnp.int32, (8, 128), 1)
    sub = lax.broadcasted_iota(jnp.int32, (8, 128), 0)
    src_ref[...] = jnp.zeros(src_ref.shape, jnp.float32)
    col_ref[...] = jnp.zeros(col_ref.shape, jnp.float32)

    def place_block(device, carry):
        atoms_before, rows_before, frame_total, my_atoms, my_rows = carry
        my_atoms = jnp.where(device == me, atoms_before, my_atoms)
        my_rows = jnp.where(device == me, rows_before, my_rows)
        frame_count = jnp.max(blocks_ref[device, 7:8, 0:1]).astype(jnp.int32)
        atom_count = jnp.max(blocks_ref[device, 7:8, 1:2]).astype(jnp.int32)
        tile = atoms_before // 128
        turn = atoms_before % 128
        low = pltpu.roll(blocks_ref[device, :, 0:128], turn, 1)
        high = pltpu.roll(blocks_ref[device, :, 128:256], turn, 1)
        inside = lane >= turn
        src_ref[tile] += jnp.where(inside, low, 0.0)
        src_ref[tile + 1] += jnp.where(inside, high, low)
        src_ref[tile + 2] += jnp.where(inside, 0.0, high)
        part = blocks_ref[device, :, 256:384]
        exists = blocks_ref[device, 7:8, 0:128]
        exists = jnp.where(lane[0:1] < 2, 1.0, exists)
        last = blocks_ref[device, 7:8, 128:256]
        a = [part[k : k + 1] for k in range(3)]
        b = [part[3 + k : 4 + k] for k in range(3)]
        cross = [a[2] * b[1] - a[1] * b[2], a[0] * b[2] - a[2] * b[0], a[1] * b[0] - a[0] * b[1]]
        rotations = (part[0:3], part[3:6], jnp.concatenate(cross, axis=0))
        shifts = (part[6:7], part[7:8], last)
        for c in range(3):
            group = jnp.concatenate([rotations[c], rotations[c], shifts[c], exists], axis=0)
            high, middle, low = split_rows(group)
            ones = jnp.broadcast_to(exists, (8, 128))
            stack = [
                jnp.where((sub >= 3) & (sub < 6), middle, high),
                jnp.where(sub < 3, low, jnp.where(sub == 6, middle, high)),
                jnp.where(sub < 3, middle, jnp.where(sub == 6, low, high)),
            ]
            stack = [x if k == c else jnp.where(sub == 7, 0.0, x) for k, x in enumerate(stack)]
            stack.append(jnp.where((sub == c) | (sub == 3 + c), ones, 0.0))
            stack.append(jnp.zeros((96, 128), jnp.float32))
            turned = jnp.concatenate(stack, axis=0).T[: 16 * most]
            lhs_ref[pl.ds(rows_before, most), c] = turned.astype(jnp.bfloat16).reshape(most, 16, 128)
        return (
            atoms_before + atom_count,
            rows_before + (frame_count + 15) // 16,
            frame_total + frame_count,
            my_atoms,
            my_rows,
        )

    group = 16
    while devices % group:
        group //= 2

    def place_group(index, carry):
        for k in range(group):
            carry = place_block(index * group + k, carry)
        return carry

    carry = (0, 0, 0, 0, 0)
    if devices == group:
        carry = place_group(0, carry)
    else:
        carry = lax.fori_loop(0, devices // group, place_group, carry)
    atom_total, row_total, frame_total, my_atoms, my_rows = carry
    lhs_ref[pl.ds(row_total, row_step)] = jnp.zeros((row_step,) + lhs_ref.shape[1:], jnp.bfloat16)
    chunks = (row_total + row_step - 1) // row_step
    behind = pl.multiple_of(chunks * ROW_CHUNK, ROW_CHUNK)
    row_ref[pl.ds(behind, frames), :] = jnp.zeros((frames, 128), jnp.float32)
    width = TILE * TILE_GROUP
    groups = (atom_total + width - 1) // width

    def build_rhs(index, carry):
        for k in range(TILE_GROUP):
            tile = index * TILE_GROUP + k
            x = jnp.concatenate([src_ref[tile * per_tile + m] for m in range(per_tile)], axis=1)
            high, middle, low = split_rows(x)
            one = jnp.ones((1, TILE), jnp.float32)
            nil = jnp.zeros((2, TILE), jnp.float32)
            rows = [high[3:6], high[3:6], one, high[0:1], high[3:6], middle[3:6], one, high[1:2]]
            rows += [middle[3:6], low[3:6], one, high[2:3], middle[0:3], low[0:3], nil]
            rhs_ref[tile] = jnp.concatenate(rows, axis=0).astype(jnp.bfloat16)
        return carry

    lax.fori_loop(0, groups, build_rhs, 0)

    def one_chunk(chunk, carry):
        start = pl.multiple_of(chunk * ROW_CHUNK, ROW_CHUNK)
        row_ref[pl.ds(start, ROW_CHUNK), :] = jnp.zeros((ROW_CHUNK, 128), jnp.float32)

        def one_group(index, carry):
            lhs = lhs_ref[pl.ds(chunk * row_step, row_step)].reshape(3 * ROW_CHUNK, 128)[:, 0:32]
            row_sums = [None] * (ROW_CHUNK // 8)
            for k in range(TILE_GROUP):
                tile = index * TILE_GROUP + k
                w = jnp.dot(lhs, rhs_ref[tile], preferred_element_type=jnp.float32)
                cap = jnp.concatenate([src_ref[tile * per_tile + m, 6:7, :] for m in range(per_tile)], axis=1)
                cap = jnp.broadcast_to(cap * clamp_length, (8, TILE))
                column = None
                for g in range(ROW_CHUNK // 8):
                    base = 48 * (g // 2) + 8 * (g % 2)
                    w0, w1, w2 = (w[base + 16 * c : base + 16 * c + 8] for c in range(3))
                    square = (w0 * w0 + w1 * w1) + (w2 * w2 + eps_square)
                    distance = jnp.minimum(square * lax.rsqrt(square), cap)
                    column = distance if column is None else column + distance
                    for m in range(per_tile):
                        piece = distance[:, 128 * m : 128 * m + 128]
                        row_sums[g] = piece if row_sums[g] is None else row_sums[g] + piece
                for m in range(per_tile):
                    col_ref[tile * per_tile + m] += column[:, 128 * m : 128 * m + 128]
            for g in range(ROW_CHUNK // 8):
                row_ref[pl.ds(start + 8 * g, 8), :] += row_sums[g]
            return carry

        return lax.fori_loop(0, groups, one_group, carry)

    lax.fori_loop(0, chunks, one_chunk, 0)

    idle = (chunks * ROW_CHUNK - frame_total).astype(jnp.float32)
    least = jnp.full((1, 128), eps_square, jnp.float32)
    least = least * lax.rsqrt(least)

    def column_sums(tile):
        cap = src_ref[tile, 6:7, :] * clamp_length
        return jnp.sum(col_ref[tile], axis=0, keepdims=True) - idle * jnp.minimum(least, cap)

    def add_tile(tile, carry):
        sums, floor = carry
        return sums + col_ref[tile], floor + jnp.minimum(least, src_ref[tile, 6:7, :] * clamp_length)

    sums, floor = lax.fori_loop(
        0,
        groups * per_tile * TILE_GROUP,
        add_tile,
        (jnp.zeros((8, 128), jnp.float32), jnp.zeros((1, 128), jnp.float32)),
    )
    loss = jnp.sum(sums, axis=0, keepdims=True) - idle * floor
    loss = jnp.sum(loss, axis=1, keepdims=True)
    atom_number = atom_total.astype(jnp.float32)
    frame_number = frame_total.astype(jnp.float32)
    scale = 1.0 / clamp_length
    total_ref[...] = loss * scale / (frame_number * atom_number)

    tile = my_atoms // 128
    turn = my_atoms % 128
    back = (128 - turn) % 128
    pieces = [pltpu.roll(jnp.broadcast_to(column_sums(tile + k), (8, 128)), back, 1) for k in range(3)]
    keep = lane < 128 - turn
    mine = jnp.concatenate([jnp.where(keep, pieces[k], pieces[k + 1]) for k in range(2)], axis=1)
    mine = exact_dot(mine, one_hot(rank_ref[0:1, :]), 0)[0:1]
    atom_ref[...] = mine[:, :own_atoms] * scale / frame_number

    rows = row_ref[pl.ds(pl.multiple_of(my_rows * 16, 16), frames), :]
    mine = jnp.broadcast_to(jnp.sum(rows.T, axis=0, keepdims=True), (8, frames))
    mine = exact_dot(mine, one_hot(rank_ref[1:2, 0:frames]), 0)[0:1]
    frame_ref[...] = mine * scale / atom_number


def shards(pred_frames, true_frames, pred_atoms, true_atoms, atom_mask, residue_types, swap_flags):
    devices = lax.axis_size("gx") * lax.axis_size("gy")
    frames = pred_frames.shape[1]
    own_atoms = pred_atoms.shape[1]
    lanes = -(-own_atoms // 128) * 128
    f32 = jnp.float32
    inputs = (residue_types, swap_flags, pred_frames, true_frames, pred_atoms, true_atoms)
    inputs += (atom_mask.reshape(1, own_atoms),)
    blocks, ranks = pl.pallas_call(
        prep_kernel,
        out_shape=(
            jax.ShapeDtypeStruct((devices, 8, lanes + frames), f32),
            jax.ShapeDtypeStruct((8, lanes), jnp.int32),
        ),
        in_specs=[HBM] * 7,
        out_specs=(VMEM, VMEM),
        scratch_shapes=[
            pltpu.SMEM(residue_types.shape, jnp.int32),
            pltpu.SMEM(swap_flags.shape, jnp.int32),
            pltpu.VMEM(pred_frames.shape, f32),
            pltpu.VMEM(true_frames.shape, f32),
            pltpu.VMEM(pred_atoms.shape, f32),
            pltpu.VMEM(true_atoms.shape, f32),
            pltpu.VMEM((1, own_atoms), jnp.int32),
            pltpu.VMEM((8, lanes), f32),
            pltpu.SemaphoreType.DMA((7,)),
        ],
        compiler_params=pltpu.CompilerParams(vmem_limit_bytes=8 << 20),
        name="prep",
    )(*[pltpu.with_memory_space_constraint(x, pltpu.HBM) for x in inputs])
    blocks = lax.all_to_all(blocks, ("gx", "gy"), 0, 0, tiled=True)
    width = TILE * TILE_GROUP
    groups = -(-(devices * own_atoms + 256) // width)
    row_groups = devices * (frames * USED_SLOTS // FRAME_SLOTS // 16) + 2 * ROW_CHUNK // 16
    scratch = [
        ((groups * width // 128, 8, 128), f32),
        ((groups * TILE_GROUP, 32, TILE), jnp.bfloat16),
        ((row_groups, 3, 16, 128), jnp.bfloat16),
        ((row_groups * 16, 128), f32),
        ((groups * width // 128, 8, 128), f32),
    ]
    room = sum(jnp.dtype(dtype).itemsize * functools.reduce(lambda a, b: a * b, shape) for shape, dtype in scratch)
    frame_loss, atom_loss, total_loss = pl.pallas_call(
        functools.partial(pair_kernel, lax.axis_size("gy")),
        out_shape=(
            jax.ShapeDtypeStruct((1, frames), f32),
            jax.ShapeDtypeStruct((1, own_atoms), f32),
            jax.ShapeDtypeStruct((1, 1), f32),
        ),
        in_specs=[VMEM, VMEM],
        out_specs=(VMEM, VMEM, VMEM),
        scratch_shapes=[pltpu.VMEM(shape, dtype) for shape, dtype in scratch],
        compiler_params=pltpu.CompilerParams(vmem_limit_bytes=room + (12 << 20)),
        name="pairs",
    )(blocks, ranks)
    return (frame_loss.reshape(frames), atom_loss.reshape(own_atoms), total_loss.reshape(1))


def solution(mesh):
    both = P(None, ("sa", "gx", "gy"))
    flat = P(("sa", "gx", "gy"))
    return jax.shard_map(
        shards,
        mesh=mesh,
        in_specs=(both, both, both, both, flat, flat, flat),
        out_specs=(flat, flat, P("sa")),
        check_vma=False,
    )
```

```python
import functools

import jax
import jax.numpy as jnp
from jax import lax
from jax.experimental import pallas as pl
from jax.experimental.pallas import tpu as pltpu
from jax.sharding import PartitionSpec as P

eps_square = 0.0001
clamp_length = 10.0

ATOM_COUNTS = (5, 11, 8, 8, 6, 9, 9, 4, 10, 8, 8, 9, 8, 11, 7, 6, 7, 14, 12, 7)
CHI_COUNTS = (0, 4, 2, 2, 1, 3, 3, 0, 2, 2, 2, 4, 3, 2, 2, 1, 1, 2, 2, 1)
FRAME_SLOTS = 8
USED_SLOTS = 6
BUILD_GROUP = 4
ATOM_SLOTS = 14
ROW_CHUNK = 352
TILE = 256
TILE_GROUP = 4
VMEM = pl.BlockSpec(memory_space=pltpu.VMEM)
HBM = pl.BlockSpec(memory_space=pltpu.HBM)


def spread_residues(scalars, positions, width):
    value = jnp.full(positions.shape, scalars[0], jnp.int32)
    first = jnp.zeros(positions.shape, jnp.int32)
    for residue in range(1, len(scalars)):
        here = positions >= residue * width
        value = jnp.where(here, scalars[residue], value)
        first = jnp.where(here, residue * width, first)
    return value, positions - first


def table_lookup(types, table):
    value = jnp.full(types.shape, table[0], jnp.int32)
    for kind in range(1, len(table)):
        if table[kind] != table[0]:
            value = jnp.where(types == kind, table[kind], value)
    return value


def split_rows(x):
    high = x.astype(jnp.bfloat16).astype(jnp.float32)
    rest = x - high
    middle = rest.astype(jnp.bfloat16).astype(jnp.float32)
    return high, middle, rest - middle


def one_hot(rank):
    size = rank.shape[1]
    place = lax.broadcasted_iota(jnp.int32, (size, size), 0)
    return jnp.where(place == rank, 1.0, 0.0).astype(jnp.bfloat16)


def exact_dot(x, selection, contract):
    rows = x.shape[0]
    parts = jnp.concatenate(split_rows(x), axis=0).astype(jnp.bfloat16)
    out = lax.dot_general(parts, selection, (((1,), (contract,)), ((), ())), preferred_element_type=jnp.float32)
    return out[:rows] + out[rows : 2 * rows] + out[2 * rows :]


def prep_kernel(*refs):
    inputs, (block_ref, rank_ref), scratch = refs[:7], refs[7:9], refs[9:]
    (types_ref, flags_ref, pf_ref, tf_ref, pa_ref, ta_ref, mask_ref, pad_ref, sems) = scratch
    fetches = [pltpu.make_async_copy(src, dst, sems.at[i]) for i, (src, dst) in enumerate(zip(inputs, scratch))]
    for fetch in fetches:
        fetch.start()
    residues = types_ref.shape[0]
    frames = pf_ref.shape[1]
    own_atoms = pa_ref.shape[1]
    lanes = pad_ref.shape[1]
    pad_ref[...] = jnp.zeros(pad_ref.shape, jnp.float32)
    for fetch in fetches:
        fetch.wait()
    codes = [types_ref[r] + 32 * flags_ref[r] for r in range(residues)]

    pad_ref[0:3, 0:own_atoms] = pa_ref[...]
    pad_ref[3:6, 0:own_atoms] = ta_ref[...]
    pad_ref[6:7, 0:own_atoms] = mask_ref[...].astype(jnp.float32)
    atoms = pad_ref[...]
    place = lax.broadcasted_iota(jnp.int32, (1, lanes), 1)
    code, slot = spread_residues(codes, place, ATOM_SLOTS)
    types = code & 31
    swapped = code >= 32
    twice = (types == 13) | (types == 18)

    def opens_pair(s):
        pair = ((s == 6) & ((types == 3) | twice)) | ((s == 7) & (types == 6)) | ((s == 8) & twice)
        return swapped & pair

    after = jnp.where(opens_pair(slot), 1, 0)
    before = jnp.where(opens_pair(slot - 1), 1, 0)
    row = lax.broadcasted_iota(jnp.int32, (8, lanes), 0)
    renamed = jnp.where(
        jnp.broadcast_to(after, (8, lanes)) == 1,
        pltpu.roll(atoms, lanes - 1, 1),
        jnp.where(jnp.broadcast_to(before, (8, lanes)) == 1, pltpu.roll(atoms, 1, 1), atoms),
    )
    atoms = jnp.where(row < 3, atoms, renamed)
    real = (slot < table_lookup(types, ATOM_COUNTS)) & (place < own_atoms)
    real = jnp.broadcast_to(jnp.where(real, 1, 0), (8, lanes)) == 1
    atoms = jnp.where((row == 6) & ~real, 0.0, atoms)
    weight = atoms[6:7]
    earlier = lax.broadcasted_iota(jnp.int32, (lanes, lanes), 0) < lax.broadcasted_iota(jnp.int32, (lanes, lanes), 1)
    earlier = jnp.where(earlier, 1.0, 0.0).astype(jnp.bfloat16)
    rank = jnp.dot(
        jnp.broadcast_to(weight, (16, lanes)).astype(jnp.bfloat16), earlier, preferred_element_type=jnp.float32
    )[0:1]
    atom_rank = jnp.where(weight > 0.5, rank, -1.0).astype(jnp.int32)
    atom_count = jnp.sum(weight, axis=1, keepdims=True)

    place = lax.broadcasted_iota(jnp.int32, (1, frames), 1)
    code, slot = spread_residues(codes, place, FRAME_SLOTS)
    types = code & 31
    swapped = code >= 32
    chi = table_lookup(types, CHI_COUNTS)
    exists = (slot == 0) | (slot == 3) | ((slot >= 4) & (slot - 3 <= chi))
    exists = jnp.where(exists, 1.0, 0.0)
    half_turn = ((types == 3) | (types == 13) | (types == 18)) & (slot == 5)
    half_turn = swapped & (half_turn | ((types == 6) & (slot == 6)))
    sign = jnp.where(half_turn, -1.0, 1.0)
    rot_pred = [[pf_ref[pl.ds(3 * a + c, 1), :] for c in range(3)] for a in range(3)]
    rot_true = [[tf_ref[pl.ds(3 * a + c, 1), :] for c in range(3)] for a in range(3)]
    rot_true = [[r[0], r[1] * sign, r[2] * sign] for r in rot_true]
    rows = []
    shifts = []
    for a in range(3):
        rel = [
            rot_pred[a][0] * rot_true[b][0] + rot_pred[a][1] * rot_true[b][1] + rot_pred[a][2] * rot_true[b][2]
            for b in range(3)
        ]
        shift = rel[0] * tf_ref[9:10, :] + rel[1] * tf_ref[10:11, :] + rel[2] * tf_ref[11:12, :]
        shifts.append(shift - pf_ref[pl.ds(9 + a, 1), :])
        if a < 2:
            rows += [-rel[0], -rel[1], -rel[2]]
    rows += shifts + [exists]
    rows += [jnp.zeros((16 - len(rows), frames), jnp.float32)]
    rank = jnp.dot(
        jnp.broadcast_to(exists, (16, frames)).astype(jnp.bfloat16),
        earlier[:frames, :frames],
        preferred_element_type=jnp.float32,
    )[0:1]
    frame_rank = jnp.where(exists > 0.5, rank, -1.0).astype(jnp.int32)
    frame_count = jnp.sum(exists, axis=1, keepdims=True)

    atoms = exact_dot(atoms, one_hot(atom_rank), 1)
    packed = exact_dot(jnp.concatenate(rows, axis=0), one_hot(frame_rank), 1)
    first = jnp.where(place == 0, frame_count, jnp.where(place == 1, atom_count, packed[9:10]))
    extra = jnp.concatenate([first, packed[8:9]], axis=1)
    atoms = jnp.where(row == 7, jnp.broadcast_to(extra, (8, lanes)), atoms)
    block = jnp.concatenate([atoms, packed[0:8]], axis=1)
    block_ref[0] = block
    rank_ref[...] = jnp.zeros(rank_ref.shape, jnp.int32)
    rank_ref[0:1, :] = atom_rank
    rank_ref[1:2, 0:frames] = frame_rank


def exchange_steps(gx_size, gy_size):
    steps = [("gy", 1 << k) for k in range(gy_size.bit_length() - 1)]
    steps += [("gx", 1 << k) for k in range(1, gx_size.bit_length() - 1)]
    return steps + [("gx", 1)]


def device_code(gx_size, gy_size):
    code = 0
    for k, (axis, step) in enumerate(exchange_steps(gx_size, gy_size)):
        code = code + jnp.where(lax.axis_index(axis) & step != 0, 1 << k, 0)
    return code


def pair_kernel(
    sizes, blocks_ref, rank_ref, frame_ref, atom_ref, total_ref, src_ref, fsrc_ref, rhs_ref, lhs_ref, row_ref, col_ref
):
    devices = blocks_ref.shape[0]
    frames = frame_ref.shape[1]
    own_atoms = atom_ref.shape[1]
    row_step = ROW_CHUNK // 16
    per_tile = TILE // 128
    me = device_code(*sizes)
    lane = lax.broadcasted_iota(jnp.int32, (8, 128), 1)
    sub = lax.broadcasted_iota(jnp.int32, (8, 128), 0)
    src_ref[...] = jnp.zeros(src_ref.shape, jnp.float32)
    fsrc_ref[...] = jnp.zeros(fsrc_ref.shape, jnp.float32)
    col_ref[...] = jnp.zeros(col_ref.shape, jnp.float32)

    def place_block(device, carry):
        atoms_before, frames_before, my_atoms, my_frames = carry
        my_atoms = jnp.where(device == me, atoms_before, my_atoms)
        my_frames = jnp.where(device == me, frames_before, my_frames)
        block = jnp.bitwise_xor(me, device)
        frame_count = jnp.max(blocks_ref[block, 7:8, 0:1]).astype(jnp.int32)
        atom_count = jnp.max(blocks_ref[block, 7:8, 1:2]).astype(jnp.int32)
        tile = atoms_before // 128
        turn = atoms_before % 128
        low = pltpu.roll(blocks_ref[block, :, 0:128], turn, 1)
        high = pltpu.roll(blocks_ref[block, :, 128:256], turn, 1)
        inside = lane >= turn
        src_ref[tile] += jnp.where(inside, low, 0.0)
        src_ref[tile + 1] += jnp.where(inside, high, low)
        src_ref[tile + 2] += jnp.where(inside, 0.0, high)
        exists = jnp.where(lane[0:1] < 2, 1.0, blocks_ref[block, 7:8, 0:128])
        last = jnp.broadcast_to(blocks_ref[block, 7:8, 128:256], (8, 128))
        tile = frames_before // 128
        turn = frames_before % 128
        low = pltpu.roll(blocks_ref[block, :, 256:384], turn, 1)
        high = pltpu.roll(jnp.where(sub == 0, last, jnp.broadcast_to(exists, (8, 128))), turn, 1)
        inside = lane >= turn
        fsrc_ref[tile, 0:8] += jnp.where(inside, low, 0.0)
        fsrc_ref[tile, 8:16] += jnp.where(inside, high, 0.0)
        fsrc_ref[tile + 1, 0:8] += jnp.where(inside, 0.0, low)
        fsrc_ref[tile + 1, 8:16] += jnp.where(inside, 0.0, high)
        return (atoms_before + atom_count, frames_before + frame_count, my_atoms, my_frames)

    group = 16
    while devices % group:
        group //= 2

    def place_group(index, carry):
        for k in range(group):
            carry = place_block(index * group + k, carry)
        return carry

    carry = (0, 0, 0, 0)
    if devices == group:
        carry = place_group(0, carry)
    else:
        carry = lax.fori_loop(0, devices // group, place_group, carry)
    atom_total, frame_total, my_atoms, my_frames = carry
    chunks = (frame_total + ROW_CHUNK - 1) // ROW_CHUNK
    width = TILE * TILE_GROUP
    groups = (atom_total + width - 1) // width
    frame_tiles = (frame_total + 127) // 128

    def build_lhs(index, carry):
        for k in range(BUILD_GROUP):
            tile = index * BUILD_GROUP + k
            part = fsrc_ref[tile, 0:8]
            last = fsrc_ref[tile, 8:9]
            exists = fsrc_ref[tile, 9:10]
            a = [part[k : k + 1] for k in range(3)]
            b = [part[3 + k : 4 + k] for k in range(3)]
            cross = [a[2] * b[1] - a[1] * b[2], a[0] * b[2] - a[2] * b[0], a[1] * b[0] - a[0] * b[1]]
            rotations = (part[0:3], part[3:6], jnp.concatenate(cross, axis=0))
            shifts = (part[6:7], part[7:8], last)
            for c in range(3):
                block = jnp.concatenate([rotations[c], rotations[c], shifts[c], exists], axis=0)
                high, middle, low = split_rows(block)
                ones = jnp.broadcast_to(exists, (8, 128))
                stack = [
                    jnp.where((sub >= 3) & (sub < 6), middle, high),
                    jnp.where(sub < 3, low, jnp.where(sub == 6, middle, high)),
                    jnp.where(sub < 3, middle, jnp.where(sub == 6, low, high)),
                ]
                stack = [x if k == c else jnp.where(sub == 7, 0.0, x) for k, x in enumerate(stack)]
                stack.append(jnp.where((sub == c) | (sub == 3 + c), ones, 0.0))
                stack.append(jnp.zeros((96, 128), jnp.float32))
                turned = jnp.concatenate(stack, axis=0).T
                lhs_ref[pl.ds(8 * tile, 8), c] = turned.astype(jnp.bfloat16).reshape(8, 16, 128)
        return carry

    build_groups = (frame_tiles + BUILD_GROUP - 1) // BUILD_GROUP
    lax.fori_loop(0, build_groups, build_lhs, 0)
    lhs_ref[pl.ds(build_groups * (8 * BUILD_GROUP), row_step)] = jnp.zeros((row_step,) + lhs_ref.shape[1:], jnp.bfloat16)
    row_ref[pl.ds(pl.multiple_of(chunks * ROW_CHUNK, 8), 256), :] = jnp.zeros((256, 128), jnp.float32)

    def build_rhs(index, carry):
        for k in range(TILE_GROUP):
            tile = index * TILE_GROUP + k
            x = jnp.concatenate([src_ref[tile * per_tile + m] for m in range(per_tile)], axis=1)
            high, middle, low = split_rows(x)
            one = jnp.ones((1, TILE), jnp.float32)
            nil = jnp.zeros((2, TILE), jnp.float32)
            rows = [high[3:6], high[3:6], one, high[0:1], high[3:6], middle[3:6], one, high[1:2]]
            rows += [middle[3:6], low[3:6], one, high[2:3], middle[0:3], low[0:3], nil]
            rhs_ref[tile] = jnp.concatenate(rows, axis=0).astype(jnp.bfloat16)
        return carry

    lax.fori_loop(0, groups, build_rhs, 0)

    def one_chunk(chunk, carry):
        start = pl.multiple_of(chunk * ROW_CHUNK, 8)
        row_ref[pl.ds(start, ROW_CHUNK), :] = jnp.zeros((ROW_CHUNK, 128), jnp.float32)

        def one_group(index, carry):
            lhs = lhs_ref[pl.ds(chunk * row_step, row_step)].reshape(3 * ROW_CHUNK, 128)[:, 0:32]
            for pair in range(0, TILE_GROUP, 2):
                tiles = [index * TILE_GROUP + pair + k for k in range(2)]
                dots = [jnp.dot(lhs, rhs_ref[tile], preferred_element_type=jnp.float32) for tile in tiles]
                caps = []
                for tile in tiles:
                    cap = jnp.concatenate([src_ref[tile * per_tile + m, 6:7, :] for m in range(per_tile)], axis=1)
                    caps.append(jnp.broadcast_to(cap * clamp_length, (8, TILE)))
                columns = [None, None]
                for g in range(ROW_CHUNK // 8):
                    base = 48 * (g // 2) + 8 * (g % 2)
                    row_sum = row_ref[pl.ds(start + 8 * g, 8), :]
                    for k in range(2):
                        w0, w1, w2 = (dots[k][base + 16 * c : base + 16 * c + 8] for c in range(3))
                        square = (w0 * w0 + w1 * w1) + (w2 * w2 + eps_square)
                        distance = jnp.minimum(square * lax.rsqrt(square), caps[k])
                        columns[k] = distance if columns[k] is None else columns[k] + distance
                        for m in range(per_tile):
                            row_sum = row_sum + distance[:, 128 * m : 128 * m + 128]
                    row_ref[pl.ds(start + 8 * g, 8), :] = row_sum
                for k, tile in enumerate(tiles):
                    for m in range(per_tile):
                        col_ref[tile * per_tile + m] += columns[k][:, 128 * m : 128 * m + 128]
            return carry

        return lax.fori_loop(0, groups, one_group, carry)

    lax.fori_loop(0, chunks, one_chunk, 0)

    idle = (chunks * ROW_CHUNK - frame_total).astype(jnp.float32)
    least = jnp.full((1, 128), eps_square, jnp.float32)
    least = least * lax.rsqrt(least)

    def column_sums(tile):
        cap = src_ref[tile, 6:7, :] * clamp_length
        return jnp.sum(col_ref[tile], axis=0, keepdims=True) - idle * jnp.minimum(least, cap)

    def add_group(index, carry):
        sums, floor = carry
        for k in range(per_tile * TILE_GROUP):
            tile = index * (per_tile * TILE_GROUP) + k
            sums = sums + col_ref[tile]
            floor = floor + jnp.minimum(least, src_ref[tile, 6:7, :] * clamp_length)
        return sums, floor

    empty = (jnp.zeros((8, 128), jnp.float32), jnp.zeros((1, 128), jnp.float32))
    sums, floor = lax.fori_loop(0, groups, add_group, empty)
    loss = jnp.sum(sums, axis=0, keepdims=True) - idle * floor
    loss = jnp.sum(loss, axis=1, keepdims=True)
    atom_number = atom_total.astype(jnp.float32)
    frame_number = frame_total.astype(jnp.float32)
    scale = 1.0 / clamp_length
    total_ref[...] = loss * scale / (frame_number * atom_number)

    tile = my_atoms // 128
    turn = my_atoms % 128
    back = (128 - turn) % 128
    pieces = [pltpu.roll(jnp.broadcast_to(column_sums(tile + k), (8, 128)), back, 1) for k in range(3)]
    keep = lane < 128 - turn
    mine = jnp.concatenate([jnp.where(keep, pieces[k], pieces[k + 1]) for k in range(2)], axis=1)
    mine = exact_dot(mine, one_hot(rank_ref[0:1, :]), 0)[0:1]
    atom_ref[...] = mine[:, :own_atoms] * scale / frame_number

    tile = my_frames // 128
    back = (128 - my_frames % 128) % 128
    pieces = []
    for k in range(2):
        rows = row_ref[pl.ds(pl.multiple_of((tile + k) * 128, 128), 128), :]
        sums = jnp.sum(rows.T, axis=0, keepdims=True)
        pieces.append(pltpu.roll(jnp.broadcast_to(sums, (8, 128)), back, 1))
    mine = jnp.where(lane < 128 - my_frames % 128, pieces[0], pieces[1])
    mine = exact_dot(mine, one_hot(rank_ref[1:2, 0:frames]), 0)[0:1]
    frame_ref[...] = mine * scale / atom_number


def shards(pred_frames, true_frames, pred_atoms, true_atoms, atom_mask, residue_types, swap_flags):
    devices = lax.axis_size("gx") * lax.axis_size("gy")
    frames = pred_frames.shape[1]
    own_atoms = pred_atoms.shape[1]
    lanes = -(-own_atoms // 128) * 128
    f32 = jnp.float32
    inputs = (residue_types, swap_flags, pred_frames, true_frames, pred_atoms, true_atoms)
    inputs += (atom_mask.reshape(1, own_atoms),)
    blocks, ranks = pl.pallas_call(
        prep_kernel,
        out_shape=(
            jax.ShapeDtypeStruct((1, 8, lanes + frames), f32),
            jax.ShapeDtypeStruct((8, lanes), jnp.int32),
        ),
        in_specs=[HBM] * 7,
        out_specs=(VMEM, VMEM),
        scratch_shapes=[
            pltpu.SMEM(residue_types.shape, jnp.int32),
            pltpu.SMEM(swap_flags.shape, jnp.int32),
            pltpu.VMEM(pred_frames.shape, f32),
            pltpu.VMEM(true_frames.shape, f32),
            pltpu.VMEM(pred_atoms.shape, f32),
            pltpu.VMEM(true_atoms.shape, f32),
            pltpu.VMEM((1, own_atoms), jnp.int32),
            pltpu.VMEM((8, lanes), f32),
            pltpu.SemaphoreType.DMA((7,)),
        ],
        compiler_params=pltpu.CompilerParams(vmem_limit_bytes=8 << 20),
        name="prep",
    )(*[pltpu.with_memory_space_constraint(x, pltpu.HBM) for x in inputs])
    for axis, step in exchange_steps(lax.axis_size("gx"), lax.axis_size("gy")):
        pairs = [(i, i ^ step) for i in range(lax.axis_size(axis))]
        blocks = jnp.concatenate([blocks, lax.ppermute(blocks, axis, pairs)], axis=0)
    width = TILE * TILE_GROUP
    groups = -(-(devices * own_atoms + 256) // width)
    most = devices * (frames * USED_SLOTS // FRAME_SLOTS)
    frame_tiles = -(-most // (128 * BUILD_GROUP)) * BUILD_GROUP + 1
    row_groups = 8 * frame_tiles + 2 * ROW_CHUNK // 16 + 16
    scratch = [
        ((groups * width // 128, 8, 128), f32),
        ((frame_tiles, 16, 128), f32),
        ((groups * TILE_GROUP, 32, TILE), jnp.bfloat16),
        ((row_groups, 3, 16, 128), jnp.bfloat16),
        ((row_groups * 16, 128), f32),
        ((groups * width // 128, 8, 128), f32),
    ]
    room = sum(jnp.dtype(dtype).itemsize * functools.reduce(lambda a, b: a * b, shape) for shape, dtype in scratch)
    frame_loss, atom_loss, total_loss = pl.pallas_call(
        functools.partial(pair_kernel, (lax.axis_size("gx"), lax.axis_size("gy"))),
        out_shape=(
            jax.ShapeDtypeStruct((1, frames), f32),
            jax.ShapeDtypeStruct((1, own_atoms), f32),
            jax.ShapeDtypeStruct((1, 1), f32),
        ),
        in_specs=[VMEM, VMEM],
        out_specs=(VMEM, VMEM, VMEM),
        scratch_shapes=[pltpu.VMEM(shape, dtype) for shape, dtype in scratch],
        compiler_params=pltpu.CompilerParams(vmem_limit_bytes=room + (12 << 20)),
        name="pairs",
    )(blocks, ranks)
    return (frame_loss.reshape(frames), atom_loss.reshape(own_atoms), total_loss.reshape(1))


def solution(mesh):
    both = P(None, ("sa", "gx", "gy"))
    flat = P(("sa", "gx", "gy"))
    return jax.shard_map(
        shards,
        mesh=mesh,
        in_specs=(both, both, both, both, flat, flat, flat),
        out_specs=(flat, flat, P("sa")),
        check_vma=False,
    )
```

```python
import functools

import jax
import jax.numpy as jnp
from jax import lax
from jax.experimental import pallas as pl
from jax.experimental.pallas import tpu as pltpu
from jax.sharding import PartitionSpec as P

eps_square = 0.0001
clamp_length = 10.0

ATOM_COUNTS = (5, 11, 8, 8, 6, 9, 9, 4, 10, 8, 8, 9, 8, 11, 7, 6, 7, 14, 12, 7)
CHI_COUNTS = (0, 4, 2, 2, 1, 3, 3, 0, 2, 2, 2, 4, 3, 2, 2, 1, 1, 2, 2, 1)
FRAME_SLOTS = 8
USED_SLOTS = 6
BUILD_GROUP = 8
ATOM_SLOTS = 14
ROW_CHUNK = 528
TILE = 256
TILE_GROUP = 8
VMEM = pl.BlockSpec(memory_space=pltpu.VMEM)
HBM = pl.BlockSpec(memory_space=pltpu.HBM)


def spread_residues(scalars, positions, width):
    value = jnp.full(positions.shape, scalars[0], jnp.int32)
    first = jnp.zeros(positions.shape, jnp.int32)
    for residue in range(1, len(scalars)):
        here = positions >= residue * width
        value = jnp.where(here, scalars[residue], value)
        first = jnp.where(here, residue * width, first)
    return value, positions - first


def table_lookup(types, table):
    value = jnp.full(types.shape, table[0], jnp.int32)
    for kind in range(1, len(table)):
        if table[kind] != table[0]:
            value = jnp.where(types == kind, table[kind], value)
    return value


def split_rows(x):
    high = x.astype(jnp.bfloat16).astype(jnp.float32)
    rest = x - high
    middle = rest.astype(jnp.bfloat16).astype(jnp.float32)
    return high, middle, rest - middle


def one_hot(rank):
    size = rank.shape[1]
    place = lax.broadcasted_iota(jnp.int32, (size, size), 0)
    return jnp.where(place == rank, 1.0, 0.0).astype(jnp.bfloat16)


def exact_dot(x, selection, contract):
    rows = x.shape[0]
    parts = jnp.concatenate(split_rows(x), axis=0).astype(jnp.bfloat16)
    out = lax.dot_general(parts, selection, (((1,), (contract,)), ((), ())), preferred_element_type=jnp.float32)
    return out[:rows] + out[rows : 2 * rows] + out[2 * rows :]


def prep_kernel(*refs):
    inputs, (block_ref, rank_ref), scratch = refs[:7], refs[7:9], refs[9:]
    (types_ref, flags_ref, pf_ref, tf_ref, pa_ref, ta_ref, mask_ref, pad_ref, sems) = scratch
    fetches = [pltpu.make_async_copy(src, dst, sems.at[i]) for i, (src, dst) in enumerate(zip(inputs, scratch))]
    for fetch in fetches:
        fetch.start()
    residues = types_ref.shape[0]
    frames = pf_ref.shape[1]
    own_atoms = pa_ref.shape[1]
    lanes = pad_ref.shape[1]
    pad_ref[...] = jnp.zeros(pad_ref.shape, jnp.float32)
    for fetch in fetches:
        fetch.wait()
    codes = [types_ref[r] + 32 * flags_ref[r] for r in range(residues)]

    pad_ref[0:3, 0:own_atoms] = pa_ref[...]
    pad_ref[3:6, 0:own_atoms] = ta_ref[...]
    pad_ref[6:7, 0:own_atoms] = mask_ref[...].astype(jnp.float32)
    atoms = pad_ref[...]
    place = lax.broadcasted_iota(jnp.int32, (1, lanes), 1)
    code, slot = spread_residues(codes, place, ATOM_SLOTS)
    types = code & 31
    swapped = code >= 32
    twice = (types == 13) | (types == 18)

    def opens_pair(s):
        pair = ((s == 6) & ((types == 3) | twice)) | ((s == 7) & (types == 6)) | ((s == 8) & twice)
        return swapped & pair

    after = jnp.where(opens_pair(slot), 1, 0)
    before = jnp.where(opens_pair(slot - 1), 1, 0)
    row = lax.broadcasted_iota(jnp.int32, (8, lanes), 0)
    renamed = jnp.where(
        jnp.broadcast_to(after, (8, lanes)) == 1,
        pltpu.roll(atoms, lanes - 1, 1),
        jnp.where(jnp.broadcast_to(before, (8, lanes)) == 1, pltpu.roll(atoms, 1, 1), atoms),
    )
    atoms = jnp.where(row < 3, atoms, renamed)
    real = (slot < table_lookup(types, ATOM_COUNTS)) & (place < own_atoms)
    real = jnp.broadcast_to(jnp.where(real, 1, 0), (8, lanes)) == 1
    atoms = jnp.where((row == 6) & ~real, 0.0, atoms)
    weight = atoms[6:7]
    earlier = lax.broadcasted_iota(jnp.int32, (lanes, lanes), 0) < lax.broadcasted_iota(jnp.int32, (lanes, lanes), 1)
    earlier = jnp.where(earlier, 1.0, 0.0).astype(jnp.bfloat16)
    rank = jnp.dot(
        jnp.broadcast_to(weight, (16, lanes)).astype(jnp.bfloat16), earlier, preferred_element_type=jnp.float32
    )[0:1]
    atom_rank = jnp.where(weight > 0.5, rank, -1.0).astype(jnp.int32)
    atom_count = jnp.sum(weight, axis=1, keepdims=True)

    place = lax.broadcasted_iota(jnp.int32, (1, frames), 1)
    code, slot = spread_residues(codes, place, FRAME_SLOTS)
    types = code & 31
    swapped = code >= 32
    chi = table_lookup(types, CHI_COUNTS)
    exists = (slot == 0) | (slot == 3) | ((slot >= 4) & (slot - 3 <= chi))
    exists = jnp.where(exists, 1.0, 0.0)
    half_turn = ((types == 3) | (types == 13) | (types == 18)) & (slot == 5)
    half_turn = swapped & (half_turn | ((types == 6) & (slot == 6)))
    sign = jnp.where(half_turn, -1.0, 1.0)
    rot_pred = [[pf_ref[pl.ds(3 * a + c, 1), :] for c in range(3)] for a in range(3)]
    rot_true = [[tf_ref[pl.ds(3 * a + c, 1), :] for c in range(3)] for a in range(3)]
    rot_true = [[r[0], r[1] * sign, r[2] * sign] for r in rot_true]
    rows = []
    shifts = []
    for a in range(3):
        rel = [
            rot_pred[a][0] * rot_true[b][0] + rot_pred[a][1] * rot_true[b][1] + rot_pred[a][2] * rot_true[b][2]
            for b in range(3)
        ]
        shift = rel[0] * tf_ref[9:10, :] + rel[1] * tf_ref[10:11, :] + rel[2] * tf_ref[11:12, :]
        shifts.append(shift - pf_ref[pl.ds(9 + a, 1), :])
        if a < 2:
            rows += [-rel[0], -rel[1], -rel[2]]
    rows += shifts + [exists]
    rows += [jnp.zeros((16 - len(rows), frames), jnp.float32)]
    rank = jnp.dot(
        jnp.broadcast_to(exists, (16, frames)).astype(jnp.bfloat16),
        earlier[:frames, :frames],
        preferred_element_type=jnp.float32,
    )[0:1]
    frame_rank = jnp.where(exists > 0.5, rank, -1.0).astype(jnp.int32)
    frame_count = jnp.sum(exists, axis=1, keepdims=True)

    atoms = exact_dot(atoms, one_hot(atom_rank), 1)
    packed = exact_dot(jnp.concatenate(rows, axis=0), one_hot(frame_rank), 1)
    first = jnp.where(place == 0, frame_count, jnp.where(place == 1, atom_count, packed[9:10]))
    extra = jnp.concatenate([first, packed[8:9]], axis=1)
    atoms = jnp.where(row == 7, jnp.broadcast_to(extra, (8, lanes)), atoms)
    block = jnp.concatenate([atoms, packed[0:8]], axis=1)
    block_ref[0] = block
    rank_ref[...] = jnp.zeros(rank_ref.shape, jnp.int32)
    rank_ref[0:1, :] = atom_rank
    rank_ref[1:2, 0:frames] = frame_rank


def exchange_steps(gx_size, gy_size):
    steps = [("gy", 1 << k) for k in range(gy_size.bit_length() - 1)]
    steps += [("gx", 1 << k) for k in range(1, gx_size.bit_length() - 1)]
    return steps + [("gx", 1)]


def device_code(gx_size, gy_size):
    code = 0
    for k, (axis, step) in enumerate(exchange_steps(gx_size, gy_size)):
        code = code + jnp.where(lax.axis_index(axis) & step != 0, 1 << k, 0)
    return code


def pair_kernel(
    sizes, blocks_ref, rank_ref, frame_ref, atom_ref, total_ref, src_ref, fsrc_ref, rhs_ref, lhs_ref, row_ref, col_ref
):
    devices = blocks_ref.shape[0]
    frames = frame_ref.shape[1]
    own_atoms = atom_ref.shape[1]
    row_step = ROW_CHUNK // 16
    per_tile = TILE // 128
    me = device_code(*sizes)
    lane = lax.broadcasted_iota(jnp.int32, (8, 128), 1)
    sub = lax.broadcasted_iota(jnp.int32, (8, 128), 0)
    src_ref[...] = jnp.zeros(src_ref.shape, jnp.float32)
    fsrc_ref[...] = jnp.zeros(fsrc_ref.shape, jnp.float32)
    col_ref[...] = jnp.zeros(col_ref.shape, jnp.float32)

    def place_block(device, carry):
        atoms_before, frames_before, my_atoms, my_frames = carry
        my_atoms = jnp.where(device == me, atoms_before, my_atoms)
        my_frames = jnp.where(device == me, frames_before, my_frames)
        block = jnp.bitwise_xor(me, device)
        frame_count = jnp.max(blocks_ref[block, 7:8, 0:1]).astype(jnp.int32)
        atom_count = jnp.max(blocks_ref[block, 7:8, 1:2]).astype(jnp.int32)
        tile = atoms_before // 128
        turn = atoms_before % 128
        low = pltpu.roll(blocks_ref[block, :, 0:128], turn, 1)
        high = pltpu.roll(blocks_ref[block, :, 128:256], turn, 1)
        inside = lane >= turn
        src_ref[tile] += jnp.where(inside, low, 0.0)
        src_ref[tile + 1] += jnp.where(inside, high, low)
        src_ref[tile + 2] += jnp.where(inside, 0.0, high)
        exists = jnp.where(lane[0:1] < 2, 1.0, blocks_ref[block, 7:8, 0:128])
        last = jnp.broadcast_to(blocks_ref[block, 7:8, 128:256], (8, 128))
        tile = frames_before // 128
        turn = frames_before % 128
        low = pltpu.roll(blocks_ref[block, :, 256:384], turn, 1)
        high = pltpu.roll(jnp.where(sub == 0, last, jnp.broadcast_to(exists, (8, 128))), turn, 1)
        inside = lane >= turn
        fsrc_ref[tile, 0:8] += jnp.where(inside, low, 0.0)
        fsrc_ref[tile, 8:16] += jnp.where(inside, high, 0.0)
        fsrc_ref[tile + 1, 0:8] += jnp.where(inside, 0.0, low)
        fsrc_ref[tile + 1, 8:16] += jnp.where(inside, 0.0, high)
        return (atoms_before + atom_count, frames_before + frame_count, my_atoms, my_frames)

    group = 16
    while devices % group:
        group //= 2

    def place_group(index, carry):
        for k in range(group):
            carry = place_block(index * group + k, carry)
        return carry

    carry = (0, 0, 0, 0)
    if devices == group:
        carry = place_group(0, carry)
    else:
        carry = lax.fori_loop(0, devices // group, place_group, carry)
    atom_total, frame_total, my_atoms, my_frames = carry
    chunks = (frame_total + ROW_CHUNK - 1) // ROW_CHUNK
    width = TILE * TILE_GROUP
    groups = (atom_total + width - 1) // width
    frame_tiles = (frame_total + 127) // 128

    def build_lhs(index, carry):
        for k in range(BUILD_GROUP):
            tile = index * BUILD_GROUP + k
            part = fsrc_ref[tile, 0:8]
            last = fsrc_ref[tile, 8:9]
            exists = fsrc_ref[tile, 9:10]
            a = [part[k : k + 1] for k in range(3)]
            b = [part[3 + k : 4 + k] for k in range(3)]
            cross = [a[2] * b[1] - a[1] * b[2], a[0] * b[2] - a[2] * b[0], a[1] * b[0] - a[0] * b[1]]
            rotations = (part[0:3], part[3:6], jnp.concatenate(cross, axis=0))
            shifts = (part[6:7], part[7:8], last)
            for c in range(3):
                block = jnp.concatenate([rotations[c], rotations[c], shifts[c], exists], axis=0)
                high, middle, low = split_rows(block)
                ones = jnp.broadcast_to(exists, (8, 128))
                stack = [
                    jnp.where((sub >= 3) & (sub < 6), middle, high),
                    jnp.where(sub < 3, low, jnp.where(sub == 6, middle, high)),
                    jnp.where(sub < 3, middle, jnp.where(sub == 6, low, high)),
                ]
                stack = [x if k == c else jnp.where(sub == 7, 0.0, x) for k, x in enumerate(stack)]
                stack.append(jnp.where((sub == c) | (sub == 3 + c), ones, 0.0))
                stack.append(jnp.zeros((96, 128), jnp.float32))
                turned = jnp.concatenate(stack, axis=0).T
                lhs_ref[pl.ds(8 * tile, 8), c] = turned.astype(jnp.bfloat16).reshape(8, 16, 128)
        return carry

    build_groups = (frame_tiles + BUILD_GROUP - 1) // BUILD_GROUP
    lax.fori_loop(0, build_groups, build_lhs, 0)
    lhs_ref[pl.ds(build_groups * (8 * BUILD_GROUP), row_step)] = jnp.zeros((row_step,) + lhs_ref.shape[1:], jnp.bfloat16)
    row_ref[pl.ds(pl.multiple_of(chunks * ROW_CHUNK, 8), 256), :] = jnp.zeros((256, 128), jnp.float32)

    def build_rhs(index, carry):
        for k in range(TILE_GROUP):
            tile = index * TILE_GROUP + k
            x = jnp.concatenate([src_ref[tile * per_tile + m] for m in range(per_tile)], axis=1)
            high, middle, low = split_rows(x)
            one = jnp.ones((1, TILE), jnp.float32)
            nil = jnp.zeros((2, TILE), jnp.float32)
            rows = [high[3:6], high[3:6], one, high[0:1], high[3:6], middle[3:6], one, high[1:2]]
            rows += [middle[3:6], low[3:6], one, high[2:3], middle[0:3], low[0:3], nil]
            rhs_ref[tile] = jnp.concatenate(rows, axis=0).astype(jnp.bfloat16)
        return carry

    lax.fori_loop(0, groups, build_rhs, 0)

    def one_chunk(chunk, carry):
        start = pl.multiple_of(chunk * ROW_CHUNK, 8)
        row_ref[pl.ds(start, ROW_CHUNK), :] = jnp.zeros((ROW_CHUNK, 128), jnp.float32)

        def one_group(index, carry):
            lhs = lhs_ref[pl.ds(chunk * row_step, row_step)].reshape(3 * ROW_CHUNK, 128)[:, 0:32]
            for pair in range(0, TILE_GROUP, 2):
                tiles = [index * TILE_GROUP + pair + k for k in range(2)]
                dots = [jnp.dot(lhs, rhs_ref[tile], preferred_element_type=jnp.float32) for tile in tiles]
                caps = []
                for tile in tiles:
                    cap = jnp.concatenate([src_ref[tile * per_tile + m, 6:7, :] for m in range(per_tile)], axis=1)
                    caps.append(jnp.broadcast_to(cap * clamp_length, (8, TILE)))
                columns = [None, None]
                for g in range(ROW_CHUNK // 8):
                    base = 48 * (g // 2) + 8 * (g % 2)
                    row_sum = row_ref[pl.ds(start + 8 * g, 8), :]
                    for k in range(2):
                        w0, w1, w2 = (dots[k][base + 16 * c : base + 16 * c + 8] for c in range(3))
                        square = (w0 * w0 + w1 * w1) + (w2 * w2 + eps_square)
                        distance = jnp.minimum(square * lax.rsqrt(square), caps[k])
                        columns[k] = distance if columns[k] is None else columns[k] + distance
                        for m in range(per_tile):
                            row_sum = row_sum + distance[:, 128 * m : 128 * m + 128]
                    row_ref[pl.ds(start + 8 * g, 8), :] = row_sum
                for k, tile in enumerate(tiles):
                    for m in range(per_tile):
                        col_ref[tile * per_tile + m] += columns[k][:, 128 * m : 128 * m + 128]
            return carry

        return lax.fori_loop(0, groups, one_group, carry)

    lax.fori_loop(0, chunks, one_chunk, 0)

    idle = (chunks * ROW_CHUNK - frame_total).astype(jnp.float32)
    least = jnp.full((1, 128), eps_square, jnp.float32)
    least = least * lax.rsqrt(least)

    def column_sums(tile):
        cap = src_ref[tile, 6:7, :] * clamp_length
        return jnp.sum(col_ref[tile], axis=0, keepdims=True) - idle * jnp.minimum(least, cap)

    def add_group(index, carry):
        sums, floor = carry
        for k in range(per_tile * TILE_GROUP):
            tile = index * (per_tile * TILE_GROUP) + k
            sums = sums + col_ref[tile]
            floor = floor + jnp.minimum(least, src_ref[tile, 6:7, :] * clamp_length)
        return sums, floor

    empty = (jnp.zeros((8, 128), jnp.float32), jnp.zeros((1, 128), jnp.float32))
    sums, floor = lax.fori_loop(0, groups, add_group, empty)
    loss = jnp.sum(sums, axis=0, keepdims=True) - idle * floor
    loss = jnp.sum(loss, axis=1, keepdims=True)
    atom_number = atom_total.astype(jnp.float32)
    frame_number = frame_total.astype(jnp.float32)
    scale = 1.0 / clamp_length
    total_ref[...] = loss * scale / (frame_number * atom_number)

    tile = my_atoms // 128
    turn = my_atoms % 128
    back = (128 - turn) % 128
    pieces = [pltpu.roll(jnp.broadcast_to(column_sums(tile + k), (8, 128)), back, 1) for k in range(3)]
    keep = lane < 128 - turn
    mine = jnp.concatenate([jnp.where(keep, pieces[k], pieces[k + 1]) for k in range(2)], axis=1)
    mine = exact_dot(mine, one_hot(rank_ref[0:1, :]), 0)[0:1]
    atom_ref[...] = mine[:, :own_atoms] * scale / frame_number

    tile = my_frames // 128
    back = (128 - my_frames % 128) % 128
    pieces = []
    for k in range(2):
        rows = row_ref[pl.ds(pl.multiple_of((tile + k) * 128, 128), 128), :]
        sums = jnp.sum(rows.T, axis=0, keepdims=True)
        pieces.append(pltpu.roll(jnp.broadcast_to(sums, (8, 128)), back, 1))
    mine = jnp.where(lane < 128 - my_frames % 128, pieces[0], pieces[1])
    mine = exact_dot(mine, one_hot(rank_ref[1:2, 0:frames]), 0)[0:1]
    frame_ref[...] = mine * scale / atom_number


def shards(pred_frames, true_frames, pred_atoms, true_atoms, atom_mask, residue_types, swap_flags):
    devices = lax.axis_size("gx") * lax.axis_size("gy")
    frames = pred_frames.shape[1]
    own_atoms = pred_atoms.shape[1]
    lanes = -(-own_atoms // 128) * 128
    f32 = jnp.float32
    inputs = (residue_types, swap_flags, pred_frames, true_frames, pred_atoms, true_atoms)
    inputs += (atom_mask.reshape(1, own_atoms),)
    blocks, ranks = pl.pallas_call(
        prep_kernel,
        out_shape=(
            jax.ShapeDtypeStruct((1, 8, lanes + frames), f32),
            jax.ShapeDtypeStruct((8, lanes), jnp.int32),
        ),
        in_specs=[HBM] * 7,
        out_specs=(VMEM, VMEM),
        scratch_shapes=[
            pltpu.SMEM(residue_types.shape, jnp.int32),
            pltpu.SMEM(swap_flags.shape, jnp.int32),
            pltpu.VMEM(pred_frames.shape, f32),
            pltpu.VMEM(true_frames.shape, f32),
            pltpu.VMEM(pred_atoms.shape, f32),
            pltpu.VMEM(true_atoms.shape, f32),
            pltpu.VMEM((1, own_atoms), jnp.int32),
            pltpu.VMEM((8, lanes), f32),
            pltpu.SemaphoreType.DMA((7,)),
        ],
        compiler_params=pltpu.CompilerParams(vmem_limit_bytes=8 << 20),
        name="prep",
    )(*[pltpu.with_memory_space_constraint(x, pltpu.HBM) for x in inputs])
    for axis, step in exchange_steps(lax.axis_size("gx"), lax.axis_size("gy")):
        pairs = [(i, i ^ step) for i in range(lax.axis_size(axis))]
        blocks = jnp.concatenate([blocks, lax.ppermute(blocks, axis, pairs)], axis=0)
    width = TILE * TILE_GROUP
    groups = -(-(devices * own_atoms + 256) // width)
    most = devices * (frames * USED_SLOTS // FRAME_SLOTS)
    frame_tiles = -(-most // (128 * BUILD_GROUP)) * BUILD_GROUP + 1
    row_groups = 8 * frame_tiles + 2 * ROW_CHUNK // 16 + 16
    scratch = [
        ((groups * width // 128, 8, 128), f32),
        ((frame_tiles, 16, 128), f32),
        ((groups * TILE_GROUP, 32, TILE), jnp.bfloat16),
        ((row_groups, 3, 16, 128), jnp.bfloat16),
        ((row_groups * 16, 128), f32),
        ((groups * width // 128, 8, 128), f32),
    ]
    room = sum(jnp.dtype(dtype).itemsize * functools.reduce(lambda a, b: a * b, shape) for shape, dtype in scratch)
    frame_loss, atom_loss, total_loss = pl.pallas_call(
        functools.partial(pair_kernel, (lax.axis_size("gx"), lax.axis_size("gy"))),
        out_shape=(
            jax.ShapeDtypeStruct((1, frames), f32),
            jax.ShapeDtypeStruct((1, own_atoms), f32),
            jax.ShapeDtypeStruct((1, 1), f32),
        ),
        in_specs=[VMEM, VMEM],
        out_specs=(VMEM, VMEM, VMEM),
        scratch_shapes=[pltpu.VMEM(shape, dtype) for shape, dtype in scratch],
        compiler_params=pltpu.CompilerParams(vmem_limit_bytes=room + (12 << 20)),
        name="pairs",
    )(blocks, ranks)
    return (frame_loss.reshape(frames), atom_loss.reshape(own_atoms), total_loss.reshape(1))


def solution(mesh):
    both = P(None, ("sa", "gx", "gy"))
    flat = P(("sa", "gx", "gy"))
    return jax.shard_map(
        shards,
        mesh=mesh,
        in_specs=(both, both, both, both, flat, flat, flat),
        out_specs=(flat, flat, P("sa")),
        check_vma=False,
    )
```

```python
import functools

import jax
import jax.numpy as jnp
from jax import lax
from jax.experimental import pallas as pl
from jax.experimental.pallas import tpu as pltpu
from jax.sharding import PartitionSpec as P

eps_square = 0.0001
clamp_length = 10.0

ATOM_COUNTS = (5, 11, 8, 8, 6, 9, 9, 4, 10, 8, 8, 9, 8, 11, 7, 6, 7, 14, 12, 7)
CHI_COUNTS = (0, 4, 2, 2, 1, 3, 3, 0, 2, 2, 2, 4, 3, 2, 2, 1, 1, 2, 2, 1)
FRAME_SLOTS = 8
USED_SLOTS = 6
BUILD_GROUP = 4
ATOM_SLOTS = 14
ROW_CHUNK = 544
TILE = 256
TILE_GROUP = 4
VMEM = pl.BlockSpec(memory_space=pltpu.VMEM)
HBM = pl.BlockSpec(memory_space=pltpu.HBM)


def spread_residues(scalars, positions, width):
    value = jnp.full(positions.shape, scalars[0], jnp.int32)
    first = jnp.zeros(positions.shape, jnp.int32)
    for residue in range(1, len(scalars)):
        here = positions >= residue * width
        value = jnp.where(here, scalars[residue], value)
        first = jnp.where(here, residue * width, first)
    return value, positions - first


def table_lookup(types, table):
    value = jnp.full(types.shape, table[0], jnp.int32)
    for kind in range(1, len(table)):
        if table[kind] != table[0]:
            value = jnp.where(types == kind, table[kind], value)
    return value


def split_rows(x):
    high = x.astype(jnp.bfloat16).astype(jnp.float32)
    rest = x - high
    middle = rest.astype(jnp.bfloat16).astype(jnp.float32)
    return high, middle, rest - middle


def one_hot(rank):
    size = rank.shape[1]
    place = lax.broadcasted_iota(jnp.int32, (size, size), 0)
    return jnp.where(place == rank, 1.0, 0.0).astype(jnp.bfloat16)


def exact_dot(x, selection, contract):
    rows = x.shape[0]
    parts = jnp.concatenate(split_rows(x), axis=0).astype(jnp.bfloat16)
    out = lax.dot_general(parts, selection, (((1,), (contract,)), ((), ())), preferred_element_type=jnp.float32)
    return out[:rows] + out[rows : 2 * rows] + out[2 * rows :]


def prep_kernel(*refs):
    inputs, (block_ref, rank_ref), scratch = refs[:7], refs[7:9], refs[9:]
    (types_ref, flags_ref, pf_ref, tf_ref, pa_ref, ta_ref, mask_ref, pad_ref, sems) = scratch
    fetches = [pltpu.make_async_copy(src, dst, sems.at[i]) for i, (src, dst) in enumerate(zip(inputs, scratch))]
    for fetch in fetches:
        fetch.start()
    residues = types_ref.shape[0]
    frames = pf_ref.shape[1]
    own_atoms = pa_ref.shape[1]
    lanes = pad_ref.shape[1]
    pad_ref[...] = jnp.zeros(pad_ref.shape, jnp.float32)
    for fetch in fetches:
        fetch.wait()
    codes = [types_ref[r] + 32 * flags_ref[r] for r in range(residues)]

    pad_ref[0:3, 0:own_atoms] = pa_ref[...]
    pad_ref[3:6, 0:own_atoms] = ta_ref[...]
    pad_ref[6:7, 0:own_atoms] = mask_ref[...].astype(jnp.float32)
    atoms = pad_ref[...]
    place = lax.broadcasted_iota(jnp.int32, (1, lanes), 1)
    code, slot = spread_residues(codes, place, ATOM_SLOTS)
    types = code & 31
    swapped = code >= 32
    twice = (types == 13) | (types == 18)

    def opens_pair(s):
        pair = ((s == 6) & ((types == 3) | twice)) | ((s == 7) & (types == 6)) | ((s == 8) & twice)
        return swapped & pair

    after = jnp.where(opens_pair(slot), 1, 0)
    before = jnp.where(opens_pair(slot - 1), 1, 0)
    row = lax.broadcasted_iota(jnp.int32, (8, lanes), 0)
    renamed = jnp.where(
        jnp.broadcast_to(after, (8, lanes)) == 1,
        pltpu.roll(atoms, lanes - 1, 1),
        jnp.where(jnp.broadcast_to(before, (8, lanes)) == 1, pltpu.roll(atoms, 1, 1), atoms),
    )
    atoms = jnp.where(row < 3, atoms, renamed)
    real = (slot < table_lookup(types, ATOM_COUNTS)) & (place < own_atoms)
    real = jnp.broadcast_to(jnp.where(real, 1, 0), (8, lanes)) == 1
    atoms = jnp.where((row == 6) & ~real, 0.0, atoms)
    weight = atoms[6:7]
    earlier = lax.broadcasted_iota(jnp.int32, (lanes, lanes), 0) < lax.broadcasted_iota(jnp.int32, (lanes, lanes), 1)
    earlier = jnp.where(earlier, 1.0, 0.0).astype(jnp.bfloat16)
    rank = jnp.dot(
        jnp.broadcast_to(weight, (16, lanes)).astype(jnp.bfloat16), earlier, preferred_element_type=jnp.float32
    )[0:1]
    atom_rank = jnp.where(weight > 0.5, rank, -1.0).astype(jnp.int32)
    atom_count = jnp.sum(weight, axis=1, keepdims=True)

    place = lax.broadcasted_iota(jnp.int32, (1, frames), 1)
    code, slot = spread_residues(codes, place, FRAME_SLOTS)
    types = code & 31
    swapped = code >= 32
    chi = table_lookup(types, CHI_COUNTS)
    exists = (slot == 0) | (slot == 3) | ((slot >= 4) & (slot - 3 <= chi))
    exists = jnp.where(exists, 1.0, 0.0)
    half_turn = ((types == 3) | (types == 13) | (types == 18)) & (slot == 5)
    half_turn = swapped & (half_turn | ((types == 6) & (slot == 6)))
    sign = jnp.where(half_turn, -1.0, 1.0)
    rot_pred = [[pf_ref[pl.ds(3 * a + c, 1), :] for c in range(3)] for a in range(3)]
    rot_true = [[tf_ref[pl.ds(3 * a + c, 1), :] for c in range(3)] for a in range(3)]
    rot_true = [[r[0], r[1] * sign, r[2] * sign] for r in rot_true]
    rows = []
    shifts = []
    for a in range(3):
        rel = [
            rot_pred[a][0] * rot_true[b][0] + rot_pred[a][1] * rot_true[b][1] + rot_pred[a][2] * rot_true[b][2]
            for b in range(3)
        ]
        shift = rel[0] * tf_ref[9:10, :] + rel[1] * tf_ref[10:11, :] + rel[2] * tf_ref[11:12, :]
        shifts.append(shift - pf_ref[pl.ds(9 + a, 1), :])
        if a < 2:
            rows += [-rel[0], -rel[1], -rel[2]]
    rows += shifts + [exists]
    rows += [jnp.zeros((16 - len(rows), frames), jnp.float32)]
    rank = jnp.dot(
        jnp.broadcast_to(exists, (16, frames)).astype(jnp.bfloat16),
        earlier[:frames, :frames],
        preferred_element_type=jnp.float32,
    )[0:1]
    frame_rank = jnp.where(exists > 0.5, rank, -1.0).astype(jnp.int32)
    frame_count = jnp.sum(exists, axis=1, keepdims=True)

    atoms = exact_dot(atoms, one_hot(atom_rank), 1)
    packed = exact_dot(jnp.concatenate(rows, axis=0), one_hot(frame_rank), 1)
    first = jnp.where(place == 0, frame_count, jnp.where(place == 1, atom_count, packed[9:10]))
    extra = jnp.concatenate([first, packed[8:9]], axis=1)
    atoms = jnp.where(row == 7, jnp.broadcast_to(extra, (8, lanes)), atoms)
    block = jnp.concatenate([atoms, packed[0:8]], axis=1)
    block_ref[0] = block
    rank_ref[...] = jnp.zeros(rank_ref.shape, jnp.int32)
    rank_ref[0:1, :] = atom_rank
    rank_ref[1:2, 0:frames] = frame_rank


def exchange_steps(gx_size, gy_size):
    steps = [("gy", 1 << k) for k in range(gy_size.bit_length() - 1)]
    steps += [("gx", 1 << k) for k in range(1, gx_size.bit_length() - 1)]
    return steps + [("gx", 1)]


def device_code(gx_size, gy_size):
    code = 0
    for k, (axis, step) in enumerate(exchange_steps(gx_size, gy_size)):
        code = code + jnp.where(lax.axis_index(axis) & step != 0, 1 << k, 0)
    return code


def place_half(blocks_ref, code, src_ref, fsrc_ref):
    devices = blocks_ref.shape[0]
    lane = lax.broadcasted_iota(jnp.int32, (8, 128), 1)
    sub = lax.broadcasted_iota(jnp.int32, (8, 128), 0)
    src_ref[...] = jnp.zeros(src_ref.shape, jnp.float32)
    fsrc_ref[...] = jnp.zeros(fsrc_ref.shape, jnp.float32)

    def place_block(device, carry):
        atoms_before, frames_before, my_atoms, my_frames = carry
        my_atoms = jnp.where(device == code, atoms_before, my_atoms)
        my_frames = jnp.where(device == code, frames_before, my_frames)
        block = jnp.bitwise_xor(code, device)
        frame_count = jnp.max(blocks_ref[block, 7:8, 0:1]).astype(jnp.int32)
        atom_count = jnp.max(blocks_ref[block, 7:8, 1:2]).astype(jnp.int32)
        tile = atoms_before // 128
        turn = atoms_before % 128
        low = pltpu.roll(blocks_ref[block, :, 0:128], turn, 1)
        high = pltpu.roll(blocks_ref[block, :, 128:256], turn, 1)
        inside = lane >= turn
        src_ref[tile] += jnp.where(inside, low, 0.0)
        src_ref[tile + 1] += jnp.where(inside, high, low)
        src_ref[tile + 2] += jnp.where(inside, 0.0, high)
        exists = jnp.where(lane[0:1] < 2, 1.0, blocks_ref[block, 7:8, 0:128])
        last = jnp.broadcast_to(blocks_ref[block, 7:8, 128:256], (8, 128))
        tile = frames_before // 128
        turn = frames_before % 128
        low = pltpu.roll(blocks_ref[block, :, 256:384], turn, 1)
        high = pltpu.roll(jnp.where(sub == 0, last, jnp.broadcast_to(exists, (8, 128))), turn, 1)
        inside = lane >= turn
        fsrc_ref[tile, 0:8] += jnp.where(inside, low, 0.0)
        fsrc_ref[tile, 8:16] += jnp.where(inside, high, 0.0)
        fsrc_ref[tile + 1, 0:8] += jnp.where(inside, 0.0, low)
        fsrc_ref[tile + 1, 8:16] += jnp.where(inside, 0.0, high)
        return (atoms_before + atom_count, frames_before + frame_count, my_atoms, my_frames)

    group = 16
    while devices % group:
        group //= 2

    def place_group(index, carry):
        for k in range(group):
            carry = place_block(index * group + k, carry)
        return carry

    carry = (0, 0, 0, 0)
    if devices == group:
        return place_group(0, carry)
    return lax.fori_loop(0, devices // group, place_group, carry)


def frame_chunks(frame_total):
    return (frame_total + ROW_CHUNK - 1) // ROW_CHUNK


def atom_groups(atom_total):
    width = TILE * TILE_GROUP
    return (atom_total + width - 1) // width


def build_rows(fsrc_ref, lhs_ref, frame_total):
    sub = lax.broadcasted_iota(jnp.int32, (8, 128), 0)

    def build(index, carry):
        for k in range(BUILD_GROUP):
            tile = index * BUILD_GROUP + k
            part = fsrc_ref[tile, 0:8]
            last = fsrc_ref[tile, 8:9]
            exists = fsrc_ref[tile, 9:10]
            a = [part[k : k + 1] for k in range(3)]
            b = [part[3 + k : 4 + k] for k in range(3)]
            cross = [a[2] * b[1] - a[1] * b[2], a[0] * b[2] - a[2] * b[0], a[1] * b[0] - a[0] * b[1]]
            rotations = (part[0:3], part[3:6], jnp.concatenate(cross, axis=0))
            shifts = (part[6:7], part[7:8], last)
            for c in range(3):
                block = jnp.concatenate([rotations[c], rotations[c], shifts[c], exists], axis=0)
                high, middle, low = split_rows(block)
                ones = jnp.broadcast_to(exists, (8, 128))
                stack = [
                    jnp.where((sub >= 3) & (sub < 6), middle, high),
                    jnp.where(sub < 3, low, jnp.where(sub == 6, middle, high)),
                    jnp.where(sub < 3, middle, jnp.where(sub == 6, low, high)),
                ]
                stack = [x if k == c else jnp.where(sub == 7, 0.0, x) for k, x in enumerate(stack)]
                stack.append(jnp.where((sub == c) | (sub == 3 + c), ones, 0.0))
                stack.append(jnp.zeros((96, 128), jnp.float32))
                turned = jnp.concatenate(stack, axis=0).T
                lhs_ref[pl.ds(8 * tile, 8), c] = turned.astype(jnp.bfloat16).reshape(8, 16, 128)
        return carry

    step = 128 * BUILD_GROUP
    groups = (frame_total + step - 1) // step
    lax.fori_loop(0, groups, build, 0)
    rows = ROW_CHUNK // 16
    lhs_ref[pl.ds(groups * (8 * BUILD_GROUP), rows)] = jnp.zeros((rows,) + lhs_ref.shape[1:], jnp.bfloat16)


def build_columns(src_ref, rhs_ref, atom_total):
    per_tile = TILE // 128

    def build(index, carry):
        for k in range(TILE_GROUP):
            tile = index * TILE_GROUP + k
            x = jnp.concatenate([src_ref[tile * per_tile + m] for m in range(per_tile)], axis=1)
            high, middle, low = split_rows(x)
            one = jnp.ones((1, TILE), jnp.float32)
            nil = jnp.zeros((2, TILE), jnp.float32)
            rows = [high[3:6], high[3:6], one, high[0:1], high[3:6], middle[3:6], one, high[1:2]]
            rows += [middle[3:6], low[3:6], one, high[2:3], middle[0:3], low[0:3], nil]
            rhs_ref[tile] = jnp.concatenate(rows, axis=0).astype(jnp.bfloat16)
        return carry

    lax.fori_loop(0, atom_groups(atom_total), build, 0)


def all_pairs(lhs_ref, frame_total, rhs_ref, src_ref, atom_total, col_ref, row_ref=None, before_ref=None):
    row_step = ROW_CHUNK // 16
    per_tile = TILE // 128
    col_ref[...] = jnp.zeros(col_ref.shape, jnp.float32)
    if row_ref is not None:
        behind = pl.multiple_of(frame_chunks(frame_total) * ROW_CHUNK, 8)
        row_ref[pl.ds(behind, 256), :] = jnp.zeros((256, 128), jnp.float32)

    def one_chunk(chunk, carry):
        start = pl.multiple_of(chunk * ROW_CHUNK, 8)
        if row_ref is not None:
            span = pl.ds(start, ROW_CHUNK)
            row_ref[span, :] = jnp.zeros((ROW_CHUNK, 128), jnp.float32) if before_ref is None else before_ref[span, :]

        def one_group(index, carry):
            lhs = lhs_ref[pl.ds(chunk * row_step, row_step)].reshape(3 * ROW_CHUNK, 128)[:, 0:32]
            for pair in range(0, TILE_GROUP, 2):
                tiles = [index * TILE_GROUP + pair + k for k in range(2)]
                dots = [jnp.dot(lhs, rhs_ref[tile], preferred_element_type=jnp.float32) for tile in tiles]
                caps = []
                for tile in tiles:
                    cap = jnp.concatenate([src_ref[tile * per_tile + m, 6:7, :] for m in range(per_tile)], axis=1)
                    caps.append(jnp.broadcast_to(cap * clamp_length, (8, TILE)))
                columns = [None, None]
                for g in range(ROW_CHUNK // 8):
                    base = 48 * (g // 2) + 8 * (g % 2)
                    row_sum = None if row_ref is None else row_ref[pl.ds(start + 8 * g, 8), :]
                    for k in range(2):
                        w0, w1, w2 = (dots[k][base + 16 * c : base + 16 * c + 8] for c in range(3))
                        square = (w0 * w0 + w1 * w1) + (w2 * w2 + eps_square)
                        distance = jnp.minimum(square * lax.rsqrt(square), caps[k])
                        columns[k] = distance if columns[k] is None else columns[k] + distance
                        if row_ref is not None:
                            for m in range(per_tile):
                                row_sum = row_sum + distance[:, 128 * m : 128 * m + 128]
                    if row_ref is not None:
                        row_ref[pl.ds(start + 8 * g, 8), :] = row_sum
                for k, tile in enumerate(tiles):
                    for m in range(per_tile):
                        col_ref[tile * per_tile + m] += columns[k][:, 128 * m : 128 * m + 128]
            return carry

        return lax.fori_loop(0, atom_groups(atom_total), one_group, carry)

    lax.fori_loop(0, frame_chunks(frame_total), one_chunk, 0)


def first_kernel(sizes, blocks_ref, src_ref, rhs_ref, lhs_ref, row_ref, col_ref, info_ref, fsrc_ref):
    code = device_code(*sizes) & (blocks_ref.shape[0] - 1)
    info = place_half(blocks_ref, code, src_ref, fsrc_ref)
    build_rows(fsrc_ref, lhs_ref, info[1])
    build_columns(src_ref, rhs_ref, info[0])
    for k, value in enumerate(info):
        info_ref[k : k + 1, :] = jnp.full((1, 128), value, jnp.int32)
    all_pairs(lhs_ref, info[1], rhs_ref, src_ref, info[0], col_ref, row_ref)


def second_kernel(
    sizes,
    blocks_ref,
    rank_ref,
    src_ref,
    rhs_ref,
    lhs_ref,
    before_ref,
    col_ref,
    info_ref,
    frame_ref,
    atom_ref,
    total_ref,
    far_src_ref,
    far_rhs_ref,
    far_lhs_ref,
    row_ref,
    near_far_ref,
    far_near_ref,
    far_far_ref,
    fsrc_ref,
):
    half = blocks_ref.shape[0]
    frames = frame_ref.shape[1]
    own_atoms = atom_ref.shape[1]
    code = device_code(*sizes)
    atoms, frame_total, my_atoms, my_frames = (jnp.max(info_ref[k : k + 1, 0:1]) for k in range(4))
    far_atoms, far_frames, _, _ = place_half(blocks_ref, code & (half - 1), far_src_ref, fsrc_ref)
    build_rows(fsrc_ref, far_lhs_ref, far_frames)
    build_columns(far_src_ref, far_rhs_ref, far_atoms)
    all_pairs(lhs_ref, frame_total, far_rhs_ref, far_src_ref, far_atoms, near_far_ref, row_ref, before_ref)
    all_pairs(far_lhs_ref, far_frames, rhs_ref, src_ref, atoms, far_near_ref)
    all_pairs(far_lhs_ref, far_frames, far_rhs_ref, far_src_ref, far_atoms, far_far_ref)

    lane = lax.broadcasted_iota(jnp.int32, (8, 128), 1)
    idle = (frame_chunks(frame_total) * ROW_CHUNK - frame_total).astype(jnp.float32)
    far_idle = (frame_chunks(far_frames) * ROW_CHUNK - far_frames).astype(jnp.float32)
    least = jnp.full((1, 128), eps_square, jnp.float32)
    least = least * lax.rsqrt(least)

    def half_sums(atom_total, atoms_ref, first_ref, second_ref):
        def add_group(index, carry):
            first, second, floor = carry
            per_group = TILE // 128 * TILE_GROUP
            for k in range(per_group):
                tile = index * per_group + k
                first = first + first_ref[tile]
                second = second + second_ref[tile]
                floor = floor + jnp.minimum(least, atoms_ref[tile, 6:7, :] * clamp_length)
            return first, second, floor

        empty = jnp.zeros((8, 128), jnp.float32)
        carry = (empty, empty, jnp.zeros((1, 128), jnp.float32))
        first, second, floor = lax.fori_loop(0, atom_groups(atom_total), add_group, carry)
        first = jnp.sum(first, axis=0, keepdims=True) - idle * floor
        return first, jnp.sum(second, axis=0, keepdims=True) - far_idle * floor

    near_near, far_near = half_sums(atoms, src_ref, col_ref, far_near_ref)
    near_far, far_far = half_sums(far_atoms, far_src_ref, near_far_ref, far_far_ref)
    upper = code >= half
    loss = jnp.where(upper, far_far, near_near) + jnp.where(upper, far_near, near_far)
    loss = loss + (jnp.where(upper, near_far, far_near) + jnp.where(upper, near_near, far_far))
    loss = jnp.sum(loss, axis=1, keepdims=True)
    atom_number = (atoms + far_atoms).astype(jnp.float32)
    frame_number = (frame_total + far_frames).astype(jnp.float32)
    scale = 1.0 / clamp_length
    total_ref[...] = loss * scale / (frame_number * atom_number)

    tile = my_atoms // 128
    turn = my_atoms % 128
    pieces = []
    for k in range(3):
        cap = src_ref[tile + k, 6:7, :] * clamp_length
        sums = jnp.sum(col_ref[tile + k] + far_near_ref[tile + k], axis=0, keepdims=True)
        sums = sums - (idle + far_idle) * jnp.minimum(least, cap)
        pieces.append(pltpu.roll(jnp.broadcast_to(sums, (8, 128)), (128 - turn) % 128, 1))
    keep = lane < 128 - turn
    mine = jnp.concatenate([jnp.where(keep, pieces[k], pieces[k + 1]) for k in range(2)], axis=1)
    mine = exact_dot(mine, one_hot(rank_ref[0:1, :]), 0)[0:1]
    atom_ref[...] = mine[:, :own_atoms] * scale / frame_number

    tile = my_frames // 128
    turn = my_frames % 128
    pieces = []
    for k in range(2):
        rows = row_ref[pl.ds(pl.multiple_of((tile + k) * 128, 128), 128), :]
        sums = jnp.sum(rows.T, axis=0, keepdims=True)
        pieces.append(pltpu.roll(jnp.broadcast_to(sums, (8, 128)), (128 - turn) % 128, 1))
    mine = jnp.where(lane < 128 - turn, pieces[0], pieces[1])
    mine = exact_dot(mine, one_hot(rank_ref[1:2, 0:frames]), 0)[0:1]
    frame_ref[...] = mine * scale / atom_number


def shards(pred_frames, true_frames, pred_atoms, true_atoms, atom_mask, residue_types, swap_flags):
    devices = lax.axis_size("gx") * lax.axis_size("gy")
    frames = pred_frames.shape[1]
    own_atoms = pred_atoms.shape[1]
    lanes = -(-own_atoms // 128) * 128
    f32 = jnp.float32
    inputs = (residue_types, swap_flags, pred_frames, true_frames, pred_atoms, true_atoms)
    inputs += (atom_mask.reshape(1, own_atoms),)
    blocks, ranks = pl.pallas_call(
        prep_kernel,
        out_shape=(
            jax.ShapeDtypeStruct((1, 8, lanes + frames), f32),
            jax.ShapeDtypeStruct((8, lanes), jnp.int32),
        ),
        in_specs=[HBM] * 7,
        out_specs=(VMEM, VMEM),
        scratch_shapes=[
            pltpu.SMEM(residue_types.shape, jnp.int32),
            pltpu.SMEM(swap_flags.shape, jnp.int32),
            pltpu.VMEM(pred_frames.shape, f32),
            pltpu.VMEM(true_frames.shape, f32),
            pltpu.VMEM(pred_atoms.shape, f32),
            pltpu.VMEM(true_atoms.shape, f32),
            pltpu.VMEM((1, own_atoms), jnp.int32),
            pltpu.VMEM((8, lanes), f32),
            pltpu.SemaphoreType.DMA((7,)),
        ],
        compiler_params=pltpu.CompilerParams(vmem_limit_bytes=8 << 20),
        name="prep",
    )(*[pltpu.with_memory_space_constraint(x, pltpu.HBM) for x in inputs])
    sizes = (lax.axis_size("gx"), lax.axis_size("gy"))
    far = None
    for axis, step in exchange_steps(*sizes):
        if far is not None:
            blocks = jnp.concatenate([blocks, far], axis=0)
        far = lax.ppermute(blocks, axis, [(i, i ^ step) for i in range(lax.axis_size(axis))])
    half = devices // 2
    groups = -(-(half * own_atoms + 256) // (TILE * TILE_GROUP))
    tiles = groups * TILE_GROUP * (TILE // 128)
    most = half * (frames * USED_SLOTS // FRAME_SLOTS)
    frame_tiles = -(-most // (128 * BUILD_GROUP)) * BUILD_GROUP + 1
    row_groups = 8 * frame_tiles + 2 * (ROW_CHUNK // 16) + 16
    columns = ((tiles, 8, 128), f32)
    frame_source = ((frame_tiles, 16, 128), f32)
    right = ((groups * TILE_GROUP, 32, TILE), jnp.bfloat16)
    left = ((row_groups, 3, 16, 128), jnp.bfloat16)
    rows = ((row_groups * 16, 128), f32)

    def room(*arrays):
        return sum(jnp.dtype(d).itemsize * functools.reduce(lambda a, b: a * b, shape) for shape, d in arrays)

    kept = [columns, right, left, rows, columns, ((8, 128), jnp.int32)]
    near = pl.pallas_call(
        functools.partial(first_kernel, sizes),
        out_shape=[jax.ShapeDtypeStruct(*x) for x in kept],
        in_specs=[VMEM],
        out_specs=[VMEM] * len(kept),
        scratch_shapes=[pltpu.VMEM(*frame_source)],
        compiler_params=pltpu.CompilerParams(vmem_limit_bytes=room(*kept, frame_source) + (8 << 20)),
        cost_estimate=pl.CostEstimate(flops=4 * 10**9, bytes_accessed=1 << 20, transcendentals=0),
        name="near",
    )(blocks)
    scratch = [columns, right, left, rows, columns, columns, columns, frame_source]
    frame_loss, atom_loss, total_loss = pl.pallas_call(
        functools.partial(second_kernel, sizes),
        out_shape=(
            jax.ShapeDtypeStruct((1, frames), f32),
            jax.ShapeDtypeStruct((1, own_atoms), f32),
            jax.ShapeDtypeStruct((1, 1), f32),
        ),
        in_specs=[VMEM] * (2 + len(kept)),
        out_specs=(VMEM, VMEM, VMEM),
        scratch_shapes=[pltpu.VMEM(*x) for x in scratch],
        compiler_params=pltpu.CompilerParams(vmem_limit_bytes=room(*kept, *scratch) + (8 << 20)),
        name="rest",
    )(far, ranks, *near)
    return (frame_loss.reshape(frames), atom_loss.reshape(own_atoms), total_loss.reshape(1))


def solution(mesh):
    both = P(None, ("sa", "gx", "gy"))
    flat = P(("sa", "gx", "gy"))
    return jax.shard_map(
        shards,
        mesh=mesh,
        in_specs=(both, both, both, both, flat, flat, flat),
        out_specs=(flat, flat, P("sa")),
        check_vma=False,
    )
```

```python
import functools

import jax
import jax.numpy as jnp
from jax import lax
from jax.experimental import pallas as pl
from jax.experimental.pallas import tpu as pltpu
from jax.sharding import PartitionSpec as P

eps_square = 0.0001
clamp_length = 10.0

ATOM_COUNTS = (5, 11, 8, 8, 6, 9, 9, 4, 10, 8, 8, 9, 8, 11, 7, 6, 7, 14, 12, 7)
CHI_COUNTS = (0, 4, 2, 2, 1, 3, 3, 0, 2, 2, 2, 4, 3, 2, 2, 1, 1, 2, 2, 1)
FRAME_SLOTS = 8
USED_SLOTS = 6
BUILD_GROUP = 4
ATOM_SLOTS = 14
ROW_CHUNK = 544
TILE = 256
TILE_GROUP = 4
VMEM = pl.BlockSpec(memory_space=pltpu.VMEM)
HBM = pl.BlockSpec(memory_space=pltpu.HBM)


def spread_residues(scalars, positions, width):
    value = jnp.full(positions.shape, scalars[0], jnp.int32)
    first = jnp.zeros(positions.shape, jnp.int32)
    for residue in range(1, len(scalars)):
        here = positions >= residue * width
        value = jnp.where(here, scalars[residue], value)
        first = jnp.where(here, residue * width, first)
    return value, positions - first


def table_lookup(types, table):
    value = jnp.full(types.shape, table[0], jnp.int32)
    for kind in range(1, len(table)):
        if table[kind] != table[0]:
            value = jnp.where(types == kind, table[kind], value)
    return value


def split_rows(x):
    high = x.astype(jnp.bfloat16).astype(jnp.float32)
    rest = x - high
    middle = rest.astype(jnp.bfloat16).astype(jnp.float32)
    return high, middle, rest - middle


def one_hot(rank):
    size = rank.shape[1]
    place = lax.broadcasted_iota(jnp.int32, (size, size), 0)
    return jnp.where(place == rank, 1.0, 0.0).astype(jnp.bfloat16)


def exact_dot(x, selection, contract):
    rows = x.shape[0]
    parts = jnp.concatenate(split_rows(x), axis=0).astype(jnp.bfloat16)
    out = lax.dot_general(parts, selection, (((1,), (contract,)), ((), ())), preferred_element_type=jnp.float32)
    return out[:rows] + out[rows : 2 * rows] + out[2 * rows :]


def prep_kernel(*refs):
    inputs, (block_ref, rank_ref), scratch = refs[:7], refs[7:9], refs[9:]
    (types_ref, flags_ref, pf_ref, tf_ref, pa_ref, ta_ref, mask_ref, pad_ref, sems) = scratch
    fetches = [pltpu.make_async_copy(src, dst, sems.at[i]) for i, (src, dst) in enumerate(zip(inputs, scratch))]
    for fetch in fetches:
        fetch.start()
    residues = types_ref.shape[0]
    frames = pf_ref.shape[1]
    own_atoms = pa_ref.shape[1]
    lanes = pad_ref.shape[1]
    pad_ref[...] = jnp.zeros(pad_ref.shape, jnp.float32)
    for fetch in fetches:
        fetch.wait()
    codes = [types_ref[r] + 32 * flags_ref[r] for r in range(residues)]

    pad_ref[0:3, 0:own_atoms] = pa_ref[...]
    pad_ref[3:6, 0:own_atoms] = ta_ref[...]
    pad_ref[6:7, 0:own_atoms] = mask_ref[...].astype(jnp.float32)
    atoms = pad_ref[...]
    place = lax.broadcasted_iota(jnp.int32, (1, lanes), 1)
    code, slot = spread_residues(codes, place, ATOM_SLOTS)
    types = code & 31
    swapped = code >= 32
    twice = (types == 13) | (types == 18)

    def opens_pair(s):
        pair = ((s == 6) & ((types == 3) | twice)) | ((s == 7) & (types == 6)) | ((s == 8) & twice)
        return swapped & pair

    after = jnp.where(opens_pair(slot), 1, 0)
    before = jnp.where(opens_pair(slot - 1), 1, 0)
    row = lax.broadcasted_iota(jnp.int32, (8, lanes), 0)
    renamed = jnp.where(
        jnp.broadcast_to(after, (8, lanes)) == 1,
        pltpu.roll(atoms, lanes - 1, 1),
        jnp.where(jnp.broadcast_to(before, (8, lanes)) == 1, pltpu.roll(atoms, 1, 1), atoms),
    )
    atoms = jnp.where(row < 3, atoms, renamed)
    real = (slot < table_lookup(types, ATOM_COUNTS)) & (place < own_atoms)
    real = jnp.broadcast_to(jnp.where(real, 1, 0), (8, lanes)) == 1
    atoms = jnp.where((row == 6) & ~real, 0.0, atoms)
    weight = atoms[6:7]
    earlier = lax.broadcasted_iota(jnp.int32, (lanes, lanes), 0) < lax.broadcasted_iota(jnp.int32, (lanes, lanes), 1)
    earlier = jnp.where(earlier, 1.0, 0.0).astype(jnp.bfloat16)
    rank = jnp.dot(
        jnp.broadcast_to(weight, (16, lanes)).astype(jnp.bfloat16), earlier, preferred_element_type=jnp.float32
    )[0:1]
    atom_rank = jnp.where(weight > 0.5, rank, -1.0).astype(jnp.int32)
    atom_count = jnp.sum(weight, axis=1, keepdims=True)

    place = lax.broadcasted_iota(jnp.int32, (1, frames), 1)
    code, slot = spread_residues(codes, place, FRAME_SLOTS)
    types = code & 31
    swapped = code >= 32
    chi = table_lookup(types, CHI_COUNTS)
    exists = (slot == 0) | (slot == 3) | ((slot >= 4) & (slot - 3 <= chi))
    exists = jnp.where(exists, 1.0, 0.0)
    half_turn = ((types == 3) | (types == 13) | (types == 18)) & (slot == 5)
    half_turn = swapped & (half_turn | ((types == 6) & (slot == 6)))
    sign = jnp.where(half_turn, -1.0, 1.0)
    rot_pred = [[pf_ref[pl.ds(3 * a + c, 1), :] for c in range(3)] for a in range(3)]
    rot_true = [[tf_ref[pl.ds(3 * a + c, 1), :] for c in range(3)] for a in range(3)]
    rot_true = [[r[0], r[1] * sign, r[2] * sign] for r in rot_true]
    rows = []
    shifts = []
    for a in range(3):
        rel = [
            rot_pred[a][0] * rot_true[b][0] + rot_pred[a][1] * rot_true[b][1] + rot_pred[a][2] * rot_true[b][2]
            for b in range(3)
        ]
        shift = rel[0] * tf_ref[9:10, :] + rel[1] * tf_ref[10:11, :] + rel[2] * tf_ref[11:12, :]
        shifts.append(shift - pf_ref[pl.ds(9 + a, 1), :])
        if a < 2:
            rows += [-rel[0], -rel[1], -rel[2]]
    rows += shifts + [exists]
    rows += [jnp.zeros((16 - len(rows), frames), jnp.float32)]
    rank = jnp.dot(
        jnp.broadcast_to(exists, (16, frames)).astype(jnp.bfloat16),
        earlier[:frames, :frames],
        preferred_element_type=jnp.float32,
    )[0:1]
    frame_rank = jnp.where(exists > 0.5, rank, -1.0).astype(jnp.int32)
    frame_count = jnp.sum(exists, axis=1, keepdims=True)

    atoms = exact_dot(atoms, one_hot(atom_rank), 1)
    packed = exact_dot(jnp.concatenate(rows, axis=0), one_hot(frame_rank), 1)
    first = jnp.where(place == 0, frame_count, jnp.where(place == 1, atom_count, packed[9:10]))
    extra = jnp.concatenate([first, packed[8:9]], axis=1)
    atoms = jnp.where(row == 7, jnp.broadcast_to(extra, (8, lanes)), atoms)
    block = jnp.concatenate([atoms, packed[0:8]], axis=1)
    block_ref[0] = block
    rank_ref[...] = jnp.zeros(rank_ref.shape, jnp.int32)
    rank_ref[0:1, :] = atom_rank
    rank_ref[1:2, 0:frames] = frame_rank


def exchange_steps(gx_size, gy_size):
    steps = [("gy", 1 << k) for k in range(gy_size.bit_length() - 1)]
    steps += [("gx", 1 << k) for k in range(1, gx_size.bit_length() - 1)]
    return steps + [("gx", 1)]


def device_code(gx_size, gy_size):
    code = 0
    for k, (axis, step) in enumerate(exchange_steps(gx_size, gy_size)):
        code = code + jnp.where(lax.axis_index(axis) & step != 0, 1 << k, 0)
    return code


def place_half(blocks_ref, code, src_ref, fsrc_ref):
    devices = blocks_ref.shape[0]
    lane = lax.broadcasted_iota(jnp.int32, (8, 128), 1)
    sub = lax.broadcasted_iota(jnp.int32, (8, 128), 0)
    src_ref[...] = jnp.zeros(src_ref.shape, jnp.float32)
    fsrc_ref[...] = jnp.zeros(fsrc_ref.shape, jnp.float32)

    def place_block(device, carry):
        atoms_before, frames_before, my_atoms, my_frames = carry
        my_atoms = jnp.where(device == code, atoms_before, my_atoms)
        my_frames = jnp.where(device == code, frames_before, my_frames)
        block = jnp.bitwise_xor(code, device)
        frame_count = jnp.max(blocks_ref[block, 7:8, 0:1]).astype(jnp.int32)
        atom_count = jnp.max(blocks_ref[block, 7:8, 1:2]).astype(jnp.int32)
        tile = atoms_before // 128
        turn = atoms_before % 128
        low = pltpu.roll(blocks_ref[block, :, 0:128], turn, 1)
        high = pltpu.roll(blocks_ref[block, :, 128:256], turn, 1)
        inside = lane >= turn
        src_ref[tile] += jnp.where(inside, low, 0.0)
        src_ref[tile + 1] += jnp.where(inside, high, low)
        src_ref[tile + 2] += jnp.where(inside, 0.0, high)
        exists = jnp.where(lane[0:1] < 2, 1.0, blocks_ref[block, 7:8, 0:128])
        last = jnp.broadcast_to(blocks_ref[block, 7:8, 128:256], (8, 128))
        tile = frames_before // 128
        turn = frames_before % 128
        low = pltpu.roll(blocks_ref[block, :, 256:384], turn, 1)
        high = pltpu.roll(jnp.where(sub == 0, last, jnp.broadcast_to(exists, (8, 128))), turn, 1)
        inside = lane >= turn
        fsrc_ref[tile, 0:8] += jnp.where(inside, low, 0.0)
        fsrc_ref[tile, 8:16] += jnp.where(inside, high, 0.0)
        fsrc_ref[tile + 1, 0:8] += jnp.where(inside, 0.0, low)
        fsrc_ref[tile + 1, 8:16] += jnp.where(inside, 0.0, high)
        return (atoms_before + atom_count, frames_before + frame_count, my_atoms, my_frames)

    group = 16
    while devices % group:
        group //= 2

    def place_group(index, carry):
        for k in range(group):
            carry = place_block(index * group + k, carry)
        return carry

    carry = (0, 0, 0, 0)
    if devices == group:
        return place_group(0, carry)
    return lax.fori_loop(0, devices // group, place_group, carry)


def frame_chunks(frame_total):
    return (frame_total + ROW_CHUNK - 1) // ROW_CHUNK


def atom_groups(atom_total):
    width = TILE * TILE_GROUP
    return (atom_total + width - 1) // width


def build_rows(fsrc_ref, lhs_ref, frame_total):
    sub = lax.broadcasted_iota(jnp.int32, (8, 128), 0)

    def build(index, carry):
        for k in range(BUILD_GROUP):
            tile = index * BUILD_GROUP + k
            part = fsrc_ref[tile, 0:8]
            last = fsrc_ref[tile, 8:9]
            exists = fsrc_ref[tile, 9:10]
            a = [part[k : k + 1] for k in range(3)]
            b = [part[3 + k : 4 + k] for k in range(3)]
            cross = [a[2] * b[1] - a[1] * b[2], a[0] * b[2] - a[2] * b[0], a[1] * b[0] - a[0] * b[1]]
            rotations = (part[0:3], part[3:6], jnp.concatenate(cross, axis=0))
            shifts = (part[6:7], part[7:8], last)
            for c in range(3):
                block = jnp.concatenate([rotations[c], rotations[c], shifts[c], exists], axis=0)
                high, middle, low = split_rows(block)
                ones = jnp.broadcast_to(exists, (8, 128))
                stack = [
                    jnp.where((sub >= 3) & (sub < 6), middle, high),
                    jnp.where(sub < 3, low, jnp.where(sub == 6, middle, high)),
                    jnp.where(sub < 3, middle, jnp.where(sub == 6, low, high)),
                ]
                stack = [x if k == c else jnp.where(sub == 7, 0.0, x) for k, x in enumerate(stack)]
                stack.append(jnp.where((sub == c) | (sub == 3 + c), ones, 0.0))
                stack.append(jnp.zeros((96, 128), jnp.float32))
                turned = jnp.concatenate(stack, axis=0).T
                lhs_ref[pl.ds(8 * tile, 8), c] = turned.astype(jnp.bfloat16).reshape(8, 16, 128)
        return carry

    step = 128 * BUILD_GROUP
    groups = (frame_total + step - 1) // step
    lax.fori_loop(0, groups, build, 0)
    rows = ROW_CHUNK // 16
    lhs_ref[pl.ds(groups * (8 * BUILD_GROUP), rows)] = jnp.zeros((rows,) + lhs_ref.shape[1:], jnp.bfloat16)


def build_columns(src_ref, rhs_ref, atom_total):
    per_tile = TILE // 128

    def build(index, carry):
        for k in range(TILE_GROUP):
            tile = index * TILE_GROUP + k
            x = jnp.concatenate([src_ref[tile * per_tile + m] for m in range(per_tile)], axis=1)
            high, middle, low = split_rows(x)
            one = jnp.ones((1, TILE), jnp.float32)
            nil = jnp.zeros((2, TILE), jnp.float32)
            rows = [high[3:6], high[3:6], one, high[0:1], high[3:6], middle[3:6], one, high[1:2]]
            rows += [middle[3:6], low[3:6], one, high[2:3], middle[0:3], low[0:3], nil]
            rhs_ref[tile] = jnp.concatenate(rows, axis=0).astype(jnp.bfloat16)
        return carry

    lax.fori_loop(0, atom_groups(atom_total), build, 0)


def all_pairs(lhs_ref, frame_total, rhs_ref, src_ref, atom_total, col_ref, row_ref=None, before_ref=None):
    row_step = ROW_CHUNK // 16
    per_tile = TILE // 128
    col_ref[...] = jnp.zeros(col_ref.shape, jnp.float32)
    if row_ref is not None:
        behind = pl.multiple_of(frame_chunks(frame_total) * ROW_CHUNK, 8)
        row_ref[pl.ds(behind, 256), :] = jnp.zeros((256, 128), jnp.float32)

    def one_chunk(chunk, carry):
        start = pl.multiple_of(chunk * ROW_CHUNK, 8)
        if row_ref is not None:
            span = pl.ds(start, ROW_CHUNK)
            row_ref[span, :] = jnp.zeros((ROW_CHUNK, 128), jnp.float32) if before_ref is None else before_ref[span, :]

        def one_group(index, carry):
            lhs = lhs_ref[pl.ds(chunk * row_step, row_step)].reshape(3 * ROW_CHUNK, 128)[:, 0:32]
            for pair in range(0, TILE_GROUP, 2):
                tiles = [index * TILE_GROUP + pair + k for k in range(2)]
                dots = [jnp.dot(lhs, rhs_ref[tile], preferred_element_type=jnp.float32) for tile in tiles]
                caps = []
                for tile in tiles:
                    cap = jnp.concatenate([src_ref[tile * per_tile + m, 6:7, :] for m in range(per_tile)], axis=1)
                    caps.append(jnp.broadcast_to(cap * clamp_length, (8, TILE)))
                columns = [None, None]
                for g in range(ROW_CHUNK // 8):
                    base = 48 * (g // 2) + 8 * (g % 2)
                    row_sum = None if row_ref is None else row_ref[pl.ds(start + 8 * g, 8), :]
                    for k in range(2):
                        w0, w1, w2 = (dots[k][base + 16 * c : base + 16 * c + 8] for c in range(3))
                        square = (w0 * w0 + w1 * w1) + (w2 * w2 + eps_square)
                        distance = jnp.minimum(square * lax.rsqrt(square), caps[k])
                        columns[k] = distance if columns[k] is None else columns[k] + distance
                        if row_ref is not None:
                            for m in range(per_tile):
                                row_sum = row_sum + distance[:, 128 * m : 128 * m + 128]
                    if row_ref is not None:
                        row_ref[pl.ds(start + 8 * g, 8), :] = row_sum
                for k, tile in enumerate(tiles):
                    for m in range(per_tile):
                        col_ref[tile * per_tile + m] += columns[k][:, 128 * m : 128 * m + 128]
            return carry

        return lax.fori_loop(0, atom_groups(atom_total), one_group, carry)

    lax.fori_loop(0, frame_chunks(frame_total), one_chunk, 0)


def idle_rows(frame_total):
    return (frame_chunks(frame_total) * ROW_CHUNK - frame_total).astype(jnp.float32)


def least_distance():
    square = jnp.full((1, 128), eps_square, jnp.float32)
    return square * lax.rsqrt(square)


def column_total(atom_total, src_ref, col_ref, idle):
    def add_group(index, carry):
        sums, floor = carry
        per_group = TILE // 128 * TILE_GROUP
        for k in range(per_group):
            tile = index * per_group + k
            sums = sums + col_ref[tile]
            floor = floor + jnp.minimum(least_distance(), src_ref[tile, 6:7, :] * clamp_length)
        return sums, floor

    carry = (jnp.zeros((8, 128), jnp.float32), jnp.zeros((1, 128), jnp.float32))
    sums, floor = lax.fori_loop(0, atom_groups(atom_total), add_group, carry)
    return jnp.sum(sums, axis=0, keepdims=True) - idle * floor


def first_kernel(sizes, blocks_ref, loss_ref, src_ref, rhs_ref, lhs_ref, row_ref, col_ref, info_ref, fsrc_ref):
    code = device_code(*sizes) & (blocks_ref.shape[0] - 1)
    info = place_half(blocks_ref, code, src_ref, fsrc_ref)
    build_rows(fsrc_ref, lhs_ref, info[1])
    build_columns(src_ref, rhs_ref, info[0])
    for k, value in enumerate(info):
        info_ref[k : k + 1, :] = jnp.full((1, 128), value, jnp.int32)
    all_pairs(lhs_ref, info[1], rhs_ref, src_ref, info[0], col_ref, row_ref)
    loss = column_total(info[0], src_ref, col_ref, idle_rows(info[1]))
    loss_ref[...] = jnp.broadcast_to(loss, loss_ref.shape)


def second_kernel(
    sizes,
    blocks_ref,
    rank_ref,
    src_ref,
    rhs_ref,
    lhs_ref,
    before_ref,
    col_ref,
    info_ref,
    frame_ref,
    atom_ref,
    cross_ref,
    far_src_ref,
    far_rhs_ref,
    far_lhs_ref,
    row_ref,
    near_far_ref,
    far_near_ref,
    fsrc_ref,
):
    half = blocks_ref.shape[0]
    frames = frame_ref.shape[1]
    own_atoms = atom_ref.shape[1]
    code = device_code(*sizes)
    atoms, frame_total, my_atoms, my_frames = (jnp.max(info_ref[k : k + 1, 0:1]) for k in range(4))
    far_atoms, far_frames, _, _ = place_half(blocks_ref, code & (half - 1), far_src_ref, fsrc_ref)
    build_rows(fsrc_ref, far_lhs_ref, far_frames)
    build_columns(far_src_ref, far_rhs_ref, far_atoms)
    all_pairs(lhs_ref, frame_total, far_rhs_ref, far_src_ref, far_atoms, near_far_ref, row_ref, before_ref)
    all_pairs(far_lhs_ref, far_frames, rhs_ref, src_ref, atoms, far_near_ref)

    lane = lax.broadcasted_iota(jnp.int32, (8, 128), 1)
    idle = idle_rows(frame_total)
    far_idle = idle_rows(far_frames)
    least = least_distance()
    near_far = column_total(far_atoms, far_src_ref, near_far_ref, idle)
    far_near = column_total(atoms, src_ref, far_near_ref, far_idle)
    atom_number = (atoms + far_atoms).astype(jnp.float32)
    frame_number = (frame_total + far_frames).astype(jnp.float32)
    scale = 1.0 / clamp_length
    upper = code >= half
    cross_ref[0:1, :] = jnp.where(upper, far_near, near_far)
    cross_ref[1:2, :] = jnp.where(upper, near_far, far_near)
    cross_ref[2:3, :] = jnp.full((1, 128), scale, jnp.float32) / (frame_number * atom_number)

    tile = my_atoms // 128
    turn = my_atoms % 128
    pieces = []
    for k in range(3):
        cap = src_ref[tile + k, 6:7, :] * clamp_length
        sums = jnp.sum(col_ref[tile + k] + far_near_ref[tile + k], axis=0, keepdims=True)
        sums = sums - (idle + far_idle) * jnp.minimum(least, cap)
        pieces.append(pltpu.roll(jnp.broadcast_to(sums, (8, 128)), (128 - turn) % 128, 1))
    keep = lane < 128 - turn
    mine = jnp.concatenate([jnp.where(keep, pieces[k], pieces[k + 1]) for k in range(2)], axis=1)
    mine = exact_dot(mine, one_hot(rank_ref[0:1, :]), 0)[0:1]
    atom_ref[...] = mine[:, :own_atoms] * scale / frame_number

    tile = my_frames // 128
    turn = my_frames % 128
    pieces = []
    for k in range(2):
        rows = row_ref[pl.ds(pl.multiple_of((tile + k) * 128, 128), 128), :]
        sums = jnp.sum(rows.T, axis=0, keepdims=True)
        pieces.append(pltpu.roll(jnp.broadcast_to(sums, (8, 128)), (128 - turn) % 128, 1))
    mine = jnp.where(lane < 128 - turn, pieces[0], pieces[1])
    mine = exact_dot(mine, one_hot(rank_ref[1:2, 0:frames]), 0)[0:1]
    frame_ref[...] = mine * scale / atom_number


def finish_kernel(sizes, near_ref, far_ref, cross_ref, frames_ref, atoms_ref, frame_ref, atom_ref, total_ref):
    upper = (device_code(*sizes) * 2) // (sizes[0] * sizes[1]) == 1
    near = near_ref[0:1, :]
    far = far_ref[0:1, :]
    loss = jnp.where(upper, far, near) + cross_ref[0:1, :]
    loss = loss + (cross_ref[1:2, :] + jnp.where(upper, near, far))
    total_ref[...] = jnp.sum(loss, axis=1, keepdims=True) * cross_ref[2:3, 0:1]
    frame_ref[...] = frames_ref[...]
    atom_ref[...] = atoms_ref[...]


def shards(pred_frames, true_frames, pred_atoms, true_atoms, atom_mask, residue_types, swap_flags):
    devices = lax.axis_size("gx") * lax.axis_size("gy")
    frames = pred_frames.shape[1]
    own_atoms = pred_atoms.shape[1]
    lanes = -(-own_atoms // 128) * 128
    f32 = jnp.float32
    inputs = (residue_types, swap_flags, pred_frames, true_frames, pred_atoms, true_atoms)
    inputs += (atom_mask.reshape(1, own_atoms),)
    blocks, ranks = pl.pallas_call(
        prep_kernel,
        out_shape=(
            jax.ShapeDtypeStruct((1, 8, lanes + frames), f32),
            jax.ShapeDtypeStruct((8, lanes), jnp.int32),
        ),
        in_specs=[HBM] * 7,
        out_specs=(VMEM, VMEM),
        scratch_shapes=[
            pltpu.SMEM(residue_types.shape, jnp.int32),
            pltpu.SMEM(swap_flags.shape, jnp.int32),
            pltpu.VMEM(pred_frames.shape, f32),
            pltpu.VMEM(true_frames.shape, f32),
            pltpu.VMEM(pred_atoms.shape, f32),
            pltpu.VMEM(true_atoms.shape, f32),
            pltpu.VMEM((1, own_atoms), jnp.int32),
            pltpu.VMEM((8, lanes), f32),
            pltpu.SemaphoreType.DMA((7,)),
        ],
        compiler_params=pltpu.CompilerParams(vmem_limit_bytes=8 << 20),
        name="prep",
    )(*[pltpu.with_memory_space_constraint(x, pltpu.HBM) for x in inputs])
    sizes = (lax.axis_size("gx"), lax.axis_size("gy"))
    far = None
    for axis, step in exchange_steps(*sizes):
        if far is not None:
            blocks = jnp.concatenate([blocks, far], axis=0)
        far = lax.ppermute(blocks, axis, [(i, i ^ step) for i in range(lax.axis_size(axis))])
    half = devices // 2
    groups = -(-(half * own_atoms + 256) // (TILE * TILE_GROUP))
    tiles = groups * TILE_GROUP * (TILE // 128)
    most = half * (frames * USED_SLOTS // FRAME_SLOTS)
    frame_tiles = -(-most // (128 * BUILD_GROUP)) * BUILD_GROUP + 1
    row_groups = 8 * frame_tiles + 2 * (ROW_CHUNK // 16) + 16
    columns = ((tiles, 8, 128), f32)
    frame_source = ((frame_tiles, 16, 128), f32)
    right = ((groups * TILE_GROUP, 32, TILE), jnp.bfloat16)
    left = ((row_groups, 3, 16, 128), jnp.bfloat16)
    rows = ((row_groups * 16, 128), f32)

    def room(*arrays):
        return sum(jnp.dtype(d).itemsize * functools.reduce(lambda a, b: a * b, shape) for shape, d in arrays)

    kept = [((8, 128), f32), columns, right, left, rows, columns, ((8, 128), jnp.int32)]
    loss, *near = pl.pallas_call(
        functools.partial(first_kernel, sizes),
        out_shape=[jax.ShapeDtypeStruct(*x) for x in kept],
        in_specs=[VMEM],
        out_specs=[VMEM] * len(kept),
        scratch_shapes=[pltpu.VMEM(*frame_source)],
        compiler_params=pltpu.CompilerParams(vmem_limit_bytes=room(*kept, frame_source) + (8 << 20)),
        cost_estimate=pl.CostEstimate(flops=4 * 10**9, bytes_accessed=1 << 20, transcendentals=0),
        name="near",
    )(blocks)
    far_loss = lax.ppermute(loss, axis, [(i, i ^ step) for i in range(lax.axis_size(axis))])
    scratch = [columns, right, left, rows, columns, columns, frame_source]
    results = [((1, frames), f32), ((1, own_atoms), f32)]
    frame_loss, atom_loss, cross = pl.pallas_call(
        functools.partial(second_kernel, sizes),
        out_shape=[jax.ShapeDtypeStruct(*x) for x in results + [((8, 128), f32)]],
        in_specs=[VMEM] * (1 + len(kept)),
        out_specs=[VMEM] * 3,
        scratch_shapes=[pltpu.VMEM(*x) for x in scratch],
        compiler_params=pltpu.CompilerParams(vmem_limit_bytes=room(*kept, *scratch) + (8 << 20)),
        cost_estimate=pl.CostEstimate(flops=8 * 10**9, bytes_accessed=1 << 20, transcendentals=0),
        name="rest",
    )(far, ranks, *near)
    frame_loss, atom_loss, total_loss = pl.pallas_call(
        functools.partial(finish_kernel, sizes),
        out_shape=[jax.ShapeDtypeStruct(*x) for x in results + [((1, 1), f32)]],
        in_specs=[VMEM] * 5,
        out_specs=[VMEM] * 3,
        compiler_params=pltpu.CompilerParams(vmem_limit_bytes=8 << 20),
        name="finish",
    )(loss, far_loss, cross, frame_loss, atom_loss)
    return (frame_loss.reshape(frames), atom_loss.reshape(own_atoms), total_loss.reshape(1))


def solution(mesh):
    both = P(None, ("sa", "gx", "gy"))
    flat = P(("sa", "gx", "gy"))
    return jax.shard_map(
        shards,
        mesh=mesh,
        in_specs=(both, both, both, both, flat, flat, flat),
        out_specs=(flat, flat, P("sa")),
        check_vma=False,
    )
```

```python
import functools

import jax
import jax.numpy as jnp
from jax import lax
from jax.experimental import pallas as pl
from jax.experimental.pallas import tpu as pltpu
from jax.sharding import PartitionSpec as P

eps_square = 0.0001
clamp_length = 10.0

ATOM_COUNTS = (5, 11, 8, 8, 6, 9, 9, 4, 10, 8, 8, 9, 8, 11, 7, 6, 7, 14, 12, 7)
CHI_COUNTS = (0, 4, 2, 2, 1, 3, 3, 0, 2, 2, 2, 4, 3, 2, 2, 1, 1, 2, 2, 1)
FRAME_SLOTS = 8
USED_SLOTS = 6
BUILD_GROUP = 4
ATOM_SLOTS = 14
ROW_CHUNK = 544
TILE = 256
TILE_GROUP = 4
VMEM = pl.BlockSpec(memory_space=pltpu.VMEM)
HBM = pl.BlockSpec(memory_space=pltpu.HBM)


def spread_residues(scalars, positions, width):
    value = jnp.full(positions.shape, scalars[0], jnp.int32)
    first = jnp.zeros(positions.shape, jnp.int32)
    for residue in range(1, len(scalars)):
        here = positions >= residue * width
        value = jnp.where(here, scalars[residue], value)
        first = jnp.where(here, residue * width, first)
    return value, positions - first


def table_lookup(types, table):
    value = jnp.full(types.shape, table[0], jnp.int32)
    for kind in range(1, len(table)):
        if table[kind] != table[0]:
            value = jnp.where(types == kind, table[kind], value)
    return value


def split_rows(x):
    high = x.astype(jnp.bfloat16).astype(jnp.float32)
    rest = x - high
    middle = rest.astype(jnp.bfloat16).astype(jnp.float32)
    return high, middle, rest - middle


def one_hot(rank):
    size = rank.shape[1]
    place = lax.broadcasted_iota(jnp.int32, (size, size), 0)
    return jnp.where(place == rank, 1.0, 0.0).astype(jnp.bfloat16)


def exact_dot(x, selection, contract):
    rows = x.shape[0]
    parts = jnp.concatenate(split_rows(x), axis=0).astype(jnp.bfloat16)
    out = lax.dot_general(parts, selection, (((1,), (contract,)), ((), ())), preferred_element_type=jnp.float32)
    return out[:rows] + out[rows : 2 * rows] + out[2 * rows :]


def prep_kernel(*refs):
    inputs, (block_ref, rank_ref), scratch = refs[:7], refs[7:9], refs[9:]
    (types_ref, flags_ref, pf_ref, tf_ref, pa_ref, ta_ref, mask_ref, pad_ref, earlier_ref, sems) = scratch
    fetches = [pltpu.make_async_copy(src, dst, sems.at[i]) for i, (src, dst) in enumerate(zip(inputs, scratch))]
    for fetch in fetches:
        fetch.start()
    residues = types_ref.shape[0]
    frames = pf_ref.shape[1]
    own_atoms = pa_ref.shape[1]
    lanes = pad_ref.shape[1]
    pad_ref[...] = jnp.zeros(pad_ref.shape, jnp.float32)
    earlier = lax.broadcasted_iota(jnp.int32, (lanes, lanes), 0) < lax.broadcasted_iota(jnp.int32, (lanes, lanes), 1)
    earlier_ref[...] = jnp.where(earlier, 1.0, 0.0).astype(jnp.bfloat16)
    for fetch in fetches:
        fetch.wait()
    codes = [types_ref[r] + 32 * flags_ref[r] for r in range(residues)]

    pad_ref[0:3, 0:own_atoms] = pa_ref[...]
    pad_ref[3:6, 0:own_atoms] = ta_ref[...]
    pad_ref[6:7, 0:own_atoms] = mask_ref[...].astype(jnp.float32)
    atoms = pad_ref[...]
    place = lax.broadcasted_iota(jnp.int32, (1, lanes), 1)
    code, slot = spread_residues(codes, place, ATOM_SLOTS)
    types = code & 31
    swapped = code >= 32
    twice = (types == 13) | (types == 18)

    def opens_pair(s):
        pair = ((s == 6) & ((types == 3) | twice)) | ((s == 7) & (types == 6)) | ((s == 8) & twice)
        return swapped & pair

    after = jnp.where(opens_pair(slot), 1, 0)
    before = jnp.where(opens_pair(slot - 1), 1, 0)
    row = lax.broadcasted_iota(jnp.int32, (8, lanes), 0)
    renamed = jnp.where(
        jnp.broadcast_to(after, (8, lanes)) == 1,
        pltpu.roll(atoms, lanes - 1, 1),
        jnp.where(jnp.broadcast_to(before, (8, lanes)) == 1, pltpu.roll(atoms, 1, 1), atoms),
    )
    atoms = jnp.where(row < 3, atoms, renamed)
    real = (slot < table_lookup(types, ATOM_COUNTS)) & (place < own_atoms)
    real = jnp.broadcast_to(jnp.where(real, 1, 0), (8, lanes)) == 1
    atoms = jnp.where((row == 6) & ~real, 0.0, atoms)
    weight = atoms[6:7]
    earlier = earlier_ref[...]
    rank = jnp.dot(
        jnp.broadcast_to(weight, (16, lanes)).astype(jnp.bfloat16), earlier, preferred_element_type=jnp.float32
    )[0:1]
    atom_rank = jnp.where(weight > 0.5, rank, -1.0).astype(jnp.int32)
    atom_count = jnp.sum(weight, axis=1, keepdims=True)

    place = lax.broadcasted_iota(jnp.int32, (1, frames), 1)
    code, slot = spread_residues(codes, place, FRAME_SLOTS)
    types = code & 31
    swapped = code >= 32
    chi = table_lookup(types, CHI_COUNTS)
    exists = (slot == 0) | (slot == 3) | ((slot >= 4) & (slot - 3 <= chi))
    exists = jnp.where(exists, 1.0, 0.0)
    half_turn = ((types == 3) | (types == 13) | (types == 18)) & (slot == 5)
    half_turn = swapped & (half_turn | ((types == 6) & (slot == 6)))
    sign = jnp.where(half_turn, -1.0, 1.0)
    rot_pred = [[pf_ref[pl.ds(3 * a + c, 1), :] for c in range(3)] for a in range(3)]
    rot_true = [[tf_ref[pl.ds(3 * a + c, 1), :] for c in range(3)] for a in range(3)]
    rot_true = [[r[0], r[1] * sign, r[2] * sign] for r in rot_true]
    rows = []
    shifts = []
    for a in range(3):
        rel = [
            rot_pred[a][0] * rot_true[b][0] + rot_pred[a][1] * rot_true[b][1] + rot_pred[a][2] * rot_true[b][2]
            for b in range(3)
        ]
        shift = rel[0] * tf_ref[9:10, :] + rel[1] * tf_ref[10:11, :] + rel[2] * tf_ref[11:12, :]
        shifts.append(shift - pf_ref[pl.ds(9 + a, 1), :])
        if a < 2:
            rows += [-rel[0], -rel[1], -rel[2]]
    rows += shifts + [exists]
    rows += [jnp.zeros((16 - len(rows), frames), jnp.float32)]
    rank = jnp.dot(
        jnp.broadcast_to(exists, (16, frames)).astype(jnp.bfloat16),
        earlier[:frames, :frames],
        preferred_element_type=jnp.float32,
    )[0:1]
    frame_rank = jnp.where(exists > 0.5, rank, -1.0).astype(jnp.int32)
    frame_count = jnp.sum(exists, axis=1, keepdims=True)

    atoms = exact_dot(atoms, one_hot(atom_rank), 1)
    packed = exact_dot(jnp.concatenate(rows, axis=0), one_hot(frame_rank), 1)
    first = jnp.where(place == 0, frame_count, jnp.where(place == 1, atom_count, packed[9:10]))
    extra = jnp.concatenate([first, packed[8:9]], axis=1)
    atoms = jnp.where(row == 7, jnp.broadcast_to(extra, (8, lanes)), atoms)
    block = jnp.concatenate([atoms, packed[0:8]], axis=1)
    block_ref[0] = block
    rank_ref[...] = jnp.zeros(rank_ref.shape, jnp.int32)
    rank_ref[0:1, :] = atom_rank
    rank_ref[1:2, 0:frames] = frame_rank


def exchange_steps(gx_size, gy_size):
    steps = [("gy", 1 << k) for k in range(gy_size.bit_length() - 1)]
    steps += [("gx", 1 << k) for k in range(1, gx_size.bit_length() - 1)]
    return steps + [("gx", 1)]


def device_code(gx_size, gy_size):
    code = 0
    for k, (axis, step) in enumerate(exchange_steps(gx_size, gy_size)):
        code = code + jnp.where(lax.axis_index(axis) & step != 0, 1 << k, 0)
    return code


def place_half(blocks_ref, code, src_ref, fsrc_ref):
    devices = blocks_ref.shape[0]
    lane = lax.broadcasted_iota(jnp.int32, (8, 128), 1)
    sub = lax.broadcasted_iota(jnp.int32, (8, 128), 0)
    src_ref[...] = jnp.zeros(src_ref.shape, jnp.float32)
    fsrc_ref[...] = jnp.zeros(fsrc_ref.shape, jnp.float32)

    def place_block(device, carry):
        atoms_before, frames_before, my_atoms, my_frames = carry
        my_atoms = jnp.where(device == code, atoms_before, my_atoms)
        my_frames = jnp.where(device == code, frames_before, my_frames)
        block = jnp.bitwise_xor(code, device)
        frame_count = jnp.max(blocks_ref[block, 7:8, 0:1]).astype(jnp.int32)
        atom_count = jnp.max(blocks_ref[block, 7:8, 1:2]).astype(jnp.int32)
        tile = atoms_before // 128
        turn = atoms_before % 128
        low = pltpu.roll(blocks_ref[block, :, 0:128], turn, 1)
        high = pltpu.roll(blocks_ref[block, :, 128:256], turn, 1)
        inside = lane >= turn
        src_ref[tile] += jnp.where(inside, low, 0.0)
        src_ref[tile + 1] += jnp.where(inside, high, low)
        src_ref[tile + 2] += jnp.where(inside, 0.0, high)
        exists = jnp.where(lane[0:1] < 2, 1.0, blocks_ref[block, 7:8, 0:128])
        last = jnp.broadcast_to(blocks_ref[block, 7:8, 128:256], (8, 128))
        tile = frames_before // 128
        turn = frames_before % 128
        low = pltpu.roll(blocks_ref[block, :, 256:384], turn, 1)
        high = pltpu.roll(jnp.where(sub == 0, last, jnp.broadcast_to(exists, (8, 128))), turn, 1)
        inside = lane >= turn
        fsrc_ref[tile, 0:8] += jnp.where(inside, low, 0.0)
        fsrc_ref[tile, 8:16] += jnp.where(inside, high, 0.0)
        fsrc_ref[tile + 1, 0:8] += jnp.where(inside, 0.0, low)
        fsrc_ref[tile + 1, 8:16] += jnp.where(inside, 0.0, high)
        return (atoms_before + atom_count, frames_before + frame_count, my_atoms, my_frames)

    group = 16
    while devices % group:
        group //= 2

    def place_group(index, carry):
        for k in range(group):
            carry = place_block(index * group + k, carry)
        return carry

    carry = (0, 0, 0, 0)
    if devices == group:
        return place_group(0, carry)
    return lax.fori_loop(0, devices // group, place_group, carry)


def frame_chunks(frame_total):
    return (frame_total + ROW_CHUNK - 1) // ROW_CHUNK


def atom_groups(atom_total):
    width = TILE * TILE_GROUP
    return (atom_total + width - 1) // width


def build_rows(fsrc_ref, lhs_ref, frame_total):
    sub = lax.broadcasted_iota(jnp.int32, (8, 128), 0)

    def build(index, carry):
        for k in range(BUILD_GROUP):
            tile = index * BUILD_GROUP + k
            part = fsrc_ref[tile, 0:8]
            last = fsrc_ref[tile, 8:9]
            exists = fsrc_ref[tile, 9:10]
            a = [part[k : k + 1] for k in range(3)]
            b = [part[3 + k : 4 + k] for k in range(3)]
            cross = [a[2] * b[1] - a[1] * b[2], a[0] * b[2] - a[2] * b[0], a[1] * b[0] - a[0] * b[1]]
            rotations = (part[0:3], part[3:6], jnp.concatenate(cross, axis=0))
            shifts = (part[6:7], part[7:8], last)
            for c in range(3):
                block = jnp.concatenate([rotations[c], rotations[c], shifts[c], exists], axis=0)
                high, middle, low = split_rows(block)
                ones = jnp.broadcast_to(exists, (8, 128))
                stack = [
                    jnp.where((sub >= 3) & (sub < 6), middle, high),
                    jnp.where(sub < 3, low, jnp.where(sub == 6, middle, high)),
                    jnp.where(sub < 3, middle, jnp.where(sub == 6, low, high)),
                ]
                stack = [x if k == c else jnp.where(sub == 7, 0.0, x) for k, x in enumerate(stack)]
                stack.append(jnp.where((sub == c) | (sub == 3 + c), ones, 0.0))
                stack.append(jnp.zeros((96, 128), jnp.float32))
                turned = jnp.concatenate(stack, axis=0).T
                lhs_ref[pl.ds(8 * tile, 8), c] = turned.astype(jnp.bfloat16).reshape(8, 16, 128)
        return carry

    step = 128 * BUILD_GROUP
    groups = (frame_total + step - 1) // step
    lax.fori_loop(0, groups, build, 0)

    def clear(index, carry):
        lhs_ref[index] = jnp.zeros(lhs_ref.shape[1:], jnp.bfloat16)
        return carry

    lax.fori_loop(groups * (8 * BUILD_GROUP), frame_chunks(frame_total) * (ROW_CHUNK // 16), clear, 0)


def build_columns(src_ref, rhs_ref, atom_total):
    per_tile = TILE // 128

    def build(index, carry):
        for k in range(TILE_GROUP):
            tile = index * TILE_GROUP + k
            x = jnp.concatenate([src_ref[tile * per_tile + m] for m in range(per_tile)], axis=1)
            high, middle, low = split_rows(x)
            one = jnp.ones((1, TILE), jnp.float32)
            nil = jnp.zeros((2, TILE), jnp.float32)
            rows = [high[3:6], high[3:6], one, high[0:1], high[3:6], middle[3:6], one, high[1:2]]
            rows += [middle[3:6], low[3:6], one, high[2:3], middle[0:3], low[0:3], nil]
            rhs_ref[tile] = jnp.concatenate(rows, axis=0).astype(jnp.bfloat16)
        return carry

    lax.fori_loop(0, atom_groups(atom_total), build, 0)


def pair_block(lhs_ref, chunk, rhs_ref, src_ref, index, col_ref, row_ref, before_ref, first):
    row_step = ROW_CHUNK // 16
    per_tile = TILE // 128
    start = chunk * ROW_CHUNK if isinstance(chunk, int) else pl.multiple_of(chunk * ROW_CHUNK, 8)
    lhs = lhs_ref[pl.ds(chunk * row_step, row_step)].reshape(3 * ROW_CHUNK, 128)[:, 0:32]
    for pair in range(0, TILE_GROUP, 2):
        tiles = [index * TILE_GROUP + pair + k for k in range(2)]
        dots = [jnp.dot(lhs, rhs_ref[tile], preferred_element_type=jnp.float32) for tile in tiles]
        caps = []
        for tile in tiles:
            cap = jnp.concatenate([src_ref[tile * per_tile + m, 6:7, :] for m in range(per_tile)], axis=1)
            caps.append(jnp.broadcast_to(cap * clamp_length, (8, TILE)))
        columns = [None, None]
        for g in range(ROW_CHUNK // 8):
            base = 48 * (g // 2) + 8 * (g % 2)
            span = pl.ds(start + 8 * g, 8)
            row_sum = None
            if row_ref is not None and not (first and pair == 0):
                row_sum = row_ref[span, :]
            elif row_ref is not None and before_ref is not None:
                row_sum = before_ref[span, :]
            for k in range(2):
                w0, w1, w2 = (dots[k][base + 16 * c : base + 16 * c + 8] for c in range(3))
                square = (w0 * w0 + w1 * w1) + (w2 * w2 + eps_square)
                distance = jnp.minimum(square * lax.rsqrt(square), caps[k])
                columns[k] = distance if columns[k] is None else columns[k] + distance
                if row_ref is not None:
                    for m in range(per_tile):
                        piece = distance[:, 128 * m : 128 * m + 128]
                        row_sum = piece if row_sum is None else row_sum + piece
            if row_ref is not None:
                row_ref[span, :] = row_sum
        for k, tile in enumerate(tiles):
            for m in range(per_tile):
                piece = columns[k][:, 128 * m : 128 * m + 128]
                if first:
                    col_ref[tile * per_tile + m] = piece
                else:
                    col_ref[tile * per_tile + m] += piece


def all_pairs(*jobs):
    simple = True
    for lhs_ref, frame_total, rhs_ref, src_ref, atom_total, col_ref, row_ref, before_ref in jobs:
        col_ref[...] = jnp.zeros(col_ref.shape, jnp.float32)
        if row_ref is not None:
            behind = pl.multiple_of(frame_chunks(frame_total) * ROW_CHUNK, 8)
            row_ref[pl.ds(behind, 256), :] = jnp.zeros((256, 128), jnp.float32)
        simple = (frame_total <= ROW_CHUNK) & (atom_total <= TILE * TILE_GROUP) & simple

    @pl.when(simple)
    def _():
        for lhs_ref, frame_total, rhs_ref, src_ref, atom_total, col_ref, row_ref, before_ref in jobs:
            pair_block(lhs_ref, 0, rhs_ref, src_ref, 0, col_ref, row_ref, before_ref, True)

    @pl.when(jnp.logical_not(simple))
    def _():
        for job in jobs:
            loop_pairs(*job)


def loop_pairs(lhs_ref, frame_total, rhs_ref, src_ref, atom_total, col_ref, row_ref, before_ref):
    def one_chunk(chunk, carry):
        if row_ref is not None:
            span = pl.ds(pl.multiple_of(chunk * ROW_CHUNK, 8), ROW_CHUNK)
            row_ref[span, :] = jnp.zeros((ROW_CHUNK, 128), jnp.float32) if before_ref is None else before_ref[span, :]

        def one_group(index, carry):
            pair_block(lhs_ref, chunk, rhs_ref, src_ref, index, col_ref, row_ref, before_ref, False)
            return carry

        return lax.fori_loop(0, atom_groups(atom_total), one_group, carry)

    lax.fori_loop(0, frame_chunks(frame_total), one_chunk, 0)


def idle_rows(frame_total):
    return (frame_chunks(frame_total) * ROW_CHUNK - frame_total).astype(jnp.float32)


def least_distance():
    square = jnp.full((1, 128), eps_square, jnp.float32)
    return square * lax.rsqrt(square)


def column_total(atom_total, src_ref, col_ref, idle):
    def add_group(index, carry):
        sums, floor = carry
        per_group = TILE // 128 * TILE_GROUP
        for k in range(per_group):
            tile = index * per_group + k
            sums = sums + col_ref[tile]
            floor = floor + jnp.minimum(least_distance(), src_ref[tile, 6:7, :] * clamp_length)
        return sums, floor

    carry = (jnp.zeros((8, 128), jnp.float32), jnp.zeros((1, 128), jnp.float32))
    sums, floor = lax.fori_loop(0, atom_groups(atom_total), add_group, carry)
    return jnp.sum(sums, axis=0, keepdims=True) - idle * floor


def first_kernel(sizes, blocks_ref, loss_ref, src_ref, rhs_ref, lhs_ref, row_ref, col_ref, info_ref, fsrc_ref):
    code = device_code(*sizes) & (blocks_ref.shape[0] - 1)
    info = place_half(blocks_ref, code, src_ref, fsrc_ref)
    build_rows(fsrc_ref, lhs_ref, info[1])
    build_columns(src_ref, rhs_ref, info[0])
    for k, value in enumerate(info):
        info_ref[k : k + 1, :] = jnp.full((1, 128), value, jnp.int32)
    all_pairs((lhs_ref, info[1], rhs_ref, src_ref, info[0], col_ref, row_ref, None))
    loss = column_total(info[0], src_ref, col_ref, idle_rows(info[1]))
    loss_ref[...] = jnp.broadcast_to(loss, loss_ref.shape)


def second_kernel(
    sizes,
    blocks_ref,
    rank_ref,
    src_ref,
    rhs_ref,
    lhs_ref,
    before_ref,
    col_ref,
    info_ref,
    frame_ref,
    atom_ref,
    cross_ref,
    far_src_ref,
    far_rhs_ref,
    far_lhs_ref,
    row_ref,
    near_far_ref,
    far_near_ref,
    fsrc_ref,
):
    half = blocks_ref.shape[0]
    frames = frame_ref.shape[1]
    own_atoms = atom_ref.shape[1]
    code = device_code(*sizes)
    atoms, frame_total, my_atoms, my_frames = (jnp.max(info_ref[k : k + 1, 0:1]) for k in range(4))
    far_atoms, far_frames, _, _ = place_half(blocks_ref, code & (half - 1), far_src_ref, fsrc_ref)
    build_rows(fsrc_ref, far_lhs_ref, far_frames)
    build_columns(far_src_ref, far_rhs_ref, far_atoms)
    all_pairs(
        (lhs_ref, frame_total, far_rhs_ref, far_src_ref, far_atoms, near_far_ref, row_ref, before_ref),
        (far_lhs_ref, far_frames, rhs_ref, src_ref, atoms, far_near_ref, None, None),
    )

    lane = lax.broadcasted_iota(jnp.int32, (8, 128), 1)
    idle = idle_rows(frame_total)
    far_idle = idle_rows(far_frames)
    least = least_distance()
    near_far = column_total(far_atoms, far_src_ref, near_far_ref, idle)
    far_near = column_total(atoms, src_ref, far_near_ref, far_idle)
    atom_number = (atoms + far_atoms).astype(jnp.float32)
    frame_number = (frame_total + far_frames).astype(jnp.float32)
    scale = 1.0 / clamp_length
    upper = code >= half
    cross_ref[0:1, :] = jnp.where(upper, far_near, near_far)
    cross_ref[1:2, :] = jnp.where(upper, near_far, far_near)
    cross_ref[2:3, :] = jnp.full((1, 128), scale, jnp.float32) / (frame_number * atom_number)

    tile = my_atoms // 128
    turn = my_atoms % 128
    pieces = []
    for k in range(3):
        cap = src_ref[tile + k, 6:7, :] * clamp_length
        sums = jnp.sum(col_ref[tile + k] + far_near_ref[tile + k], axis=0, keepdims=True)
        sums = sums - (idle + far_idle) * jnp.minimum(least, cap)
        pieces.append(pltpu.roll(jnp.broadcast_to(sums, (8, 128)), (128 - turn) % 128, 1))
    keep = lane < 128 - turn
    mine = jnp.concatenate([jnp.where(keep, pieces[k], pieces[k + 1]) for k in range(2)], axis=1)
    mine = exact_dot(mine, one_hot(rank_ref[0:1, :]), 0)[0:1]
    atom_ref[...] = mine[:, :own_atoms] * scale / frame_number

    tile = my_frames // 128
    turn = my_frames % 128
    pieces = []
    for k in range(2):
        rows = row_ref[pl.ds(pl.multiple_of((tile + k) * 128, 128), 128), :]
        sums = jnp.sum(rows.T, axis=0, keepdims=True)
        pieces.append(pltpu.roll(jnp.broadcast_to(sums, (8, 128)), (128 - turn) % 128, 1))
    mine = jnp.where(lane < 128 - turn, pieces[0], pieces[1])
    mine = exact_dot(mine, one_hot(rank_ref[1:2, 0:frames]), 0)[0:1]
    frame_ref[...] = mine * scale / atom_number


def finish_kernel(sizes, near_ref, far_ref, cross_ref, frames_ref, atoms_ref, frame_ref, atom_ref, total_ref):
    upper = (device_code(*sizes) * 2) // (sizes[0] * sizes[1]) == 1
    near = near_ref[0:1, :]
    far = far_ref[0:1, :]
    loss = jnp.where(upper, far, near) + cross_ref[0:1, :]
    loss = loss + (cross_ref[1:2, :] + jnp.where(upper, near, far))
    total_ref[...] = jnp.sum(loss, axis=1, keepdims=True) * cross_ref[2:3, 0:1]
    frame_ref[...] = frames_ref[...]
    atom_ref[...] = atoms_ref[...]


def shards(pred_frames, true_frames, pred_atoms, true_atoms, atom_mask, residue_types, swap_flags):
    devices = lax.axis_size("gx") * lax.axis_size("gy")
    frames = pred_frames.shape[1]
    own_atoms = pred_atoms.shape[1]
    lanes = -(-own_atoms // 128) * 128
    f32 = jnp.float32
    inputs = (residue_types, swap_flags, pred_frames, true_frames, pred_atoms, true_atoms)
    inputs += (atom_mask.reshape(1, own_atoms),)
    blocks, ranks = pl.pallas_call(
        prep_kernel,
        out_shape=(
            jax.ShapeDtypeStruct((1, 8, lanes + frames), f32),
            jax.ShapeDtypeStruct((8, lanes), jnp.int32),
        ),
        in_specs=[HBM] * 7,
        out_specs=(VMEM, VMEM),
        scratch_shapes=[
            pltpu.SMEM(residue_types.shape, jnp.int32),
            pltpu.SMEM(swap_flags.shape, jnp.int32),
            pltpu.VMEM(pred_frames.shape, f32),
            pltpu.VMEM(true_frames.shape, f32),
            pltpu.VMEM(pred_atoms.shape, f32),
            pltpu.VMEM(true_atoms.shape, f32),
            pltpu.VMEM((1, own_atoms), jnp.int32),
            pltpu.VMEM((8, lanes), f32),
            pltpu.VMEM((lanes, lanes), jnp.bfloat16),
            pltpu.SemaphoreType.DMA((7,)),
        ],
        compiler_params=pltpu.CompilerParams(vmem_limit_bytes=8 << 20),
        name="prep",
    )(*[pltpu.with_memory_space_constraint(x, pltpu.HBM) for x in inputs])
    sizes = (lax.axis_size("gx"), lax.axis_size("gy"))
    far = None
    for axis, step in exchange_steps(*sizes):
        if far is not None:
            blocks = jnp.concatenate([blocks, far], axis=0)
        far = lax.ppermute(blocks, axis, [(i, i ^ step) for i in range(lax.axis_size(axis))])
    half = devices // 2
    groups = -(-(half * own_atoms + 256) // (TILE * TILE_GROUP))
    tiles = groups * TILE_GROUP * (TILE // 128)
    most = half * (frames * USED_SLOTS // FRAME_SLOTS)
    frame_tiles = -(-most // (128 * BUILD_GROUP)) * BUILD_GROUP + 1
    row_groups = 8 * frame_tiles + 2 * (ROW_CHUNK // 16) + 16
    columns = ((tiles, 8, 128), f32)
    frame_source = ((frame_tiles, 16, 128), f32)
    right = ((groups * TILE_GROUP, 32, TILE), jnp.bfloat16)
    left = ((row_groups, 3, 16, 128), jnp.bfloat16)
    rows = ((row_groups * 16, 128), f32)

    def room(*arrays):
        return sum(jnp.dtype(d).itemsize * functools.reduce(lambda a, b: a * b, shape) for shape, d in arrays)

    kept = [((8, 128), f32), columns, right, left, rows, columns, ((8, 128), jnp.int32)]
    loss, *near = pl.pallas_call(
        functools.partial(first_kernel, sizes),
        out_shape=[jax.ShapeDtypeStruct(*x) for x in kept],
        in_specs=[VMEM],
        out_specs=[VMEM] * len(kept),
        scratch_shapes=[pltpu.VMEM(*frame_source)],
        compiler_params=pltpu.CompilerParams(vmem_limit_bytes=room(*kept, frame_source) + (8 << 20)),
        cost_estimate=pl.CostEstimate(flops=4 * 10**9, bytes_accessed=1 << 20, transcendentals=0),
        name="near",
    )(blocks)
    far_loss = lax.ppermute(loss, axis, [(i, i ^ step) for i in range(lax.axis_size(axis))])
    scratch = [columns, right, left, rows, columns, columns, frame_source]
    results = [((1, frames), f32), ((1, own_atoms), f32)]
    frame_loss, atom_loss, cross = pl.pallas_call(
        functools.partial(second_kernel, sizes),
        out_shape=[jax.ShapeDtypeStruct(*x) for x in results + [((8, 128), f32)]],
        in_specs=[VMEM] * (1 + len(kept)),
        out_specs=[VMEM] * 3,
        scratch_shapes=[pltpu.VMEM(*x) for x in scratch],
        compiler_params=pltpu.CompilerParams(vmem_limit_bytes=room(*kept, *scratch) + (8 << 20)),
        cost_estimate=pl.CostEstimate(flops=8 * 10**9, bytes_accessed=1 << 20, transcendentals=0),
        name="rest",
    )(far, ranks, *near)
    frame_loss, atom_loss, total_loss = pl.pallas_call(
        functools.partial(finish_kernel, sizes),
        out_shape=[jax.ShapeDtypeStruct(*x) for x in results + [((1, 1), f32)]],
        in_specs=[VMEM] * 5,
        out_specs=[VMEM] * 3,
        compiler_params=pltpu.CompilerParams(vmem_limit_bytes=8 << 20),
        name="finish",
    )(loss, far_loss, cross, frame_loss, atom_loss)
    return (frame_loss.reshape(frames), atom_loss.reshape(own_atoms), total_loss.reshape(1))


def solution(mesh):
    both = P(None, ("sa", "gx", "gy"))
    flat = P(("sa", "gx", "gy"))
    return jax.shard_map(
        shards,
        mesh=mesh,
        in_specs=(both, both, both, both, flat, flat, flat),
        out_specs=(flat, flat, P("sa")),
        check_vma=False,
    )
```

```python
import functools

import jax
import jax.numpy as jnp
from jax import lax
from jax.experimental import pallas as pl
from jax.experimental.pallas import tpu as pltpu
from jax.sharding import PartitionSpec as P

eps_square = 0.0001
clamp_length = 10.0

ATOM_COUNTS = (5, 11, 8, 8, 6, 9, 9, 4, 10, 8, 8, 9, 8, 11, 7, 6, 7, 14, 12, 7)
CHI_COUNTS = (0, 4, 2, 2, 1, 3, 3, 0, 2, 2, 2, 4, 3, 2, 2, 1, 1, 2, 2, 1)
FRAME_SLOTS = 8
USED_SLOTS = 6
BUILD_GROUP = 4
ATOM_SLOTS = 14
ROW_CHUNK = 544
TILE = 256
TILE_GROUP = 4
VMEM = pl.BlockSpec(memory_space=pltpu.VMEM)
HBM = pl.BlockSpec(memory_space=pltpu.HBM)


def spread_residues(scalars, positions, width):
    value = jnp.full(positions.shape, scalars[0], jnp.int32)
    first = jnp.zeros(positions.shape, jnp.int32)
    for residue in range(1, len(scalars)):
        here = positions >= residue * width
        value = jnp.where(here, scalars[residue], value)
        first = jnp.where(here, residue * width, first)
    return value, positions - first


def table_lookup(types, table):
    value = jnp.full(types.shape, table[0], jnp.int32)
    for kind in range(1, len(table)):
        if table[kind] != table[0]:
            value = jnp.where(types == kind, table[kind], value)
    return value


def split_rows(x):
    high = x.astype(jnp.bfloat16).astype(jnp.float32)
    rest = x - high
    middle = rest.astype(jnp.bfloat16).astype(jnp.float32)
    return high, middle, rest - middle


def one_hot(rank):
    size = rank.shape[1]
    place = lax.broadcasted_iota(jnp.int32, (size, size), 0)
    return jnp.where(place == rank, 1.0, 0.0).astype(jnp.bfloat16)


def exact_dot(x, selection, contract):
    rows = x.shape[0]
    parts = jnp.concatenate(split_rows(x), axis=0).astype(jnp.bfloat16)
    out = lax.dot_general(parts, selection, (((1,), (contract,)), ((), ())), preferred_element_type=jnp.float32)
    return out[:rows] + out[rows : 2 * rows] + out[2 * rows :]


def prep_kernel(*refs):
    inputs, (block_ref, rank_ref), scratch = refs[:7], refs[7:9], refs[9:]
    (types_ref, flags_ref, pf_ref, tf_ref, pa_ref, ta_ref, mask_ref, pad_ref, earlier_ref, sems) = scratch
    fetches = [pltpu.make_async_copy(src, dst, sems.at[i]) for i, (src, dst) in enumerate(zip(inputs, scratch))]
    for fetch in fetches:
        fetch.start()
    residues = types_ref.shape[0]
    frames = pf_ref.shape[1]
    own_atoms = pa_ref.shape[1]
    lanes = pad_ref.shape[1]
    pad_ref[...] = jnp.zeros(pad_ref.shape, jnp.float32)
    earlier = lax.broadcasted_iota(jnp.int32, (lanes, lanes), 0) < lax.broadcasted_iota(jnp.int32, (lanes, lanes), 1)
    earlier_ref[...] = jnp.where(earlier, 1.0, 0.0).astype(jnp.bfloat16)
    for fetch in fetches:
        fetch.wait()
    codes = [types_ref[r] + 32 * flags_ref[r] for r in range(residues)]

    pad_ref[0:3, 0:own_atoms] = pa_ref[...]
    pad_ref[3:6, 0:own_atoms] = ta_ref[...]
    pad_ref[6:7, 0:own_atoms] = mask_ref[...].astype(jnp.float32)
    atoms = pad_ref[...]
    place = lax.broadcasted_iota(jnp.int32, (1, lanes), 1)
    code, slot = spread_residues(codes, place, ATOM_SLOTS)
    types = code & 31
    swapped = code >= 32
    twice = (types == 13) | (types == 18)

    def opens_pair(s):
        pair = ((s == 6) & ((types == 3) | twice)) | ((s == 7) & (types == 6)) | ((s == 8) & twice)
        return swapped & pair

    after = jnp.where(opens_pair(slot), 1, 0)
    before = jnp.where(opens_pair(slot - 1), 1, 0)
    row = lax.broadcasted_iota(jnp.int32, (8, lanes), 0)
    renamed = jnp.where(
        jnp.broadcast_to(after, (8, lanes)) == 1,
        pltpu.roll(atoms, lanes - 1, 1),
        jnp.where(jnp.broadcast_to(before, (8, lanes)) == 1, pltpu.roll(atoms, 1, 1), atoms),
    )
    atoms = jnp.where(row < 3, atoms, renamed)
    real = (slot < table_lookup(types, ATOM_COUNTS)) & (place < own_atoms)
    real = jnp.broadcast_to(jnp.where(real, 1, 0), (8, lanes)) == 1
    atoms = jnp.where((row == 6) & ~real, 0.0, atoms)
    weight = atoms[6:7]
    earlier = earlier_ref[...]
    rank = jnp.dot(
        jnp.broadcast_to(weight, (16, lanes)).astype(jnp.bfloat16), earlier, preferred_element_type=jnp.float32
    )[0:1]
    atom_rank = jnp.where(weight > 0.5, rank, -1.0).astype(jnp.int32)
    atom_count = jnp.sum(weight, axis=1, keepdims=True)

    place = lax.broadcasted_iota(jnp.int32, (1, frames), 1)
    code, slot = spread_residues(codes, place, FRAME_SLOTS)
    types = code & 31
    swapped = code >= 32
    chi = table_lookup(types, CHI_COUNTS)
    exists = (slot == 0) | (slot == 3) | ((slot >= 4) & (slot - 3 <= chi))
    exists = jnp.where(exists, 1.0, 0.0)
    half_turn = ((types == 3) | (types == 13) | (types == 18)) & (slot == 5)
    half_turn = swapped & (half_turn | ((types == 6) & (slot == 6)))
    sign = jnp.where(half_turn, -1.0, 1.0)
    rot_pred = [[pf_ref[pl.ds(3 * a + c, 1), :] for c in range(3)] for a in range(3)]
    rot_true = [[tf_ref[pl.ds(3 * a + c, 1), :] for c in range(3)] for a in range(3)]
    rot_true = [[r[0], r[1] * sign, r[2] * sign] for r in rot_true]
    rows = []
    shifts = []
    for a in range(3):
        rel = [
            rot_pred[a][0] * rot_true[b][0] + rot_pred[a][1] * rot_true[b][1] + rot_pred[a][2] * rot_true[b][2]
            for b in range(3)
        ]
        shift = rel[0] * tf_ref[9:10, :] + rel[1] * tf_ref[10:11, :] + rel[2] * tf_ref[11:12, :]
        shifts.append(shift - pf_ref[pl.ds(9 + a, 1), :])
        if a < 2:
            rows += [-rel[0], -rel[1], -rel[2]]
    rows += shifts + [exists]
    rows += [jnp.zeros((16 - len(rows), frames), jnp.float32)]
    rank = jnp.dot(
        jnp.broadcast_to(exists, (16, frames)).astype(jnp.bfloat16),
        earlier[:frames, :frames],
        preferred_element_type=jnp.float32,
    )[0:1]
    frame_rank = jnp.where(exists > 0.5, rank, -1.0).astype(jnp.int32)
    frame_count = jnp.sum(exists, axis=1, keepdims=True)

    atoms = exact_dot(atoms, one_hot(atom_rank), 1)
    packed = exact_dot(jnp.concatenate(rows, axis=0), one_hot(frame_rank), 1)
    first = jnp.where(place == 0, frame_count, jnp.where(place == 1, atom_count, packed[9:10]))
    extra = jnp.concatenate([first, packed[8:9]], axis=1)
    atoms = jnp.where(row == 7, jnp.broadcast_to(extra, (8, lanes)), atoms)
    block = jnp.concatenate([atoms, packed[0:8]], axis=1)
    block_ref[0] = block
    rank_ref[...] = jnp.zeros(rank_ref.shape, jnp.int32)
    rank_ref[0:1, :] = atom_rank
    rank_ref[1:2, 0:frames] = frame_rank


def exchange_steps(gx_size, gy_size):
    steps = [("gx", 1 << k) for k in reversed(range(1, gx_size.bit_length() - 1))]
    steps += [("gy", 1 << k) for k in range(gy_size.bit_length() - 1)]
    return steps + [("gx", 1)]


def device_code(gx_size, gy_size):
    code = 0
    for k, (axis, step) in enumerate(exchange_steps(gx_size, gy_size)):
        code = code + jnp.where(lax.axis_index(axis) & step != 0, 1 << k, 0)
    return code


def place_half(blocks_ref, code, src_ref, fsrc_ref):
    devices = blocks_ref.shape[0]
    lane = lax.broadcasted_iota(jnp.int32, (8, 128), 1)
    sub = lax.broadcasted_iota(jnp.int32, (8, 128), 0)
    src_ref[...] = jnp.zeros(src_ref.shape, jnp.float32)
    fsrc_ref[...] = jnp.zeros(fsrc_ref.shape, jnp.float32)

    def place_block(device, carry):
        atoms_before, frames_before, my_atoms, my_frames = carry
        my_atoms = jnp.where(device == code, atoms_before, my_atoms)
        my_frames = jnp.where(device == code, frames_before, my_frames)
        block = jnp.bitwise_xor(code, device)
        frame_count = jnp.max(blocks_ref[block, 7:8, 0:1]).astype(jnp.int32)
        atom_count = jnp.max(blocks_ref[block, 7:8, 1:2]).astype(jnp.int32)
        tile = atoms_before // 128
        turn = atoms_before % 128
        low = pltpu.roll(blocks_ref[block, :, 0:128], turn, 1)
        high = pltpu.roll(blocks_ref[block, :, 128:256], turn, 1)
        inside = lane >= turn
        src_ref[tile] += jnp.where(inside, low, 0.0)
        src_ref[tile + 1] += jnp.where(inside, high, low)
        src_ref[tile + 2] += jnp.where(inside, 0.0, high)
        exists = jnp.where(lane[0:1] < 2, 1.0, blocks_ref[block, 7:8, 0:128])
        last = jnp.broadcast_to(blocks_ref[block, 7:8, 128:256], (8, 128))
        tile = frames_before // 128
        turn = frames_before % 128
        low = pltpu.roll(blocks_ref[block, :, 256:384], turn, 1)
        high = pltpu.roll(jnp.where(sub == 0, last, jnp.broadcast_to(exists, (8, 128))), turn, 1)
        inside = lane >= turn
        fsrc_ref[tile, 0:8] += jnp.where(inside, low, 0.0)
        fsrc_ref[tile, 8:16] += jnp.where(inside, high, 0.0)
        fsrc_ref[tile + 1, 0:8] += jnp.where(inside, 0.0, low)
        fsrc_ref[tile + 1, 8:16] += jnp.where(inside, 0.0, high)
        return (atoms_before + atom_count, frames_before + frame_count, my_atoms, my_frames)

    group = 16
    while devices % group:
        group //= 2

    def place_group(index, carry):
        for k in range(group):
            carry = place_block(index * group + k, carry)
        return carry

    carry = (0, 0, 0, 0)
    if devices == group:
        return place_group(0, carry)
    return lax.fori_loop(0, devices // group, place_group, carry)


def frame_chunks(frame_total):
    return (frame_total + ROW_CHUNK - 1) // ROW_CHUNK


def atom_groups(atom_total):
    width = TILE * TILE_GROUP
    return (atom_total + width - 1) // width


def build_rows(fsrc_ref, lhs_ref, frame_total):
    sub = lax.broadcasted_iota(jnp.int32, (8, 128), 0)

    def build(index, carry):
        for k in range(BUILD_GROUP):
            tile = index * BUILD_GROUP + k
            part = fsrc_ref[tile, 0:8]
            last = fsrc_ref[tile, 8:9]
            exists = fsrc_ref[tile, 9:10]
            a = [part[k : k + 1] for k in range(3)]
            b = [part[3 + k : 4 + k] for k in range(3)]
            cross = [a[2] * b[1] - a[1] * b[2], a[0] * b[2] - a[2] * b[0], a[1] * b[0] - a[0] * b[1]]
            rotations = (part[0:3], part[3:6], jnp.concatenate(cross, axis=0))
            shifts = (part[6:7], part[7:8], last)
            for c in range(3):
                block = jnp.concatenate([rotations[c], rotations[c], shifts[c], exists], axis=0)
                high, middle, low = split_rows(block)
                ones = jnp.broadcast_to(exists, (8, 128))
                stack = [
                    jnp.where((sub >= 3) & (sub < 6), middle, high),
                    jnp.where(sub < 3, low, jnp.where(sub == 6, middle, high)),
                    jnp.where(sub < 3, middle, jnp.where(sub == 6, low, high)),
                ]
                stack = [x if k == c else jnp.where(sub == 7, 0.0, x) for k, x in enumerate(stack)]
                stack.append(jnp.where((sub == c) | (sub == 3 + c), ones, 0.0))
                stack.append(jnp.zeros((96, 128), jnp.float32))
                turned = jnp.concatenate(stack, axis=0).T
                lhs_ref[pl.ds(8 * tile, 8), c] = turned.astype(jnp.bfloat16).reshape(8, 16, 128)
        return carry

    step = 128 * BUILD_GROUP
    groups = (frame_total + step - 1) // step
    lax.fori_loop(0, groups, build, 0)

    def clear(index, carry):
        lhs_ref[index] = jnp.zeros(lhs_ref.shape[1:], jnp.bfloat16)
        return carry

    lax.fori_loop(groups * (8 * BUILD_GROUP), frame_chunks(frame_total) * (ROW_CHUNK // 16), clear, 0)


def build_columns(src_ref, rhs_ref, atom_total):
    per_tile = TILE // 128

    def build(index, carry):
        for k in range(TILE_GROUP):
            tile = index * TILE_GROUP + k
            x = jnp.concatenate([src_ref[tile * per_tile + m] for m in range(per_tile)], axis=1)
            high, middle, low = split_rows(x)
            one = jnp.ones((1, TILE), jnp.float32)
            nil = jnp.zeros((2, TILE), jnp.float32)
            rows = [high[3:6], high[3:6], one, high[0:1], high[3:6], middle[3:6], one, high[1:2]]
            rows += [middle[3:6], low[3:6], one, high[2:3], middle[0:3], low[0:3], nil]
            rhs_ref[tile] = jnp.concatenate(rows, axis=0).astype(jnp.bfloat16)
        return carry

    lax.fori_loop(0, atom_groups(atom_total), build, 0)


def pair_block(lhs_ref, chunk, rhs_ref, src_ref, index, col_ref, row_ref, before_ref, first):
    row_step = ROW_CHUNK // 16
    per_tile = TILE // 128
    start = chunk * ROW_CHUNK if isinstance(chunk, int) else pl.multiple_of(chunk * ROW_CHUNK, 8)
    lhs = lhs_ref[pl.ds(chunk * row_step, row_step)].reshape(3 * ROW_CHUNK, 128)[:, 0:32]
    for pair in range(0, TILE_GROUP, 2):
        tiles = [index * TILE_GROUP + pair + k for k in range(2)]
        dots = [jnp.dot(lhs, rhs_ref[tile], preferred_element_type=jnp.float32) for tile in tiles]
        caps = []
        for tile in tiles:
            cap = jnp.concatenate([src_ref[tile * per_tile + m, 6:7, :] for m in range(per_tile)], axis=1)
            caps.append(jnp.broadcast_to(cap * clamp_length, (8, TILE)))
        columns = [None, None]
        for g in range(ROW_CHUNK // 8):
            base = 48 * (g // 2) + 8 * (g % 2)
            span = pl.ds(start + 8 * g, 8)
            row_sum = None
            if row_ref is not None and not (first and pair == 0):
                row_sum = row_ref[span, :]
            elif row_ref is not None and before_ref is not None:
                row_sum = before_ref[span, :]
            for k in range(2):
                w0, w1, w2 = (dots[k][base + 16 * c : base + 16 * c + 8] for c in range(3))
                square = (w0 * w0 + w1 * w1) + (w2 * w2 + eps_square)
                distance = jnp.minimum(square * lax.rsqrt(square), caps[k])
                columns[k] = distance if columns[k] is None else columns[k] + distance
                if row_ref is not None:
                    for m in range(per_tile):
                        piece = distance[:, 128 * m : 128 * m + 128]
                        row_sum = piece if row_sum is None else row_sum + piece
            if row_ref is not None:
                row_ref[span, :] = row_sum
        for k, tile in enumerate(tiles):
            for m in range(per_tile):
                piece = columns[k][:, 128 * m : 128 * m + 128]
                if first:
                    col_ref[tile * per_tile + m] = piece
                else:
                    col_ref[tile * per_tile + m] += piece


def all_pairs(*jobs):
    simple = True
    for lhs_ref, frame_total, rhs_ref, src_ref, atom_total, col_ref, row_ref, before_ref in jobs:
        col_ref[...] = jnp.zeros(col_ref.shape, jnp.float32)
        if row_ref is not None:
            behind = pl.multiple_of(frame_chunks(frame_total) * ROW_CHUNK, 8)
            row_ref[pl.ds(behind, 256), :] = jnp.zeros((256, 128), jnp.float32)
        simple = (frame_total <= ROW_CHUNK) & (atom_total <= TILE * TILE_GROUP) & simple

    @pl.when(simple)
    def _():
        for lhs_ref, frame_total, rhs_ref, src_ref, atom_total, col_ref, row_ref, before_ref in jobs:
            pair_block(lhs_ref, 0, rhs_ref, src_ref, 0, col_ref, row_ref, before_ref, True)

    @pl.when(jnp.logical_not(simple))
    def _():
        for job in jobs:
            loop_pairs(*job)


def loop_pairs(lhs_ref, frame_total, rhs_ref, src_ref, atom_total, col_ref, row_ref, before_ref):
    def one_chunk(chunk, carry):
        if row_ref is not None:
            span = pl.ds(pl.multiple_of(chunk * ROW_CHUNK, 8), ROW_CHUNK)
            row_ref[span, :] = jnp.zeros((ROW_CHUNK, 128), jnp.float32) if before_ref is None else before_ref[span, :]

        def one_group(index, carry):
            pair_block(lhs_ref, chunk, rhs_ref, src_ref, index, col_ref, row_ref, before_ref, False)
            return carry

        return lax.fori_loop(0, atom_groups(atom_total), one_group, carry)

    lax.fori_loop(0, frame_chunks(frame_total), one_chunk, 0)


def idle_rows(frame_total):
    return (frame_chunks(frame_total) * ROW_CHUNK - frame_total).astype(jnp.float32)


def least_distance():
    square = jnp.full((1, 128), eps_square, jnp.float32)
    return square * lax.rsqrt(square)


def column_total(atom_total, src_ref, col_ref, idle):
    def add_group(index, carry):
        sums, floor = carry
        per_group = TILE // 128 * TILE_GROUP
        for k in range(per_group):
            tile = index * per_group + k
            sums = sums + col_ref[tile]
            floor = floor + jnp.minimum(least_distance(), src_ref[tile, 6:7, :] * clamp_length)
        return sums, floor

    carry = (jnp.zeros((8, 128), jnp.float32), jnp.zeros((1, 128), jnp.float32))
    sums, floor = lax.fori_loop(0, atom_groups(atom_total), add_group, carry)
    return jnp.sum(sums, axis=0, keepdims=True) - idle * floor


def first_kernel(sizes, blocks_ref, loss_ref, src_ref, rhs_ref, lhs_ref, row_ref, col_ref, info_ref, fsrc_ref):
    code = device_code(*sizes) & (blocks_ref.shape[0] - 1)
    info = place_half(blocks_ref, code, src_ref, fsrc_ref)
    build_rows(fsrc_ref, lhs_ref, info[1])
    build_columns(src_ref, rhs_ref, info[0])
    for k, value in enumerate(info):
        info_ref[k : k + 1, :] = jnp.full((1, 128), value, jnp.int32)
    all_pairs((lhs_ref, info[1], rhs_ref, src_ref, info[0], col_ref, row_ref, None))
    loss = column_total(info[0], src_ref, col_ref, idle_rows(info[1]))
    loss_ref[...] = jnp.broadcast_to(loss, loss_ref.shape)


def second_kernel(
    sizes,
    blocks_ref,
    rank_ref,
    src_ref,
    rhs_ref,
    lhs_ref,
    before_ref,
    col_ref,
    info_ref,
    frame_ref,
    atom_ref,
    cross_ref,
    far_src_ref,
    far_rhs_ref,
    far_lhs_ref,
    row_ref,
    near_far_ref,
    far_near_ref,
    fsrc_ref,
):
    half = blocks_ref.shape[0]
    frames = frame_ref.shape[1]
    own_atoms = atom_ref.shape[1]
    code = device_code(*sizes)
    atoms, frame_total, my_atoms, my_frames = (jnp.max(info_ref[k : k + 1, 0:1]) for k in range(4))
    far_atoms, far_frames, _, _ = place_half(blocks_ref, code & (half - 1), far_src_ref, fsrc_ref)
    build_rows(fsrc_ref, far_lhs_ref, far_frames)
    build_columns(far_src_ref, far_rhs_ref, far_atoms)
    all_pairs(
        (lhs_ref, frame_total, far_rhs_ref, far_src_ref, far_atoms, near_far_ref, row_ref, before_ref),
        (far_lhs_ref, far_frames, rhs_ref, src_ref, atoms, far_near_ref, None, None),
    )

    lane = lax.broadcasted_iota(jnp.int32, (8, 128), 1)
    idle = idle_rows(frame_total)
    far_idle = idle_rows(far_frames)
    least = least_distance()
    near_far = column_total(far_atoms, far_src_ref, near_far_ref, idle)
    far_near = column_total(atoms, src_ref, far_near_ref, far_idle)
    atom_number = (atoms + far_atoms).astype(jnp.float32)
    frame_number = (frame_total + far_frames).astype(jnp.float32)
    scale = 1.0 / clamp_length
    upper = code >= half
    cross_ref[0:1, :] = jnp.where(upper, far_near, near_far)
    cross_ref[1:2, :] = jnp.where(upper, near_far, far_near)
    cross_ref[2:3, :] = jnp.full((1, 128), scale, jnp.float32) / (frame_number * atom_number)

    tile = my_atoms // 128
    turn = my_atoms % 128
    pieces = []
    for k in range(3):
        cap = src_ref[tile + k, 6:7, :] * clamp_length
        sums = jnp.sum(col_ref[tile + k] + far_near_ref[tile + k], axis=0, keepdims=True)
        sums = sums - (idle + far_idle) * jnp.minimum(least, cap)
        pieces.append(pltpu.roll(jnp.broadcast_to(sums, (8, 128)), (128 - turn) % 128, 1))
    keep = lane < 128 - turn
    mine = jnp.concatenate([jnp.where(keep, pieces[k], pieces[k + 1]) for k in range(2)], axis=1)
    mine = exact_dot(mine, one_hot(rank_ref[0:1, :]), 0)[0:1]
    atom_ref[...] = mine[:, :own_atoms] * scale / frame_number

    tile = my_frames // 128
    turn = my_frames % 128
    pieces = []
    for k in range(2):
        rows = row_ref[pl.ds(pl.multiple_of((tile + k) * 128, 128), 128), :]
        sums = jnp.sum(rows.T, axis=0, keepdims=True)
        pieces.append(pltpu.roll(jnp.broadcast_to(sums, (8, 128)), (128 - turn) % 128, 1))
    mine = jnp.where(lane < 128 - turn, pieces[0], pieces[1])
    mine = exact_dot(mine, one_hot(rank_ref[1:2, 0:frames]), 0)[0:1]
    frame_ref[...] = mine * scale / atom_number


def finish_kernel(sizes, near_ref, far_ref, cross_ref, frames_ref, atoms_ref, frame_ref, atom_ref, total_ref):
    upper = (device_code(*sizes) * 2) // (sizes[0] * sizes[1]) == 1
    near = near_ref[0:1, :]
    far = far_ref[0:1, :]
    loss = jnp.where(upper, far, near) + cross_ref[0:1, :]
    loss = loss + (cross_ref[1:2, :] + jnp.where(upper, near, far))
    total_ref[...] = jnp.sum(loss, axis=1, keepdims=True) * cross_ref[2:3, 0:1]
    frame_ref[...] = frames_ref[...]
    atom_ref[...] = atoms_ref[...]


def shards(pred_frames, true_frames, pred_atoms, true_atoms, atom_mask, residue_types, swap_flags):
    devices = lax.axis_size("gx") * lax.axis_size("gy")
    frames = pred_frames.shape[1]
    own_atoms = pred_atoms.shape[1]
    lanes = -(-own_atoms // 128) * 128
    f32 = jnp.float32
    inputs = (residue_types, swap_flags, pred_frames, true_frames, pred_atoms, true_atoms)
    inputs += (atom_mask.reshape(1, own_atoms),)
    blocks, ranks = pl.pallas_call(
        prep_kernel,
        out_shape=(
            jax.ShapeDtypeStruct((1, 8, lanes + frames), f32),
            jax.ShapeDtypeStruct((8, lanes), jnp.int32),
        ),
        in_specs=[HBM] * 7,
        out_specs=(VMEM, VMEM),
        scratch_shapes=[
            pltpu.SMEM(residue_types.shape, jnp.int32),
            pltpu.SMEM(swap_flags.shape, jnp.int32),
            pltpu.VMEM(pred_frames.shape, f32),
            pltpu.VMEM(true_frames.shape, f32),
            pltpu.VMEM(pred_atoms.shape, f32),
            pltpu.VMEM(true_atoms.shape, f32),
            pltpu.VMEM((1, own_atoms), jnp.int32),
            pltpu.VMEM((8, lanes), f32),
            pltpu.VMEM((lanes, lanes), jnp.bfloat16),
            pltpu.SemaphoreType.DMA((7,)),
        ],
        compiler_params=pltpu.CompilerParams(vmem_limit_bytes=8 << 20),
        name="prep",
    )(*[pltpu.with_memory_space_constraint(x, pltpu.HBM) for x in inputs])
    sizes = (lax.axis_size("gx"), lax.axis_size("gy"))
    far = None
    for axis, step in exchange_steps(*sizes):
        if far is not None:
            blocks = jnp.concatenate([blocks, far], axis=0)
        far = lax.ppermute(blocks, axis, [(i, i ^ step) for i in range(lax.axis_size(axis))])
    half = devices // 2
    groups = -(-(half * own_atoms + 256) // (TILE * TILE_GROUP))
    tiles = groups * TILE_GROUP * (TILE // 128)
    most = half * (frames * USED_SLOTS // FRAME_SLOTS)
    frame_tiles = -(-most // (128 * BUILD_GROUP)) * BUILD_GROUP + 1
    row_groups = 8 * frame_tiles + 2 * (ROW_CHUNK // 16) + 16
    columns = ((tiles, 8, 128), f32)
    frame_source = ((frame_tiles, 16, 128), f32)
    right = ((groups * TILE_GROUP, 32, TILE), jnp.bfloat16)
    left = ((row_groups, 3, 16, 128), jnp.bfloat16)
    rows = ((row_groups * 16, 128), f32)

    def room(*arrays):
        return sum(jnp.dtype(d).itemsize * functools.reduce(lambda a, b: a * b, shape) for shape, d in arrays)

    kept = [((8, 128), f32), columns, right, left, rows, columns, ((8, 128), jnp.int32)]
    loss, *near = pl.pallas_call(
        functools.partial(first_kernel, sizes),
        out_shape=[jax.ShapeDtypeStruct(*x) for x in kept],
        in_specs=[VMEM],
        out_specs=[VMEM] * len(kept),
        scratch_shapes=[pltpu.VMEM(*frame_source)],
        compiler_params=pltpu.CompilerParams(vmem_limit_bytes=room(*kept, frame_source) + (8 << 20)),
        cost_estimate=pl.CostEstimate(flops=4 * 10**9, bytes_accessed=1 << 20, transcendentals=0),
        name="near",
    )(blocks)
    far_loss = lax.ppermute(loss, axis, [(i, i ^ step) for i in range(lax.axis_size(axis))])
    scratch = [columns, right, left, rows, columns, columns, frame_source]
    results = [((1, frames), f32), ((1, own_atoms), f32)]
    frame_loss, atom_loss, cross = pl.pallas_call(
        functools.partial(second_kernel, sizes),
        out_shape=[jax.ShapeDtypeStruct(*x) for x in results + [((8, 128), f32)]],
        in_specs=[VMEM] * (1 + len(kept)),
        out_specs=[VMEM] * 3,
        scratch_shapes=[pltpu.VMEM(*x) for x in scratch],
        compiler_params=pltpu.CompilerParams(vmem_limit_bytes=room(*kept, *scratch) + (8 << 20)),
        cost_estimate=pl.CostEstimate(flops=8 * 10**9, bytes_accessed=1 << 20, transcendentals=0),
        name="rest",
    )(far, ranks, *near)
    frame_loss, atom_loss, total_loss = pl.pallas_call(
        functools.partial(finish_kernel, sizes),
        out_shape=[jax.ShapeDtypeStruct(*x) for x in results + [((1, 1), f32)]],
        in_specs=[VMEM] * 5,
        out_specs=[VMEM] * 3,
        compiler_params=pltpu.CompilerParams(vmem_limit_bytes=8 << 20),
        name="finish",
    )(loss, far_loss, cross, frame_loss, atom_loss)
    return (frame_loss.reshape(frames), atom_loss.reshape(own_atoms), total_loss.reshape(1))


def solution(mesh):
    both = P(None, ("sa", "gx", "gy"))
    flat = P(("sa", "gx", "gy"))
    return jax.shard_map(
        shards,
        mesh=mesh,
        in_specs=(both, both, both, both, flat, flat, flat),
        out_specs=(flat, flat, P("sa")),
        check_vma=False,
    )
```
